32 devices in a mesh: groups: 2 (over y), band: 4 (over z), chan: 4 (over x, core).
Axes of the slice: x: 2, y: 2, z: 4, core: 2. Of those that a mesh axis runs over, the one named last changes fastest.
Arguments:
- slide_region: float32 [16, 32, 8192], P('chan', ('groups', 'band')), parts along dimension 1, may hold values from -6 to 6
- row_taps: float32 [16, 257], P('chan'), may hold values from -0.375 to 0.375
- column_taps: float32 [16, 257], replicated, may hold values from -0.375 to 0.375
- channel_mix: float32 [16, 16], replicated, may hold values from -1.5 to 1.5
Outputs:
- filtered: float32 [16, 32, 8192], P('chan', ('groups', 'band')), parts along dimension 1
The draws below stay inside these ranges and needn't reach their ends.
There are 2 independent parts, one for each index of `groups`. The reference program is written for one: setup_inputs(seed, part) draws one part's arguments, and reference() takes and returns one part's arrays. A program takes and returns all parts, laid end to end along the dimension named above; an argument that names none is the same for every part. Nothing has to cross between parts.
All inputs are finite; a program needn't handle non-finite values.
Results may differ from the reference program's by a relative error of at most 0.00007.
Values sent between devices are 32-bit elements; how exact they have to be, the bound alone decides.
A program may use at most 64 MiB of HBM per device.

```python
import jax
import jax.numpy as jnp
from jax import lax

C = 16
TAPS = 257
COLS = 8192
ROWS = 16


def block_scale(own_key, shape, split, least, largest):
    loudness, own = 1.0, jax.random.fold_in(own_key, 6)
    for axis_at, shards_of in split:
        draws = jnp.exp(jax.random.uniform(jax.random.fold_in(own, axis_at), (shards_of,), jnp.float32, least / len(split), largest / len(split)))
        loudness = loudness * jnp.repeat(draws, shape[axis_at] // shards_of).reshape([-1 if axis == axis_at else 1 for axis in range(len(shape))])
    return loudness


def scatter_about(own_key, shape, spread, reach, shards=(), dtype=jnp.bfloat16):
    loudness = block_scale(own_key, shape, shards, -0.22, 0.18) if shards else 1.0
    drawn = jax.random.normal(own_key, shape, jnp.float32) * spread * loudness
    return jnp.minimum(jnp.maximum(drawn, -reach), reach).astype(dtype)


def setup_inputs(seed: int = 0, part: int = 0) -> dict:
    arg_keys = jax.random.split(jax.random.key(seed), 5)
    part_splits = jax.random.split(jax.random.fold_in(arg_keys[4], part), 5)
    slide_region = scatter_about(part_splits[0], (C, ROWS, COLS), 1.0, 6.0, ((0, 4), (1, 4)), jnp.float32)
    row_taps = scatter_about(arg_keys[1], (C, TAPS), TAPS ** -0.5, 0.375, ((0, 4),), jnp.float32)
    column_taps = scatter_about(arg_keys[2], (C, TAPS), TAPS ** -0.5, 0.375, (), jnp.float32)
    channel_mix = scatter_about(arg_keys[3], (C, C), C ** -0.5, 1.5, (), jnp.float32)
    return dict(slide_region=slide_region, row_taps=row_taps, column_taps=column_taps, channel_mix=channel_mix)


def depthwise(signal, filter_taps, horizontal):
    channels = signal.shape[0]
    margin = (filter_taps.shape[1] - 1) // 2
    if horizontal:
        kernel = filter_taps[:, None, None, :]
        padding = ((0, 0), (margin, margin))
    else:
        kernel = filter_taps[:, None, :, None]
        padding = ((margin, margin), (0, 0))
    result = lax.conv_general_dilated(signal[None], kernel, (1, 1), padding,
                                      dimension_numbers=("NCHW", "OIHW", "NCHW"),
                                      feature_group_count=channels,
                                      precision=lax.Precision.HIGHEST)
    return result[0]


def reference(slide_region, row_taps, column_taps, channel_mix):
    across = depthwise(slide_region, row_taps, True)
    vertical = depthwise(across, column_taps, False)
    return jnp.einsum("oc,chw->ohw", channel_mix, vertical, precision=lax.Precision.HIGHEST)
```

```python
import functools

import jax
import jax.numpy as jnp
from jax import lax
from jax.experimental import pallas as pl
from jax.experimental.pallas import tpu as pltpu
from jax.sharding import PartitionSpec as P

precise = lax.Precision.HIGHEST


def band_tables(filter_taps, tile_size):
    channels, length = filter_taps.shape
    margin = (length - 1) // 2
    period = 4 * tile_size
    border = 3 * tile_size + length
    widened = jnp.pad(filter_taps, ((0, 0), (border, border)))
    lowest = margin - tile_size + border
    window = widened[:, lowest : lowest + 3 * tile_size]
    vector = jnp.pad(window, ((0, 0), (0, tile_size)))
    repeated = jnp.tile(vector, (1, tile_size))[:, : tile_size * (period - 1)]
    toeplitz = repeated.reshape(channels, tile_size, period - 1)[:, :, : 3 * tile_size]
    stacked = jnp.transpose(toeplitz, (0, 2, 1))
    return stacked.reshape(channels, 3, tile_size, tile_size)


def along_columns(signal, filter_taps):
    tile_size = 128
    tables = band_tables(filter_taps, tile_size)
    channels, row_count, col_count = signal.shape
    tile_count = col_count // tile_size
    tiled = signal.reshape(channels, row_count, tile_count, tile_size)
    padded = jnp.pad(tiled, ((0, 0), (0, 0), (1, 1), (0, 0)))
    result = jnp.einsum(
        "crti,cij->crtj", padded[:, :, 0:tile_count], tables[:, 0], precision=precise
    )
    result = result + jnp.einsum(
        "crti,cij->crtj", padded[:, :, 1 : tile_count + 1], tables[:, 1], precision=precise
    )
    result = result + jnp.einsum(
        "crti,cij->crtj", padded[:, :, 2:], tables[:, 2], precision=precise
    )
    return result.reshape(channels, row_count, col_count)


def along_rows(signal, filter_taps):
    channels, row_count, col_count = signal.shape
    tile_size = 128 if row_count % 128 == 0 else row_count
    tables = band_tables(filter_taps, tile_size)
    tile_count = row_count // tile_size
    tiled = signal.reshape(channels, tile_count, tile_size, col_count)
    padded = jnp.pad(tiled, ((0, 0), (1, 1), (0, 0), (0, 0)))
    result = jnp.einsum("ctiw,cij->ctjw", padded[:, 0:tile_count], tables[:, 0], precision=precise)
    result = result + jnp.einsum(
        "ctiw,cij->ctjw", padded[:, 1 : tile_count + 1], tables[:, 1], precision=precise
    )
    result = result + jnp.einsum("ctiw,cij->ctjw", padded[:, 2:], tables[:, 2], precision=precise)
    return result.reshape(channels, row_count, col_count)


def on_device(slide_region, row_taps, column_taps, channel_mix):
    local_channels = slide_region.shape[0]
    across = along_columns(slide_region, row_taps)
    column_band = lax.all_to_all(across, "band", split_axis=2, concat_axis=1, tiled=True)
    first_channel = lax.axis_index("chan") * local_channels
    own_taps = lax.dynamic_slice_in_dim(column_taps, first_channel, local_channels, 0)
    vertical = along_rows(column_band, own_taps)
    own_mixing = lax.dynamic_slice_in_dim(channel_mix, first_channel, local_channels, 0)
    blended = jnp.einsum(
        "oc,chw->ohw",
        own_mixing,
        lax.all_gather(vertical, "chan", axis=0, tiled=True),
        precision=precise,
    )
    return lax.all_to_all(blended, "band", split_axis=1, concat_axis=2, tiled=True)


LANES = 128
CHUNKS = 2


def split(value):
    high = value.astype(jnp.bfloat16)
    return high, (value - high.astype(jnp.float32)).astype(jnp.bfloat16)


def product(left, right, dims):
    (left_high, left_low), (right_high, right_low) = left, right
    dot = functools.partial(
        lax.dot_general, dimension_numbers=(dims, ((), ())), preferred_element_type=jnp.float32
    )
    return dot(left_high, right_high) + (dot(left_low, right_high) + dot(left_high, right_low))


def filter_table(taps):
    shape = (LANES, LANES)
    lane = lax.broadcasted_iota(jnp.int32, shape, 1)
    row = lax.broadcasted_iota(jnp.int32, shape, 0)
    first, second = (
        pltpu.roll(
            jnp.broadcast_to(taps[:, at : at + LANES], shape), 0, 1, stride=1, stride_axis=0
        )
        for at in (0, LANES)
    )
    last = jnp.broadcast_to(taps[:, 2 * LANES :], shape)
    zero = jnp.zeros(shape, jnp.float32)
    return jnp.concatenate(
        [
            jnp.where(lane >= row, first, zero),
            jnp.where(lane >= row, second, first),
            jnp.where(lane == row, last, jnp.where(lane < row, second, zero)),
        ],
        axis=1,
    )


def mixing_table(column_taps, channel_mix, chans, bands, local_channels, local_rows):
    channels = chans * local_channels
    height = bands * local_rows
    block = local_channels * local_rows
    size = chans * bands * block
    margin = (column_taps.shape[1] - 1) // 2

    def coordinates(index):
        device, inner = index // block, index % block
        return (
            local_channels * (device % chans) + inner // local_rows,
            local_rows * (device // chans) + inner % local_rows,
        )

    tall = (size, channels)
    wide = (channels, size)
    pick_tall = (
        coordinates(lax.broadcasted_iota(jnp.int32, tall, 0))[0]
        == lax.broadcasted_iota(jnp.int32, tall, 1)
    ).astype(jnp.float32)
    pick_wide = (
        coordinates(lax.broadcasted_iota(jnp.int32, wide, 1))[0]
        == lax.broadcasted_iota(jnp.int32, wide, 0)
    ).astype(jnp.float32)
    weights = jnp.dot(
        jnp.dot(pick_tall, channel_mix, precision=precise), pick_wide, precision=precise
    )
    taps = lax.dot_general(
        column_taps[:, : 2 * margin],
        pick_wide,
        (((0,), (0,)), ((), ())),
        precision=precise,
    )
    square = (size, size)
    apart = (
        coordinates(lax.broadcasted_iota(jnp.int32, square, 1))[1]
        - coordinates(lax.broadcasted_iota(jnp.int32, square, 0))[1]
    )
    spread = jnp.zeros(square, jnp.float32)
    for distance in range(1 - height, height):
        at = margin + distance
        spread = jnp.where(apart == distance, taps[at : at + 1, :], spread)
    return weights * spread


def fused_kernel(
    chans, bands, x_hbm, row_hbm, column_hbm, mix_hbm, out_ref,
    x_buf, row_taps, column_taps, channel_mix, tables,
    send_one, recv_one, send_two, mixing,
    ready, x_sem, row_sem, small_sem, send_sem, recv_one_sem, recv_two_sem,
):
    local_channels, x_rows, _ = x_hbm.shape
    devices, _, block_rows, _ = send_two.shape
    tiles = send_one.shape[1]
    local_rows = block_rows // tiles
    band_rows = x_rows // bands
    others = pl.ds(0, devices - 1)
    chan, band = lax.axis_index("chan"), lax.axis_index("band")
    me = band * chans + chan
    half = bands // 2
    left = band < half

    row_load = pltpu.make_async_copy(row_hbm, row_taps, row_sem)
    row_load.start()
    x_inside = x_buf.at[:, pl.ds(8, x_rows)]
    for c in range(local_channels):
        pltpu.make_async_copy(x_hbm.at[c], x_inside.at[c], x_sem).start()

    far = [jnp.where(left, half + k, half - 1 - k) for k in range(half)]
    near = [jnp.where(left, 0, half) + (band + k) % half for k in range(1, half)]

    def peers(to_band, own):
        return [
            ({"chan": chan ^ step, "band": to_band}, to_band * chans + (chan ^ step))
            for step in range(1 if own else 0, chans)
        ]

    targets = [(to, peers(to, False)) for to in far + near] + [(band, peers(band, True))]

    barrier = pltpu.get_barrier_semaphore()
    greet = functools.partial(
        pl.semaphore_signal, inc=1, device_id_type=pl.DeviceIdType.MESH
    )

    def greet_all(semaphore, upward):
        for to, names in targets[:-1]:

            @pl.when((to > band) if upward else (to < band))
            def _():
                for name, _slot in names:
                    greet(semaphore, device_id=name)

        for name, slot in targets[-1][1]:

            @pl.when((slot > me) if upward else (slot < me))
            def _():
                greet(semaphore, device_id=name)

    greet_all(barrier, True)
    small_loads = [
        pltpu.make_async_copy(column_hbm, column_taps, small_sem.at[0]),
        pltpu.make_async_copy(mix_hbm, channel_mix, small_sem.at[1]),
    ]
    for load in small_loads:
        load.start()

    edge = jnp.zeros((8, LANES), jnp.float32)
    for c in range(local_channels):
        x_buf[c, 0:8, :] = edge
        x_buf[c, x_rows + 8 : x_rows + 16, :] = edge

    @pl.when(me > 0)
    def _():
        pl.semaphore_wait(barrier, me)

    greet_all(ready.at[band], False)

    row_load.wait()
    for c in range(local_channels):
        tables[c, 0], tables[c, 1] = split(filter_table(row_taps[c : c + 1, :]))
    pltpu.make_async_copy(x_hbm, x_inside, x_sem).wait()

    def filter_band(which):
        start = pl.multiple_of(which * band_rows, 8)
        for c in range(local_channels):
            wide = x_buf[c, pl.ds(start, band_rows + 16), :]
            window = jnp.concatenate(
                [
                    wide[8 + (k - 1) * local_rows : 8 + (k - 1) * local_rows + band_rows]
                    for k in range(3)
                ],
                axis=1,
            )
            filtered = product(split(window), (tables[c, 0], tables[c, 1]), ((1,), (1,)))
            for device in range(chans):
                for tile in range(tiles):
                    at = (device * tiles + tile) * local_rows
                    send_one[
                        which * chans + device,
                        tile,
                        c * local_rows : (c + 1) * local_rows,
                        :,
                    ] = filtered[at : at + local_rows, :]

    step = tiles // CHUNKS

    def copy_one(chunk, name, slot):
        part = pl.ds(chunk * step, step)
        return pltpu.make_async_remote_copy(
            src_ref=send_one.at[slot, part],
            dst_ref=recv_one.at[part, me],
            send_sem=send_sem.at[0],
            recv_sem=recv_one_sem.at[chunk],
            device_id=name,
            device_id_type=pl.DeviceIdType.MESH,
        )

    for to, names in targets:
        own = to is band
        filter_band(to)
        above = (chans - 1 - chan) if own else chans

        @pl.when((above > 0) if own else (to > band))
        def _():
            pl.semaphore_wait(ready.at[to], above)

        for name, slot in names:
            copy_one(0, name, slot).start()
    for chunk in range(1, CHUNKS):
        for to, names in targets:
            for name, slot in names:
                copy_one(chunk, name, slot).start()
    recv_one[:, me] = send_one[me]

    for load in small_loads:
        load.wait()
    table = mixing_table(
        column_taps[...], channel_mix[...], chans, bands, local_channels, local_rows
    )
    mixing[0], mixing[1] = split(table)

    rows = step * local_rows

    def copy_two(chunk, name, slot):
        return pltpu.make_async_remote_copy(
            src_ref=send_two.at[slot, :, pl.ds(chunk * rows, rows)],
            dst_ref=out_ref.at[
                :, pl.ds(pl.multiple_of(me * block_rows + chunk * rows, 8), rows)
            ],
            send_sem=send_sem.at[1],
            recv_sem=recv_two_sem,
            device_id=name,
            device_id_type=pl.DeviceIdType.MESH,
        )

    for chunk in range(CHUNKS):
        part = pl.ds(chunk * step, step)
        landed = recv_one.at[part, others]
        pltpu.make_async_copy(landed, landed, recv_one_sem.at[chunk]).wait()
        columns = jnp.concatenate(
            [
                recv_one[chunk * step + tile].reshape(mixing.shape[1], LANES)
                for tile in range(step)
            ],
            axis=1,
        )
        mixed = product((mixing[0], mixing[1]), split(columns), ((1,), (0,)))
        for device in range(devices):
            for c in range(local_channels):
                at = (device * local_channels + c) * local_rows
                for tile in range(step):
                    to = (chunk * step + tile) * local_rows
                    send_two[device, c, to : to + local_rows, :] = mixed[
                        at : at + local_rows, tile * LANES : (tile + 1) * LANES
                    ]
        there = pl.ds(pl.multiple_of(me * block_rows + chunk * rows, 8), rows)
        for _to, names in targets:
            for name, slot in names:
                copy_two(chunk, name, slot).start()
        out_ref[:, there, :] = send_two[me, :, chunk * rows : (chunk + 1) * rows, :]

    sent = send_one.at[others]
    pltpu.make_async_copy(sent, sent, send_sem.at[0]).wait()
    sent = send_two.at[others]
    pltpu.make_async_copy(sent, sent, send_sem.at[1]).wait()
    landed = out_ref.at[:, pl.ds(0, (devices - 1) * block_rows)]
    pltpu.make_async_copy(landed, landed, recv_two_sem).wait()


def fused(chans, bands, slide_region, row_taps, column_taps, channel_mix):
    local_channels, local_rows, width = slide_region.shape
    devices = chans * bands
    total_tiles = width // LANES
    tiles = total_tiles // devices
    block = local_channels * local_rows
    tiled = slide_region.reshape(local_channels, local_rows, total_tiles, LANES)
    tiled = tiled.transpose(0, 2, 1, 3).reshape(local_channels, total_tiles * local_rows, LANES)
    vmem = pl.BlockSpec(memory_space=pltpu.VMEM)
    anywhere = pl.BlockSpec(memory_space=pl.ANY)
    dma = pltpu.SemaphoreType.DMA
    out = pl.pallas_call(
        functools.partial(fused_kernel, chans, bands),
        out_shape=pltpu.VMEM(tiled.shape, jnp.float32),
        in_specs=[anywhere] * 4,
        out_specs=vmem,
        scratch_shapes=[
            pltpu.VMEM((local_channels, tiled.shape[1] + 16, LANES), jnp.float32),
            pltpu.VMEM(row_taps.shape, jnp.float32),
            pltpu.VMEM(column_taps.shape, jnp.float32),
            pltpu.VMEM(channel_mix.shape, jnp.float32),
            pltpu.VMEM((local_channels, 2, LANES, 3 * LANES), jnp.bfloat16),
            pltpu.VMEM((devices, tiles, block, LANES), jnp.float32),
            pltpu.VMEM((tiles, devices, block, LANES), jnp.float32),
            pltpu.VMEM((devices, local_channels, tiles * local_rows, LANES), jnp.float32),
            pltpu.VMEM((2, devices * block, devices * block), jnp.bfloat16),
            pltpu.SemaphoreType.REGULAR((bands,)),
            dma,
            dma,
            dma((2,)),
            dma((2,)),
            dma((CHUNKS,)),
            dma,
        ],
        compiler_params=pltpu.CompilerParams(collective_id=0, has_side_effects=True),
    )(tiled, row_taps, column_taps, channel_mix)
    out = out.reshape(local_channels, total_tiles, local_rows, LANES)
    return out.transpose(0, 2, 1, 3).reshape(slide_region.shape)


def power_of_two(number):
    return number & (number - 1) == 0


def program(chans, bands, slide_region, row_taps, column_taps, channel_mix):
    local_channels, local_rows, width = slide_region.shape
    devices = chans * bands
    margin = (row_taps.shape[1] - 1) // 2
    fits = (
        power_of_two(chans)
        and power_of_two(bands)
        and bands > 1
        and width % (devices * LANES * CHUNKS) == 0
        and margin == LANES
        and column_taps.shape[1] == row_taps.shape[1]
        and local_rows == 4
        and local_rows * bands <= margin
        and local_channels * local_rows % 8 == 0
        and width // (devices * LANES * CHUNKS) * local_rows % 8 == 0
        and devices * local_channels * local_rows <= 512
    )
    if fits:
        return fused(chans, bands, slide_region, row_taps, column_taps, channel_mix)
    return on_device(slide_region, row_taps, column_taps, channel_mix)


def solution(mesh):
    in_specs = (P("chan", ("groups", "band"), None), P("chan", None), P(), P())
    out_specs = P("chan", ("groups", "band"), None)
    return jax.shard_map(
        functools.partial(program, mesh.shape["chan"], mesh.shape["band"]),
        mesh=mesh,
        in_specs=in_specs,
        out_specs=out_specs,
        check_vma=False,
    )
```

```python
import functools

import jax
import jax.numpy as jnp
from jax import lax
from jax.experimental import pallas as pl
from jax.experimental.pallas import tpu as pltpu
from jax.sharding import PartitionSpec as P

precise = lax.Precision.HIGHEST


def band_tables(filter_taps, tile_size):
    channels, length = filter_taps.shape
    margin = (length - 1) // 2
    period = 4 * tile_size
    border = 3 * tile_size + length
    widened = jnp.pad(filter_taps, ((0, 0), (border, border)))
    lowest = margin - tile_size + border
    window = widened[:, lowest : lowest + 3 * tile_size]
    vector = jnp.pad(window, ((0, 0), (0, tile_size)))
    repeated = jnp.tile(vector, (1, tile_size))[:, : tile_size * (period - 1)]
    toeplitz = repeated.reshape(channels, tile_size, period - 1)[:, :, : 3 * tile_size]
    stacked = jnp.transpose(toeplitz, (0, 2, 1))
    return stacked.reshape(channels, 3, tile_size, tile_size)


def along_columns(signal, filter_taps):
    tile_size = 128
    tables = band_tables(filter_taps, tile_size)
    channels, row_count, col_count = signal.shape
    tile_count = col_count // tile_size
    tiled = signal.reshape(channels, row_count, tile_count, tile_size)
    padded = jnp.pad(tiled, ((0, 0), (0, 0), (1, 1), (0, 0)))
    result = jnp.einsum(
        "crti,cij->crtj", padded[:, :, 0:tile_count], tables[:, 0], precision=precise
    )
    result = result + jnp.einsum(
        "crti,cij->crtj", padded[:, :, 1 : tile_count + 1], tables[:, 1], precision=precise
    )
    result = result + jnp.einsum(
        "crti,cij->crtj", padded[:, :, 2:], tables[:, 2], precision=precise
    )
    return result.reshape(channels, row_count, col_count)


def along_rows(signal, filter_taps):
    channels, row_count, col_count = signal.shape
    tile_size = 128 if row_count % 128 == 0 else row_count
    tables = band_tables(filter_taps, tile_size)
    tile_count = row_count // tile_size
    tiled = signal.reshape(channels, tile_count, tile_size, col_count)
    padded = jnp.pad(tiled, ((0, 0), (1, 1), (0, 0), (0, 0)))
    result = jnp.einsum("ctiw,cij->ctjw", padded[:, 0:tile_count], tables[:, 0], precision=precise)
    result = result + jnp.einsum(
        "ctiw,cij->ctjw", padded[:, 1 : tile_count + 1], tables[:, 1], precision=precise
    )
    result = result + jnp.einsum("ctiw,cij->ctjw", padded[:, 2:], tables[:, 2], precision=precise)
    return result.reshape(channels, row_count, col_count)


def on_device(slide_region, row_taps, column_taps, channel_mix):
    local_channels = slide_region.shape[0]
    across = along_columns(slide_region, row_taps)
    column_band = lax.all_to_all(across, "band", split_axis=2, concat_axis=1, tiled=True)
    first_channel = lax.axis_index("chan") * local_channels
    own_taps = lax.dynamic_slice_in_dim(column_taps, first_channel, local_channels, 0)
    vertical = along_rows(column_band, own_taps)
    own_mixing = lax.dynamic_slice_in_dim(channel_mix, first_channel, local_channels, 0)
    blended = jnp.einsum(
        "oc,chw->ohw",
        own_mixing,
        lax.all_gather(vertical, "chan", axis=0, tiled=True),
        precision=precise,
    )
    return lax.all_to_all(blended, "band", split_axis=1, concat_axis=2, tiled=True)


LANES = 128
CHUNKS = 2


def split(value):
    high = value.astype(jnp.bfloat16)
    return high, (value - high.astype(jnp.float32)).astype(jnp.bfloat16)


def product(left, right, dims):
    (left_high, left_low), (right_high, right_low) = left, right
    dot = functools.partial(
        lax.dot_general, dimension_numbers=(dims, ((), ())), preferred_element_type=jnp.float32
    )
    return dot(left_high, right_high) + (dot(left_low, right_high) + dot(left_high, right_low))


def filter_table(taps):
    shape = (LANES, LANES)
    lane = lax.broadcasted_iota(jnp.int32, shape, 1)
    row = lax.broadcasted_iota(jnp.int32, shape, 0)
    first, second = (
        pltpu.roll(
            jnp.broadcast_to(taps[:, at : at + LANES], shape), 0, 1, stride=1, stride_axis=0
        )
        for at in (0, LANES)
    )
    last = jnp.broadcast_to(taps[:, 2 * LANES :], shape)
    zero = jnp.zeros(shape, jnp.float32)
    return jnp.concatenate(
        [
            jnp.where(lane >= row, first, zero),
            jnp.where(lane >= row, second, first),
            jnp.where(lane == row, last, jnp.where(lane < row, second, zero)),
        ],
        axis=1,
    )


def mixing_table(column_taps, channel_mix, chans, bands, local_channels, local_rows):
    channels = chans * local_channels
    height = bands * local_rows
    block = local_channels * local_rows
    size = chans * bands * block
    margin = (column_taps.shape[1] - 1) // 2

    def coordinates(index):
        device, inner = index // block, index % block
        return (
            local_channels * (device % chans) + inner // local_rows,
            local_rows * (device // chans) + inner % local_rows,
        )

    tall = (size, channels)
    wide = (channels, size)
    pick_tall = (
        coordinates(lax.broadcasted_iota(jnp.int32, tall, 0))[0]
        == lax.broadcasted_iota(jnp.int32, tall, 1)
    ).astype(jnp.float32)
    pick_wide = (
        coordinates(lax.broadcasted_iota(jnp.int32, wide, 1))[0]
        == lax.broadcasted_iota(jnp.int32, wide, 0)
    ).astype(jnp.float32)
    weights = jnp.dot(
        jnp.dot(pick_tall, channel_mix, precision=precise), pick_wide, precision=precise
    )
    taps = lax.dot_general(
        column_taps[:, : 2 * margin],
        pick_wide,
        (((0,), (0,)), ((), ())),
        precision=precise,
    )
    square = (size, size)
    apart = (
        coordinates(lax.broadcasted_iota(jnp.int32, square, 1))[1]
        - coordinates(lax.broadcasted_iota(jnp.int32, square, 0))[1]
    )
    spread = jnp.zeros(square, jnp.float32)
    for distance in range(1 - height, height):
        at = margin + distance
        spread = jnp.where(apart == distance, taps[at : at + 1, :], spread)
    return weights * spread


def fused_kernel(
    chans, bands, x_hbm, row_hbm, column_hbm, mix_hbm, out_ref,
    x_buf, row_taps, column_taps, channel_mix, tables,
    send_one, recv_one, send_two, mixing,
    ready, x_sem, row_sem, small_sem, send_sem, recv_one_sem, recv_two_sem,
):
    local_channels, x_rows, _ = x_hbm.shape
    devices, _, block_rows, _ = send_two.shape
    tiles = send_one.shape[1]
    local_rows = block_rows // tiles
    band_rows = x_rows // bands
    others = pl.ds(0, devices - 1)
    chan, band = lax.axis_index("chan"), lax.axis_index("band")
    me = band * chans + chan
    half = bands // 2
    left = band < half

    row_load = pltpu.make_async_copy(row_hbm, row_taps, row_sem)
    row_load.start()
    x_inside = x_buf.at[:, pl.ds(8, x_rows)]
    for c in range(local_channels):
        pltpu.make_async_copy(x_hbm.at[c], x_inside.at[c], x_sem).start()

    far = [jnp.where(left, half + k, half - 1 - k) for k in range(half)]
    near = [jnp.where(left, 0, half) + (band + k) % half for k in range(1, half)]

    def peers(to_band, own):
        return [
            ({"chan": chan ^ step, "band": to_band}, to_band * chans + (chan ^ step))
            for step in range(1 if own else 0, chans)
        ]

    targets = [(to, peers(to, False)) for to in far + near] + [(band, peers(band, True))]
    rising = [(to, peers(to, False)) for to in (jnp.where(left, half + k, k) for k in range(half))]

    barrier = pltpu.get_barrier_semaphore()
    greet = functools.partial(
        pl.semaphore_signal, inc=1, device_id_type=pl.DeviceIdType.MESH
    )

    def greet_all(semaphore, upward):
        for to, names in targets[:-1]:

            @pl.when((to > band) if upward else (to < band))
            def _():
                for name, _slot in names:
                    greet(semaphore, device_id=name)

        for name, slot in targets[-1][1]:

            @pl.when((slot > me) if upward else (slot < me))
            def _():
                greet(semaphore, device_id=name)

    greet_all(barrier, True)
    small_loads = [
        pltpu.make_async_copy(column_hbm, column_taps, small_sem.at[0]),
        pltpu.make_async_copy(mix_hbm, channel_mix, small_sem.at[1]),
    ]
    for load in small_loads:
        load.start()

    edge = jnp.zeros((8, LANES), jnp.float32)
    for c in range(local_channels):
        x_buf[c, 0:8, :] = edge
        x_buf[c, x_rows + 8 : x_rows + 16, :] = edge

    @pl.when(me > 0)
    def _():
        pl.semaphore_wait(barrier, me)

    greet_all(ready.at[band], False)

    row_load.wait()
    for c in range(local_channels):
        tables[c, 0:LANES], tables[c, LANES:] = split(filter_table(row_taps[c : c + 1, :]))
    pltpu.make_async_copy(x_hbm, x_inside, x_sem).wait()

    def filter_band(which):
        start = pl.multiple_of(which * band_rows, 8)
        for c in range(local_channels):
            wide = x_buf[c, pl.ds(start, band_rows + 16), :]
            window = jnp.concatenate(
                [
                    wide[8 + (k - 1) * local_rows : 8 + (k - 1) * local_rows + band_rows]
                    for k in range(3)
                ],
                axis=1,
            )
            both = lax.dot_general(
                jnp.concatenate(split(window), axis=0),
                tables[c],
                (((1,), (1,)), ((), ())),
                preferred_element_type=jnp.float32,
            )
            filtered = both[:band_rows, :LANES] + (
                both[band_rows:, :LANES] + both[:band_rows, LANES:]
            )
            for device in range(chans):
                for tile in range(tiles):
                    at = (device * tiles + tile) * local_rows
                    send_one[
                        which * chans + device,
                        tile,
                        c * local_rows : (c + 1) * local_rows,
                        :,
                    ] = filtered[at : at + local_rows, :]

    step = tiles // CHUNKS

    def copy_one(chunk, name, slot):
        part = pl.ds(chunk * step, step)
        return pltpu.make_async_remote_copy(
            src_ref=send_one.at[slot, part],
            dst_ref=recv_one.at[part, me],
            send_sem=send_sem.at[0],
            recv_sem=recv_one_sem.at[chunk],
            device_id=name,
            device_id_type=pl.DeviceIdType.MESH,
        )

    for to, names in targets:
        own = to is band
        filter_band(to)
        above = (chans - 1 - chan) if own else chans

        @pl.when((above > 0) if own else (to > band))
        def _():
            pl.semaphore_wait(ready.at[to], above)

        for name, slot in names:
            copy_one(0, name, slot).start()
    for chunk in range(1, CHUNKS):
        for to, names in targets:
            for name, slot in names:
                copy_one(chunk, name, slot).start()
    recv_one[:, me] = send_one[me]

    for load in small_loads:
        load.wait()
    table = mixing_table(
        column_taps[...], channel_mix[...], chans, bands, local_channels, local_rows
    )
    mixing[0], mixing[1] = split(table)

    rows = step * local_rows

    def copy_two(chunk, name, slot):
        return pltpu.make_async_remote_copy(
            src_ref=send_two.at[slot, :, pl.ds(chunk * rows, rows)],
            dst_ref=out_ref.at[
                :, pl.ds(pl.multiple_of(me * block_rows + chunk * rows, 8), rows)
            ],
            send_sem=send_sem.at[1],
            recv_sem=recv_two_sem,
            device_id=name,
            device_id_type=pl.DeviceIdType.MESH,
        )

    late = band == half

    def send_rising(chunk):
        last = chunk == CHUNKS - 1
        for at, (_to, names) in enumerate(rising):
            if at == 0:
                for name, slot in names:
                    copy_two(chunk, name, slot).start()
                continue
            if last:
                @pl.when(late)
                def _():
                    for earlier in range(CHUNKS - 1):
                        for name, slot in names[1:4]:
                            copy_two(earlier, name, slot).start()

                for name, slot in names:
                    copy_two(chunk, name, slot).start()
            else:
                for name, slot in names[:1] + names[4:]:
                    copy_two(chunk, name, slot).start()

                @pl.when(jnp.logical_not(late))
                def _():
                    for name, slot in names[1:4]:
                        copy_two(chunk, name, slot).start()

    for chunk in range(CHUNKS):
        part = pl.ds(chunk * step, step)
        landed = recv_one.at[part, others]
        pltpu.make_async_copy(landed, landed, recv_one_sem.at[chunk]).wait()
        columns = jnp.concatenate(
            [
                recv_one[chunk * step + tile].reshape(mixing.shape[1], LANES)
                for tile in range(step)
            ],
            axis=1,
        )
        mixed = product((mixing[0], mixing[1]), split(columns), ((1,), (0,)))
        for device in range(devices):
            for c in range(local_channels):
                at = (device * local_channels + c) * local_rows
                for tile in range(step):
                    to = (chunk * step + tile) * local_rows
                    send_two[device, c, to : to + local_rows, :] = mixed[
                        at : at + local_rows, tile * LANES : (tile + 1) * LANES
                    ]
        there = pl.ds(pl.multiple_of(me * block_rows + chunk * rows, 8), rows)
        send_rising(chunk)
        for _to, names in targets[half:]:
            for name, slot in names:
                copy_two(chunk, name, slot).start()
        out_ref[:, there, :] = send_two[me, :, chunk * rows : (chunk + 1) * rows, :]

    sent = send_one.at[others]
    pltpu.make_async_copy(sent, sent, send_sem.at[0]).wait()
    sent = send_two.at[others]
    pltpu.make_async_copy(sent, sent, send_sem.at[1]).wait()
    landed = out_ref.at[:, pl.ds(0, (devices - 1) * block_rows)]
    pltpu.make_async_copy(landed, landed, recv_two_sem).wait()


def fused(chans, bands, slide_region, row_taps, column_taps, channel_mix):
    local_channels, local_rows, width = slide_region.shape
    devices = chans * bands
    total_tiles = width // LANES
    tiles = total_tiles // devices
    block = local_channels * local_rows
    tiled = slide_region.reshape(local_channels, local_rows, total_tiles, LANES)
    tiled = tiled.transpose(0, 2, 1, 3).reshape(local_channels, total_tiles * local_rows, LANES)
    vmem = pl.BlockSpec(memory_space=pltpu.VMEM)
    anywhere = pl.BlockSpec(memory_space=pl.ANY)
    dma = pltpu.SemaphoreType.DMA
    out = pl.pallas_call(
        functools.partial(fused_kernel, chans, bands),
        out_shape=pltpu.VMEM(tiled.shape, jnp.float32),
        in_specs=[anywhere] * 4,
        out_specs=vmem,
        scratch_shapes=[
            pltpu.VMEM((local_channels, tiled.shape[1] + 16, LANES), jnp.float32),
            pltpu.VMEM(row_taps.shape, jnp.float32),
            pltpu.VMEM(column_taps.shape, jnp.float32),
            pltpu.VMEM(channel_mix.shape, jnp.float32),
            pltpu.VMEM((local_channels, 2 * LANES, 3 * LANES), jnp.bfloat16),
            pltpu.VMEM((devices, tiles, block, LANES), jnp.float32),
            pltpu.VMEM((tiles, devices, block, LANES), jnp.float32),
            pltpu.VMEM((devices, local_channels, tiles * local_rows, LANES), jnp.float32),
            pltpu.VMEM((2, devices * block, devices * block), jnp.bfloat16),
            pltpu.SemaphoreType.REGULAR((bands,)),
            dma,
            dma,
            dma((2,)),
            dma((2,)),
            dma((CHUNKS,)),
            dma,
        ],
        compiler_params=pltpu.CompilerParams(collective_id=0, has_side_effects=True),
    )(tiled, row_taps, column_taps, channel_mix)
    out = out.reshape(local_channels, total_tiles, local_rows, LANES)
    return out.transpose(0, 2, 1, 3).reshape(slide_region.shape)


def power_of_two(number):
    return number & (number - 1) == 0


def program(chans, bands, slide_region, row_taps, column_taps, channel_mix):
    local_channels, local_rows, width = slide_region.shape
    devices = chans * bands
    margin = (row_taps.shape[1] - 1) // 2
    fits = (
        power_of_two(chans)
        and power_of_two(bands)
        and bands > 1
        and width % (devices * LANES * CHUNKS) == 0
        and margin == LANES
        and column_taps.shape[1] == row_taps.shape[1]
        and local_rows == 4
        and local_rows * bands <= margin
        and local_channels * local_rows % 8 == 0
        and width // (devices * LANES * CHUNKS) * local_rows % 8 == 0
        and devices * local_channels * local_rows <= 512
    )
    if fits:
        return fused(chans, bands, slide_region, row_taps, column_taps, channel_mix)
    return on_device(slide_region, row_taps, column_taps, channel_mix)


def solution(mesh):
    in_specs = (P("chan", ("groups", "band"), None), P("chan", None), P(), P())
    out_specs = P("chan", ("groups", "band"), None)
    return jax.shard_map(
        functools.partial(program, mesh.shape["chan"], mesh.shape["band"]),
        mesh=mesh,
        in_specs=in_specs,
        out_specs=out_specs,
        check_vma=False,
    )
```

```python
import functools

import jax
import jax.numpy as jnp
from jax import lax
from jax.experimental import pallas as pl
from jax.experimental.pallas import tpu as pltpu
from jax.sharding import PartitionSpec as P

precise = lax.Precision.HIGHEST


def band_tables(filter_taps, tile_size):
    channels, length = filter_taps.shape
    margin = (length - 1) // 2
    period = 4 * tile_size
    border = 3 * tile_size + length
    widened = jnp.pad(filter_taps, ((0, 0), (border, border)))
    lowest = margin - tile_size + border
    window = widened[:, lowest : lowest + 3 * tile_size]
    vector = jnp.pad(window, ((0, 0), (0, tile_size)))
    repeated = jnp.tile(vector, (1, tile_size))[:, : tile_size * (period - 1)]
    toeplitz = repeated.reshape(channels, tile_size, period - 1)[:, :, : 3 * tile_size]
    stacked = jnp.transpose(toeplitz, (0, 2, 1))
    return stacked.reshape(channels, 3, tile_size, tile_size)


def along_columns(signal, filter_taps):
    tile_size = 128
    tables = band_tables(filter_taps, tile_size)
    channels, row_count, col_count = signal.shape
    tile_count = col_count // tile_size
    tiled = signal.reshape(channels, row_count, tile_count, tile_size)
    padded = jnp.pad(tiled, ((0, 0), (0, 0), (1, 1), (0, 0)))
    result = jnp.einsum(
        "crti,cij->crtj", padded[:, :, 0:tile_count], tables[:, 0], precision=precise
    )
    result = result + jnp.einsum(
        "crti,cij->crtj", padded[:, :, 1 : tile_count + 1], tables[:, 1], precision=precise
    )
    result = result + jnp.einsum(
        "crti,cij->crtj", padded[:, :, 2:], tables[:, 2], precision=precise
    )
    return result.reshape(channels, row_count, col_count)


def along_rows(signal, filter_taps):
    channels, row_count, col_count = signal.shape
    tile_size = 128 if row_count % 128 == 0 else row_count
    tables = band_tables(filter_taps, tile_size)
    tile_count = row_count // tile_size
    tiled = signal.reshape(channels, tile_count, tile_size, col_count)
    padded = jnp.pad(tiled, ((0, 0), (1, 1), (0, 0), (0, 0)))
    result = jnp.einsum("ctiw,cij->ctjw", padded[:, 0:tile_count], tables[:, 0], precision=precise)
    result = result + jnp.einsum(
        "ctiw,cij->ctjw", padded[:, 1 : tile_count + 1], tables[:, 1], precision=precise
    )
    result = result + jnp.einsum("ctiw,cij->ctjw", padded[:, 2:], tables[:, 2], precision=precise)
    return result.reshape(channels, row_count, col_count)


def on_device(slide_region, row_taps, column_taps, channel_mix):
    local_channels = slide_region.shape[0]
    across = along_columns(slide_region, row_taps)
    column_band = lax.all_to_all(across, "band", split_axis=2, concat_axis=1, tiled=True)
    first_channel = lax.axis_index("chan") * local_channels
    own_taps = lax.dynamic_slice_in_dim(column_taps, first_channel, local_channels, 0)
    vertical = along_rows(column_band, own_taps)
    own_mixing = lax.dynamic_slice_in_dim(channel_mix, first_channel, local_channels, 0)
    blended = jnp.einsum(
        "oc,chw->ohw",
        own_mixing,
        lax.all_gather(vertical, "chan", axis=0, tiled=True),
        precision=precise,
    )
    return lax.all_to_all(blended, "band", split_axis=1, concat_axis=2, tiled=True)


LANES = 128
CHUNKS = 2


def split(value):
    high = value.astype(jnp.bfloat16)
    return high, (value - high.astype(jnp.float32)).astype(jnp.bfloat16)


def product(left, right, dims):
    (left_high, left_low), (right_high, right_low) = left, right
    dot = functools.partial(
        lax.dot_general, dimension_numbers=(dims, ((), ())), preferred_element_type=jnp.float32
    )
    return dot(left_high, right_high) + (dot(left_low, right_high) + dot(left_high, right_low))


def filter_table(taps):
    shape = (LANES, LANES)
    lane = lax.broadcasted_iota(jnp.int32, shape, 1)
    row = lax.broadcasted_iota(jnp.int32, shape, 0)
    first, second = (
        pltpu.roll(
            jnp.broadcast_to(taps[:, at : at + LANES], shape), 0, 1, stride=1, stride_axis=0
        )
        for at in (0, LANES)
    )
    last = jnp.broadcast_to(taps[:, 2 * LANES :], shape)
    zero = jnp.zeros(shape, jnp.float32)
    return jnp.concatenate(
        [
            jnp.where(lane >= row, first, zero),
            jnp.where(lane >= row, second, first),
            jnp.where(lane == row, last, jnp.where(lane < row, second, zero)),
        ],
        axis=1,
    )


def mixing_table(column_taps, channel_mix, chans, bands, local_channels, local_rows):
    channels = chans * local_channels
    height = bands * local_rows
    block = local_channels * local_rows
    size = chans * bands * block
    margin = (column_taps.shape[1] - 1) // 2

    def coordinates(index):
        device, inner = index // block, index % block
        return (
            local_channels * (device % chans) + inner // local_rows,
            local_rows * (device // chans) + inner % local_rows,
        )

    tall = (size, channels)
    wide = (channels, size)
    pick_tall = (
        coordinates(lax.broadcasted_iota(jnp.int32, tall, 0))[0]
        == lax.broadcasted_iota(jnp.int32, tall, 1)
    ).astype(jnp.float32)
    pick_wide = (
        coordinates(lax.broadcasted_iota(jnp.int32, wide, 1))[0]
        == lax.broadcasted_iota(jnp.int32, wide, 0)
    ).astype(jnp.float32)
    weights = jnp.dot(
        jnp.dot(pick_tall, channel_mix, precision=precise), pick_wide, precision=precise
    )
    taps = lax.dot_general(
        column_taps[:, : 2 * margin],
        pick_wide,
        (((0,), (0,)), ((), ())),
        precision=precise,
    )
    square = (size, size)
    apart = (
        coordinates(lax.broadcasted_iota(jnp.int32, square, 1))[1]
        - coordinates(lax.broadcasted_iota(jnp.int32, square, 0))[1]
    )
    spread = jnp.zeros(square, jnp.float32)
    for distance in range(1 - height, height):
        at = margin + distance
        spread = jnp.where(apart == distance, taps[at : at + 1, :], spread)
    return weights * spread


def fused_kernel(
    chans, bands, x_hbm, row_hbm, column_hbm, mix_hbm, out_ref,
    x_buf, row_taps, column_taps, channel_mix, tables,
    send_one, recv_one, send_two, mixing,
    ready, x_sem, row_sem, small_sem, send_sem, recv_one_sem, recv_two_sem,
):
    local_channels, x_rows, _ = x_hbm.shape
    devices, _, block_rows, _ = send_two.shape
    tiles = send_one.shape[1]
    local_rows = block_rows // tiles
    band_rows = x_rows // bands
    others = pl.ds(0, devices - 1)
    chan, band = lax.axis_index("chan"), lax.axis_index("band")
    me = band * chans + chan
    half = bands // 2
    left = band < half

    row_load = pltpu.make_async_copy(row_hbm, row_taps, row_sem)
    row_load.start()
    x_inside = x_buf.at[:, pl.ds(8, x_rows)]
    for c in range(local_channels):
        pltpu.make_async_copy(x_hbm.at[c], x_inside.at[c], x_sem).start()

    far = [jnp.where(left, half + k, half - 1 - k) for k in range(half)]
    near = [jnp.where(left, 0, half) + (band + k) % half for k in range(1, half)]

    def peers(to_band, own):
        return [
            ({"chan": chan ^ step, "band": to_band}, to_band * chans + (chan ^ step))
            for step in range(1 if own else 0, chans)
        ]

    targets = [(to, peers(to, False)) for to in far + near] + [(band, peers(band, True))]
    rising = [
        (to, [({"chan": jnp.int32(k), "band": to}, to * chans + k) for k in range(chans)])
        for to in (jnp.where(left, half + k, k) for k in range(half))
    ]

    barrier = pltpu.get_barrier_semaphore()
    greet = functools.partial(
        pl.semaphore_signal, inc=1, device_id_type=pl.DeviceIdType.MESH
    )

    def rank(which):
        return jnp.where(which < half, 2 * (half - 1 - which), 2 * (which - half) + 1)

    mine = rank(band)

    def greet_all(semaphore, upward):
        for to, names in targets[:-1]:

            @pl.when((rank(to) > mine) if upward else (rank(to) < mine))
            def _():
                for name, _slot in names:
                    greet(semaphore, device_id=name)

        for name, slot in targets[-1][1]:

            @pl.when((slot > me) if upward else (slot < me))
            def _():
                greet(semaphore, device_id=name)

    greet_all(barrier, True)
    small_loads = [
        pltpu.make_async_copy(column_hbm, column_taps, small_sem.at[0]),
        pltpu.make_async_copy(mix_hbm, channel_mix, small_sem.at[1]),
    ]
    for load in small_loads:
        load.start()

    edge = jnp.zeros((8, LANES), jnp.float32)
    for c in range(local_channels):
        x_buf[c, 0:8, :] = edge
        x_buf[c, x_rows + 8 : x_rows + 16, :] = edge

    def meet():
        below = mine * chans + chan

        @pl.when(below > 0)
        def _():
            pl.semaphore_wait(barrier, below)

        greet_all(ready.at[band], False)

    meet_first = jnp.logical_and(2 * chan >= chans, band > 0)
    pl.when(meet_first)(meet)

    row_load.wait()
    for c in range(local_channels):
        tables[c, 0:LANES], tables[c, LANES:] = split(filter_table(row_taps[c : c + 1, :]))
    pltpu.make_async_copy(x_hbm, x_inside, x_sem).wait()

    def filter_band(which):
        start = pl.multiple_of(which * band_rows, 8)
        for c in range(local_channels):
            wide = x_buf[c, pl.ds(start, band_rows + 16), :]
            window = jnp.concatenate(
                [
                    wide[8 + (k - 1) * local_rows : 8 + (k - 1) * local_rows + band_rows]
                    for k in range(3)
                ],
                axis=1,
            )
            both = lax.dot_general(
                jnp.concatenate(split(window), axis=0),
                tables[c],
                (((1,), (1,)), ((), ())),
                preferred_element_type=jnp.float32,
            )
            filtered = both[:band_rows, :LANES] + (
                both[band_rows:, :LANES] + both[:band_rows, LANES:]
            )
            for device in range(chans):
                for tile in range(tiles):
                    at = (device * tiles + tile) * local_rows
                    send_one[
                        which * chans + device,
                        tile,
                        c * local_rows : (c + 1) * local_rows,
                        :,
                    ] = filtered[at : at + local_rows, :]

    step = tiles // CHUNKS

    def copy_one(chunk, name, slot):
        part = pl.ds(chunk * step, step)
        return pltpu.make_async_remote_copy(
            src_ref=send_one.at[slot, part],
            dst_ref=recv_one.at[part, me],
            send_sem=send_sem.at[0],
            recv_sem=recv_one_sem.at[chunk],
            device_id=name,
            device_id_type=pl.DeviceIdType.MESH,
        )

    for to, names in targets:
        own = to is band
        filter_band(to)
        if to is targets[0][0]:
            pl.when(jnp.logical_not(meet_first))(meet)
        above = (chans - 1 - chan) if own else chans

        @pl.when((above > 0) if own else (rank(to) > mine))
        def _():
            pl.semaphore_wait(ready.at[to], above)

        for name, slot in names:
            copy_one(0, name, slot).start()
    for chunk in range(1, CHUNKS):
        for to, names in targets:
            for name, slot in names:
                copy_one(chunk, name, slot).start()
    recv_one[:, me] = send_one[me]

    for load in small_loads:
        load.wait()
    table = mixing_table(
        column_taps[...], channel_mix[...], chans, bands, local_channels, local_rows
    )
    mixing[0], mixing[1] = split(table)

    rows = step * local_rows

    def copy_two(chunk, name, slot):
        return pltpu.make_async_remote_copy(
            src_ref=send_two.at[slot, :, pl.ds(chunk * rows, rows)],
            dst_ref=out_ref.at[
                :, pl.ds(pl.multiple_of(me * block_rows + chunk * rows, 8), rows)
            ],
            send_sem=send_sem.at[1],
            recv_sem=recv_two_sem,
            device_id=name,
            device_id_type=pl.DeviceIdType.MESH,
        )

    late = band == half

    def send_rising(chunk):
        last = chunk == CHUNKS - 1
        for at, (_to, names) in enumerate(rising):
            if at == 0:
                for name, slot in names:
                    copy_two(chunk, name, slot).start()
                continue
            if last:
                @pl.when(late)
                def _():
                    for earlier in range(CHUNKS - 1):
                        for name, slot in names[1:4]:
                            copy_two(earlier, name, slot).start()

                for name, slot in names:
                    copy_two(chunk, name, slot).start()
            else:
                for name, slot in names[:1] + names[4:]:
                    copy_two(chunk, name, slot).start()

                @pl.when(jnp.logical_not(late))
                def _():
                    for name, slot in names[1:4]:
                        copy_two(chunk, name, slot).start()

    for chunk in range(CHUNKS):
        part = pl.ds(chunk * step, step)
        landed = recv_one.at[part, others]
        pltpu.make_async_copy(landed, landed, recv_one_sem.at[chunk]).wait()
        columns = jnp.concatenate(
            [
                recv_one[chunk * step + tile].reshape(mixing.shape[1], LANES)
                for tile in range(step)
            ],
            axis=1,
        )
        mixed = product((mixing[0], mixing[1]), split(columns), ((1,), (0,)))
        for device in range(devices):
            for c in range(local_channels):
                at = (device * local_channels + c) * local_rows
                for tile in range(step):
                    to = (chunk * step + tile) * local_rows
                    send_two[device, c, to : to + local_rows, :] = mixed[
                        at : at + local_rows, tile * LANES : (tile + 1) * LANES
                    ]
        there = pl.ds(pl.multiple_of(me * block_rows + chunk * rows, 8), rows)
        send_rising(chunk)
        for _to, names in targets[half:]:
            for name, slot in names:
                copy_two(chunk, name, slot).start()
        out_ref[:, there, :] = send_two[me, :, chunk * rows : (chunk + 1) * rows, :]

    sent = send_one.at[others]
    pltpu.make_async_copy(sent, sent, send_sem.at[0]).wait()
    sent = send_two.at[others]
    pltpu.make_async_copy(sent, sent, send_sem.at[1]).wait()
    landed = out_ref.at[:, pl.ds(0, (devices - 1) * block_rows)]
    pltpu.make_async_copy(landed, landed, recv_two_sem).wait()


def fused(chans, bands, slide_region, row_taps, column_taps, channel_mix):
    local_channels, local_rows, width = slide_region.shape
    devices = chans * bands
    total_tiles = width // LANES
    tiles = total_tiles // devices
    block = local_channels * local_rows
    tiled = slide_region.reshape(local_channels, local_rows, total_tiles, LANES)
    tiled = tiled.transpose(0, 2, 1, 3).reshape(local_channels, total_tiles * local_rows, LANES)
    vmem = pl.BlockSpec(memory_space=pltpu.VMEM)
    anywhere = pl.BlockSpec(memory_space=pl.ANY)
    dma = pltpu.SemaphoreType.DMA
    out = pl.pallas_call(
        functools.partial(fused_kernel, chans, bands),
        out_shape=pltpu.VMEM(tiled.shape, jnp.float32),
        in_specs=[anywhere] * 4,
        out_specs=vmem,
        scratch_shapes=[
            pltpu.VMEM((local_channels, tiled.shape[1] + 16, LANES), jnp.float32),
            pltpu.VMEM(row_taps.shape, jnp.float32),
            pltpu.VMEM(column_taps.shape, jnp.float32),
            pltpu.VMEM(channel_mix.shape, jnp.float32),
            pltpu.VMEM((local_channels, 2 * LANES, 3 * LANES), jnp.bfloat16),
            pltpu.VMEM((devices, tiles, block, LANES), jnp.float32),
            pltpu.VMEM((tiles, devices, block, LANES), jnp.float32),
            pltpu.VMEM((devices, local_channels, tiles * local_rows, LANES), jnp.float32),
            pltpu.VMEM((2, devices * block, devices * block), jnp.bfloat16),
            pltpu.SemaphoreType.REGULAR((bands,)),
            dma,
            dma,
            dma((2,)),
            dma((2,)),
            dma((CHUNKS,)),
            dma,
        ],
        compiler_params=pltpu.CompilerParams(collective_id=0, has_side_effects=True),
    )(tiled, row_taps, column_taps, channel_mix)
    out = out.reshape(local_channels, total_tiles, local_rows, LANES)
    return out.transpose(0, 2, 1, 3).reshape(slide_region.shape)


def power_of_two(number):
    return number & (number - 1) == 0


def program(chans, bands, slide_region, row_taps, column_taps, channel_mix):
    local_channels, local_rows, width = slide_region.shape
    devices = chans * bands
    margin = (row_taps.shape[1] - 1) // 2
    fits = (
        power_of_two(chans)
        and power_of_two(bands)
        and bands > 1
        and width % (devices * LANES * CHUNKS) == 0
        and margin == LANES
        and column_taps.shape[1] == row_taps.shape[1]
        and local_rows == 4
        and local_rows * bands <= margin
        and local_channels * local_rows % 8 == 0
        and width // (devices * LANES * CHUNKS) * local_rows % 8 == 0
        and devices * local_channels * local_rows <= 512
    )
    if fits:
        return fused(chans, bands, slide_region, row_taps, column_taps, channel_mix)
    return on_device(slide_region, row_taps, column_taps, channel_mix)


def solution(mesh):
    in_specs = (P("chan", ("groups", "band"), None), P("chan", None), P(), P())
    out_specs = P("chan", ("groups", "band"), None)
    return jax.shard_map(
        functools.partial(program, mesh.shape["chan"], mesh.shape["band"]),
        mesh=mesh,
        in_specs=in_specs,
        out_specs=out_specs,
        check_vma=False,
    )
```

```python
import functools

import jax
import jax.numpy as jnp
from jax import lax
from jax.experimental import pallas as pl
from jax.experimental.pallas import tpu as pltpu
from jax.sharding import PartitionSpec as P

precise = lax.Precision.HIGHEST


def band_tables(filter_taps, tile_size):
    channels, length = filter_taps.shape
    margin = (length - 1) // 2
    period = 4 * tile_size
    border = 3 * tile_size + length
    widened = jnp.pad(filter_taps, ((0, 0), (border, border)))
    lowest = margin - tile_size + border
    window = widened[:, lowest : lowest + 3 * tile_size]
    vector = jnp.pad(window, ((0, 0), (0, tile_size)))
    repeated = jnp.tile(vector, (1, tile_size))[:, : tile_size * (period - 1)]
    toeplitz = repeated.reshape(channels, tile_size, period - 1)[:, :, : 3 * tile_size]
    stacked = jnp.transpose(toeplitz, (0, 2, 1))
    return stacked.reshape(channels, 3, tile_size, tile_size)


def along_columns(signal, filter_taps):
    tile_size = 128
    tables = band_tables(filter_taps, tile_size)
    channels, row_count, col_count = signal.shape
    tile_count = col_count // tile_size
    tiled = signal.reshape(channels, row_count, tile_count, tile_size)
    padded = jnp.pad(tiled, ((0, 0), (0, 0), (1, 1), (0, 0)))
    result = jnp.einsum(
        "crti,cij->crtj", padded[:, :, 0:tile_count], tables[:, 0], precision=precise
    )
    result = result + jnp.einsum(
        "crti,cij->crtj", padded[:, :, 1 : tile_count + 1], tables[:, 1], precision=precise
    )
    result = result + jnp.einsum(
        "crti,cij->crtj", padded[:, :, 2:], tables[:, 2], precision=precise
    )
    return result.reshape(channels, row_count, col_count)


def along_rows(signal, filter_taps):
    channels, row_count, col_count = signal.shape
    tile_size = 128 if row_count % 128 == 0 else row_count
    tables = band_tables(filter_taps, tile_size)
    tile_count = row_count // tile_size
    tiled = signal.reshape(channels, tile_count, tile_size, col_count)
    padded = jnp.pad(tiled, ((0, 0), (1, 1), (0, 0), (0, 0)))
    result = jnp.einsum("ctiw,cij->ctjw", padded[:, 0:tile_count], tables[:, 0], precision=precise)
    result = result + jnp.einsum(
        "ctiw,cij->ctjw", padded[:, 1 : tile_count + 1], tables[:, 1], precision=precise
    )
    result = result + jnp.einsum("ctiw,cij->ctjw", padded[:, 2:], tables[:, 2], precision=precise)
    return result.reshape(channels, row_count, col_count)


def on_device(slide_region, row_taps, column_taps, channel_mix):
    local_channels = slide_region.shape[0]
    across = along_columns(slide_region, row_taps)
    column_band = lax.all_to_all(across, "band", split_axis=2, concat_axis=1, tiled=True)
    first_channel = lax.axis_index("chan") * local_channels
    own_taps = lax.dynamic_slice_in_dim(column_taps, first_channel, local_channels, 0)
    vertical = along_rows(column_band, own_taps)
    own_mixing = lax.dynamic_slice_in_dim(channel_mix, first_channel, local_channels, 0)
    blended = jnp.einsum(
        "oc,chw->ohw",
        own_mixing,
        lax.all_gather(vertical, "chan", axis=0, tiled=True),
        precision=precise,
    )
    return lax.all_to_all(blended, "band", split_axis=1, concat_axis=2, tiled=True)


LANES = 128
CHUNKS = 2


def split(value):
    high = value.astype(jnp.bfloat16)
    return high, (value - high.astype(jnp.float32)).astype(jnp.bfloat16)


def product(left, right, dims):
    (left_high, left_low), (right_high, right_low) = left, right
    dot = functools.partial(
        lax.dot_general, dimension_numbers=(dims, ((), ())), preferred_element_type=jnp.float32
    )
    return dot(left_high, right_high) + (dot(left_low, right_high) + dot(left_high, right_low))


def filter_table(taps):
    shape = (LANES, LANES)
    lane = lax.broadcasted_iota(jnp.int32, shape, 1)
    row = lax.broadcasted_iota(jnp.int32, shape, 0)
    first, second = (
        pltpu.roll(
            jnp.broadcast_to(taps[:, at : at + LANES], shape), 0, 1, stride=1, stride_axis=0
        )
        for at in (0, LANES)
    )
    last = jnp.broadcast_to(taps[:, 2 * LANES :], shape)
    zero = jnp.zeros(shape, jnp.float32)
    return jnp.concatenate(
        [
            jnp.where(lane >= row, first, zero),
            jnp.where(lane >= row, second, first),
            jnp.where(lane == row, last, jnp.where(lane < row, second, zero)),
        ],
        axis=1,
    )


def mixing_table(column_taps, channel_mix, chans, bands, local_channels, local_rows):
    channels = chans * local_channels
    height = bands * local_rows
    block = local_channels * local_rows
    size = chans * bands * block
    margin = (column_taps.shape[1] - 1) // 2

    def coordinates(index):
        device, inner = index // block, index % block
        return (
            local_channels * (device % chans) + inner // local_rows,
            local_rows * (device // chans) + inner % local_rows,
        )

    tall = (size, channels)
    wide = (channels, size)
    pick_tall = (
        coordinates(lax.broadcasted_iota(jnp.int32, tall, 0))[0]
        == lax.broadcasted_iota(jnp.int32, tall, 1)
    ).astype(jnp.float32)
    pick_wide = (
        coordinates(lax.broadcasted_iota(jnp.int32, wide, 1))[0]
        == lax.broadcasted_iota(jnp.int32, wide, 0)
    ).astype(jnp.float32)
    weights = jnp.dot(
        jnp.dot(pick_tall, channel_mix, precision=precise), pick_wide, precision=precise
    )
    taps = lax.dot_general(
        column_taps[:, : 2 * margin],
        pick_wide,
        (((0,), (0,)), ((), ())),
        precision=precise,
    )
    square = (size, size)
    apart = (
        coordinates(lax.broadcasted_iota(jnp.int32, square, 1))[1]
        - coordinates(lax.broadcasted_iota(jnp.int32, square, 0))[1]
    )
    spread = jnp.zeros(square, jnp.float32)
    for distance in range(1 - height, height):
        at = margin + distance
        spread = jnp.where(apart == distance, taps[at : at + 1, :], spread)
    return weights * spread


def fused_kernel(
    chans, bands, x_hbm, row_hbm, column_hbm, mix_hbm, out_ref,
    x_buf, row_taps, column_taps, channel_mix, tables,
    send_one, recv_one, send_two, mixing,
    ready, x_sem, row_sem, small_sem, send_sem, recv_one_sem, recv_two_sem,
):
    local_channels, x_rows, _ = x_hbm.shape
    devices, _, block_rows, _ = send_two.shape
    tiles = send_one.shape[1]
    local_rows = block_rows // tiles
    band_rows = x_rows // bands
    others = pl.ds(0, devices - 1)
    chan, band = lax.axis_index("chan"), lax.axis_index("band")
    me = band * chans + chan
    half = bands // 2
    left = band < half

    row_load = pltpu.make_async_copy(row_hbm, row_taps, row_sem)
    row_load.start()
    x_inside = x_buf.at[:, pl.ds(8, x_rows)]
    for c in range(local_channels):
        pltpu.make_async_copy(x_hbm.at[c], x_inside.at[c], x_sem).start()

    low = 2 * chan < chans
    inner = jnp.logical_or(band == half - 1, band == half)
    outer = jnp.logical_not(inner)
    high = jnp.logical_not(low)
    beside = band ^ 1
    across = band ^ 3
    first = jnp.where(inner, across, band ^ 2)
    second = jnp.where(inner, band ^ 2, across)

    def device(to_chan, to_band):
        to_chan = jnp.int32(to_chan) if isinstance(to_chan, int) else to_chan
        return {"chan": to_chan, "band": to_band}, to_band * chans + to_chan

    def whole(to_band):
        return [device(to_chan, to_band) for to_chan in range(chans)]

    own = [device(chan ^ step, band) for step in range(1, chans)]
    middle = chans // 2

    barrier = pltpu.get_barrier_semaphore()
    inner_ready, outer_ready, go_first, go_outer, go_all = (ready.at[k] for k in range(5))

    def greet(semaphore, *names):
        for name, _slot in names:
            pl.semaphore_signal(
                semaphore, inc=1, device_id=name, device_id_type=pl.DeviceIdType.MESH
            )

    @pl.when(inner)
    def _():
        pl.when(low)(lambda: greet(barrier, *whole(across)[:middle]))
        greet(barrier, *whole(across)[middle:], *whole(beside))

    small_loads = [
        pltpu.make_async_copy(column_hbm, column_taps, small_sem.at[0]),
        pltpu.make_async_copy(mix_hbm, channel_mix, small_sem.at[1]),
    ]
    for load in small_loads:
        load.start()

    edge = jnp.zeros((8, LANES), jnp.float32)
    for c in range(local_channels):
        x_buf[c, 0:8, :] = edge
        x_buf[c, x_rows + 8 : x_rows + 16, :] = edge

    def meet():
        pl.semaphore_wait(barrier, jnp.where(jnp.logical_and(inner, low), middle, chans))

        @pl.when(jnp.logical_and(inner, high))
        def _():
            greet(inner_ready, *whole(across)[:middle])

        @pl.when(outer)
        def _():
            greet(outer_ready, *whole(beside))

    meet_first = jnp.logical_and(high, jnp.logical_not(left))
    pl.when(meet_first)(meet)

    def make_tables(channels):
        for c in channels:
            tables[c, 0:LANES], tables[c, LANES:] = split(filter_table(row_taps[c : c + 1, :]))

    def filter_band(which, channels):
        start = pl.multiple_of(which * band_rows, 8)
        for c in channels:
            wide = x_buf[c, pl.ds(start, band_rows + 16), :]
            window = jnp.concatenate(
                [
                    wide[8 + (k - 1) * local_rows : 8 + (k - 1) * local_rows + band_rows]
                    for k in range(3)
                ],
                axis=1,
            )
            both = lax.dot_general(
                jnp.concatenate(split(window), axis=0),
                tables[c],
                (((1,), (1,)), ((), ())),
                preferred_element_type=jnp.float32,
            )
            filtered = both[:band_rows, :LANES] + (
                both[band_rows:, :LANES] + both[:band_rows, LANES:]
            )
            for to in range(chans):
                for tile in range(tiles):
                    at = (to * tiles + tile) * local_rows
                    send_one[
                        which * chans + to,
                        tile,
                        c * local_rows : (c + 1) * local_rows,
                        :,
                    ] = filtered[at : at + local_rows, :]

    step = tiles // CHUNKS
    block = local_channels * local_rows
    every = (0, block)

    def send(chunk, names, rows=every):
        part, lines = pl.ds(chunk * step, step), pl.ds(rows[0], rows[1])
        for name, slot in names:
            pltpu.make_async_remote_copy(
                src_ref=send_one.at[slot, part, lines],
                dst_ref=recv_one.at[part, me, lines],
                send_sem=send_sem.at[0],
                recv_sem=recv_one_sem.at[chunk],
                device_id=name,
                device_id_type=pl.DeviceIdType.MESH,
            ).start()

    row_load.wait()
    near, far = whole(first)[:middle], whole(first)[middle:]
    both_high = jnp.logical_and(inner, high)
    both_low = jnp.logical_and(inner, low)
    for piece in range(2):
        channels = range(piece * local_channels // 2, (piece + 1) * local_channels // 2)
        rows = (piece * block // 2, block // 2)
        make_tables(channels)
        if piece == 0:
            pltpu.make_async_copy(x_hbm, x_inside, x_sem).wait()
        filter_band(first, channels)
        if piece == 0:
            pl.when(jnp.logical_not(meet_first))(meet)
        pl.when(inner)(lambda: send(0, near, rows))
        pl.when(both_high)(lambda: send(0, far, rows))
    for chunk in range(1, CHUNKS):
        pl.when(inner)(lambda: send(chunk, near))
        pl.when(both_high)(lambda: send(chunk, far))
    for to in (beside, second, band):
        filter_band(to, range(local_channels))

    @pl.when(both_low)
    def _():
        pl.semaphore_wait(inner_ready, middle)
        for chunk in range(CHUNKS):
            send(chunk, far)

    @pl.when(inner)
    def _():
        pl.semaphore_wait(outer_ready, chans)
        greet(go_first, device(chan, beside))
        greet(go_outer, device(chan, across))

    pl.when(inner)(lambda: send(0, whole(beside)))

    @pl.when(outer)
    def _():
        pl.semaphore_wait(go_first, 1)
        send(0, near + far)
        send(0, whole(beside))
        send(0, own)

    @pl.when(inner)
    def _():
        pl.semaphore_wait(go_outer, 1)
        greet(go_all, device(chan, beside))

    @pl.when(outer)
    def _():
        pl.semaphore_wait(go_all, 1)

    send(0, whole(second))
    pl.when(inner)(lambda: send(0, own))
    for chunk in range(1, CHUNKS):
        pl.when(outer)(lambda: send(chunk, near + far))
        send(chunk, whole(second))
        send(chunk, whole(beside))
        send(chunk, own)
    recv_one[:, me] = send_one[me]

    for load in small_loads:
        load.wait()
    table = mixing_table(
        column_taps[...], channel_mix[...], chans, bands, local_channels, local_rows
    )
    mixing[0], mixing[1] = split(table)

    rows = step * local_rows

    def back(chunk, name, slot):
        pltpu.make_async_remote_copy(
            src_ref=send_two.at[slot, :, pl.ds(chunk * rows, rows)],
            dst_ref=out_ref.at[
                :, pl.ds(pl.multiple_of(me * block_rows + chunk * rows, 8), rows)
            ],
            send_sem=send_sem.at[1],
            recv_sem=recv_two_sem,
            device_id=name,
            device_id_type=pl.DeviceIdType.MESH,
        ).start()

    late = band == half
    prompt = jnp.logical_not(late)

    def send_back(chunk):
        for part in range(2):
            for k in range(half):
                for name, slot in whole(jnp.where(left, half + k, k))[
                    part * middle : (part + 1) * middle
                ]:
                    if part == 0 or k == 0:
                        back(chunk, name, slot)
                    elif chunk < CHUNKS - 1:
                        pl.when(prompt)(functools.partial(back, chunk, name, slot))
                    else:
                        for held in range(chunk):
                            pl.when(late)(functools.partial(back, held, name, slot))
                        back(chunk, name, slot)
        for name, slot in whole(beside) + own:
            back(chunk, name, slot)

    for chunk in range(CHUNKS):
        part = pl.ds(chunk * step, step)
        landed = recv_one.at[part, others]
        pltpu.make_async_copy(landed, landed, recv_one_sem.at[chunk]).wait()
        columns = jnp.concatenate(
            [
                recv_one[chunk * step + tile].reshape(mixing.shape[1], LANES)
                for tile in range(step)
            ],
            axis=1,
        )
        mixed = product((mixing[0], mixing[1]), split(columns), ((1,), (0,)))
        for to_device in range(devices):
            for c in range(local_channels):
                at = (to_device * local_channels + c) * local_rows
                for tile in range(step):
                    to = (chunk * step + tile) * local_rows
                    send_two[to_device, c, to : to + local_rows, :] = mixed[
                        at : at + local_rows, tile * LANES : (tile + 1) * LANES
                    ]
        there = pl.ds(pl.multiple_of(me * block_rows + chunk * rows, 8), rows)
        send_back(chunk)
        out_ref[:, there, :] = send_two[me, :, chunk * rows : (chunk + 1) * rows, :]

    sent = send_one.at[others]
    pltpu.make_async_copy(sent, sent, send_sem.at[0]).wait()
    sent = send_two.at[others]
    pltpu.make_async_copy(sent, sent, send_sem.at[1]).wait()
    landed = out_ref.at[:, pl.ds(0, (devices - 1) * block_rows)]
    pltpu.make_async_copy(landed, landed, recv_two_sem).wait()


def fused(chans, bands, slide_region, row_taps, column_taps, channel_mix):
    local_channels, local_rows, width = slide_region.shape
    devices = chans * bands
    total_tiles = width // LANES
    tiles = total_tiles // devices
    block = local_channels * local_rows
    tiled = slide_region.reshape(local_channels, local_rows, total_tiles, LANES)
    tiled = tiled.transpose(0, 2, 1, 3).reshape(local_channels, total_tiles * local_rows, LANES)
    vmem = pl.BlockSpec(memory_space=pltpu.VMEM)
    anywhere = pl.BlockSpec(memory_space=pl.ANY)
    dma = pltpu.SemaphoreType.DMA
    out = pl.pallas_call(
        functools.partial(fused_kernel, chans, bands),
        out_shape=pltpu.VMEM(tiled.shape, jnp.float32),
        in_specs=[anywhere] * 4,
        out_specs=vmem,
        scratch_shapes=[
            pltpu.VMEM((local_channels, tiled.shape[1] + 16, LANES), jnp.float32),
            pltpu.VMEM(row_taps.shape, jnp.float32),
            pltpu.VMEM(column_taps.shape, jnp.float32),
            pltpu.VMEM(channel_mix.shape, jnp.float32),
            pltpu.VMEM((local_channels, 2 * LANES, 3 * LANES), jnp.bfloat16),
            pltpu.VMEM((devices, tiles, block, LANES), jnp.float32),
            pltpu.VMEM((tiles, devices, block, LANES), jnp.float32),
            pltpu.VMEM((devices, local_channels, tiles * local_rows, LANES), jnp.float32),
            pltpu.VMEM((2, devices * block, devices * block), jnp.bfloat16),
            pltpu.SemaphoreType.REGULAR((5,)),
            dma,
            dma,
            dma((2,)),
            dma((2,)),
            dma((CHUNKS,)),
            dma,
        ],
        compiler_params=pltpu.CompilerParams(collective_id=0, has_side_effects=True),
    )(tiled, row_taps, column_taps, channel_mix)
    out = out.reshape(local_channels, total_tiles, local_rows, LANES)
    return out.transpose(0, 2, 1, 3).reshape(slide_region.shape)


def power_of_two(number):
    return number & (number - 1) == 0


def program(chans, bands, slide_region, row_taps, column_taps, channel_mix):
    local_channels, local_rows, width = slide_region.shape
    devices = chans * bands
    margin = (row_taps.shape[1] - 1) // 2
    fits = (
        power_of_two(chans)
        and chans > 1
        and bands == 4
        and width % (devices * LANES * CHUNKS) == 0
        and margin == LANES
        and column_taps.shape[1] == row_taps.shape[1]
        and local_rows == 4
        and local_channels * local_rows % 16 == 0
        and local_rows * bands <= margin
        and width // (devices * LANES * CHUNKS) * local_rows % 8 == 0
        and devices * local_channels * local_rows <= 512
    )
    if fits:
        return fused(chans, bands, slide_region, row_taps, column_taps, channel_mix)
    return on_device(slide_region, row_taps, column_taps, channel_mix)


def solution(mesh):
    in_specs = (P("chan", ("groups", "band"), None), P("chan", None), P(), P())
    out_specs = P("chan", ("groups", "band"), None)
    return jax.shard_map(
        functools.partial(program, mesh.shape["chan"], mesh.shape["band"]),
        mesh=mesh,
        in_specs=in_specs,
        out_specs=out_specs,
        check_vma=False,
    )
```

```python
import functools

import jax
import jax.numpy as jnp
from jax import lax
from jax.experimental import pallas as pl
from jax.experimental.pallas import tpu as pltpu
from jax.sharding import PartitionSpec as P

precise = lax.Precision.HIGHEST


def band_tables(filter_taps, tile_size):
    channels, length = filter_taps.shape
    margin = (length - 1) // 2
    period = 4 * tile_size
    border = 3 * tile_size + length
    widened = jnp.pad(filter_taps, ((0, 0), (border, border)))
    lowest = margin - tile_size + border
    window = widened[:, lowest : lowest + 3 * tile_size]
    vector = jnp.pad(window, ((0, 0), (0, tile_size)))
    repeated = jnp.tile(vector, (1, tile_size))[:, : tile_size * (period - 1)]
    toeplitz = repeated.reshape(channels, tile_size, period - 1)[:, :, : 3 * tile_size]
    stacked = jnp.transpose(toeplitz, (0, 2, 1))
    return stacked.reshape(channels, 3, tile_size, tile_size)


def along_columns(signal, filter_taps):
    tile_size = 128
    tables = band_tables(filter_taps, tile_size)
    channels, row_count, col_count = signal.shape
    tile_count = col_count // tile_size
    tiled = signal.reshape(channels, row_count, tile_count, tile_size)
    padded = jnp.pad(tiled, ((0, 0), (0, 0), (1, 1), (0, 0)))
    result = jnp.einsum(
        "crti,cij->crtj", padded[:, :, 0:tile_count], tables[:, 0], precision=precise
    )
    result = result + jnp.einsum(
        "crti,cij->crtj", padded[:, :, 1 : tile_count + 1], tables[:, 1], precision=precise
    )
    result = result + jnp.einsum(
        "crti,cij->crtj", padded[:, :, 2:], tables[:, 2], precision=precise
    )
    return result.reshape(channels, row_count, col_count)


def along_rows(signal, filter_taps):
    channels, row_count, col_count = signal.shape
    tile_size = 128 if row_count % 128 == 0 else row_count
    tables = band_tables(filter_taps, tile_size)
    tile_count = row_count // tile_size
    tiled = signal.reshape(channels, tile_count, tile_size, col_count)
    padded = jnp.pad(tiled, ((0, 0), (1, 1), (0, 0), (0, 0)))
    result = jnp.einsum("ctiw,cij->ctjw", padded[:, 0:tile_count], tables[:, 0], precision=precise)
    result = result + jnp.einsum(
        "ctiw,cij->ctjw", padded[:, 1 : tile_count + 1], tables[:, 1], precision=precise
    )
    result = result + jnp.einsum("ctiw,cij->ctjw", padded[:, 2:], tables[:, 2], precision=precise)
    return result.reshape(channels, row_count, col_count)


def on_device(slide_region, row_taps, column_taps, channel_mix):
    local_channels = slide_region.shape[0]
    across = along_columns(slide_region, row_taps)
    column_band = lax.all_to_all(across, "band", split_axis=2, concat_axis=1, tiled=True)
    first_channel = lax.axis_index("chan") * local_channels
    own_taps = lax.dynamic_slice_in_dim(column_taps, first_channel, local_channels, 0)
    vertical = along_rows(column_band, own_taps)
    own_mixing = lax.dynamic_slice_in_dim(channel_mix, first_channel, local_channels, 0)
    blended = jnp.einsum(
        "oc,chw->ohw",
        own_mixing,
        lax.all_gather(vertical, "chan", axis=0, tiled=True),
        precision=precise,
    )
    return lax.all_to_all(blended, "band", split_axis=1, concat_axis=2, tiled=True)


LANES = 128
CHUNKS = 2


def split(value):
    high = value.astype(jnp.bfloat16)
    return high, (value - high.astype(jnp.float32)).astype(jnp.bfloat16)


def product(left, right, dims):
    (left_high, left_low), (right_high, right_low) = left, right
    dot = functools.partial(
        lax.dot_general, dimension_numbers=(dims, ((), ())), preferred_element_type=jnp.float32
    )
    return dot(left_high, right_high) + (dot(left_low, right_high) + dot(left_high, right_low))


def filter_table(taps):
    shape = (LANES, LANES)
    lane = lax.broadcasted_iota(jnp.int32, shape, 1)
    row = lax.broadcasted_iota(jnp.int32, shape, 0)
    first, second = (
        pltpu.roll(
            jnp.broadcast_to(taps[:, at : at + LANES], shape), 0, 1, stride=1, stride_axis=0
        )
        for at in (0, LANES)
    )
    last = jnp.broadcast_to(taps[:, 2 * LANES :], shape)
    zero = jnp.zeros(shape, jnp.float32)
    return jnp.concatenate(
        [
            jnp.where(lane >= row, first, zero),
            jnp.where(lane >= row, second, first),
            jnp.where(lane == row, last, jnp.where(lane < row, second, zero)),
        ],
        axis=1,
    )


def mixing_table(column_taps, channel_mix, chans, bands, local_channels, local_rows):
    channels = chans * local_channels
    height = bands * local_rows
    block = local_channels * local_rows
    size = chans * bands * block
    margin = (column_taps.shape[1] - 1) // 2

    def coordinates(index):
        device, inner = index // block, index % block
        return (
            local_channels * (device % chans) + inner // local_rows,
            local_rows * (device // chans) + inner % local_rows,
        )

    tall = (size, channels)
    wide = (channels, size)
    pick_tall = (
        coordinates(lax.broadcasted_iota(jnp.int32, tall, 0))[0]
        == lax.broadcasted_iota(jnp.int32, tall, 1)
    ).astype(jnp.float32)
    pick_wide = (
        coordinates(lax.broadcasted_iota(jnp.int32, wide, 1))[0]
        == lax.broadcasted_iota(jnp.int32, wide, 0)
    ).astype(jnp.float32)
    weights = jnp.dot(
        jnp.dot(pick_tall, channel_mix, precision=precise), pick_wide, precision=precise
    )
    taps = lax.dot_general(
        column_taps[:, : 2 * margin],
        pick_wide,
        (((0,), (0,)), ((), ())),
        precision=precise,
    )
    square = (size, size)
    apart = (
        coordinates(lax.broadcasted_iota(jnp.int32, square, 1))[1]
        - coordinates(lax.broadcasted_iota(jnp.int32, square, 0))[1]
    )
    spread = jnp.zeros(square, jnp.float32)
    for distance in range(1 - height, height):
        at = margin + distance
        spread = jnp.where(apart == distance, taps[at : at + 1, :], spread)
    return weights * spread


def fused_kernel(
    chans, bands, x_hbm, row_hbm, column_hbm, mix_hbm, out_ref,
    x_buf, row_taps, column_taps, channel_mix, tables,
    send_one, recv_one, send_two, mixing,
    ready, x_sem, row_sem, send_sem, recv_one_sem, recv_two_sem,
):
    local_channels, x_rows, _ = x_hbm.shape
    devices, _, block_rows, _ = send_two.shape
    tiles = send_one.shape[1]
    local_rows = block_rows // tiles
    band_rows = x_rows // bands
    others = pl.ds(0, devices - 1)
    chan, band = lax.axis_index("chan"), lax.axis_index("band")
    me = band * chans + chan
    half = bands // 2
    left = band < half

    row_load = pltpu.make_async_copy(row_hbm, row_taps, row_sem)
    row_load.start()
    x_inside = x_buf.at[:, pl.ds(8, x_rows)]
    for c in range(local_channels):
        pltpu.make_async_copy(x_hbm.at[c], x_inside.at[c], x_sem).start()

    low = 2 * chan < chans
    inner = jnp.logical_or(band == half - 1, band == half)
    outer = jnp.logical_not(inner)
    high = jnp.logical_not(low)
    beside = band ^ 1
    across = band ^ 3
    first = jnp.where(inner, across, band ^ 2)
    second = jnp.where(inner, band ^ 2, across)

    def device(to_chan, to_band):
        to_chan = jnp.int32(to_chan) if isinstance(to_chan, int) else to_chan
        return {"chan": to_chan, "band": to_band}, to_band * chans + to_chan

    def whole(to_band):
        return [device(to_chan, to_band) for to_chan in range(chans)]

    own = [device(chan ^ step, band) for step in range(1, chans)]
    middle = chans // 2

    barrier = pltpu.get_barrier_semaphore()
    inner_ready = ready.at[0]
    outer_ready = go_first = ready.at[1]
    go_outer = go_all = ready.at[2]

    def greet(semaphore, *names):
        for name, _slot in names:
            pl.semaphore_signal(
                semaphore, inc=1, device_id=name, device_id_type=pl.DeviceIdType.MESH
            )

    @pl.when(inner)
    def _():
        pl.when(low)(lambda: greet(barrier, *whole(across)[:middle]))
        greet(barrier, *whole(across)[middle:], *whole(beside))

    edge = jnp.zeros((8, LANES), jnp.float32)
    for c in range(local_channels):
        x_buf[c, 0:8, :] = edge
        x_buf[c, x_rows + 8 : x_rows + 16, :] = edge

    def meet():
        pl.semaphore_wait(barrier, jnp.where(jnp.logical_and(inner, low), middle, chans))

        @pl.when(jnp.logical_and(inner, high))
        def _():
            greet(inner_ready, *whole(across)[:middle])

        @pl.when(outer)
        def _():
            greet(outer_ready, *whole(beside))

    meet_first = jnp.logical_and(high, jnp.logical_not(left))
    pl.when(meet_first)(meet)

    def make_tables(channels):
        for c in channels:
            tables[c, 0:LANES], tables[c, LANES:] = split(filter_table(row_taps[c : c + 1, :]))

    def filter_band(which, channels):
        start = pl.multiple_of(which * band_rows, 8)
        for c in channels:
            wide = x_buf[c, pl.ds(start, band_rows + 16), :]
            window = jnp.concatenate(
                [
                    wide[8 + (k - 1) * local_rows : 8 + (k - 1) * local_rows + band_rows]
                    for k in range(3)
                ],
                axis=1,
            )
            both = lax.dot_general(
                jnp.concatenate(split(window), axis=0),
                tables[c],
                (((1,), (1,)), ((), ())),
                preferred_element_type=jnp.float32,
            )
            filtered = both[:band_rows, :LANES] + (
                both[band_rows:, :LANES] + both[:band_rows, LANES:]
            )
            for to in range(chans):
                for tile in range(tiles):
                    at = (to * tiles + tile) * local_rows
                    send_one[
                        which * chans + to,
                        tile,
                        c * local_rows : (c + 1) * local_rows,
                        :,
                    ] = filtered[at : at + local_rows, :]

    step = tiles // CHUNKS
    block = local_channels * local_rows
    every = (0, block)

    def send(chunk, names, rows=every):
        part, lines = pl.ds(chunk * step, step), pl.ds(rows[0], rows[1])
        for name, slot in names:
            pltpu.make_async_remote_copy(
                src_ref=send_one.at[slot, part, lines],
                dst_ref=recv_one.at[part, me, lines],
                send_sem=send_sem.at[0],
                recv_sem=recv_one_sem.at[chunk],
                device_id=name,
                device_id_type=pl.DeviceIdType.MESH,
            ).start()

    row_load.wait()
    near, far = whole(first)[:middle], whole(first)[middle:]
    both_high = jnp.logical_and(inner, high)
    both_low = jnp.logical_and(inner, low)
    for piece in range(2):
        channels = range(piece * local_channels // 2, (piece + 1) * local_channels // 2)
        rows = (piece * block // 2, block // 2)
        make_tables(channels)
        if piece == 0:
            pltpu.make_async_copy(x_hbm, x_inside, x_sem).wait()
        filter_band(first, channels)
        if piece == 0:
            pl.when(jnp.logical_not(meet_first))(meet)
        pl.when(inner)(lambda: send(0, near, rows))
        pl.when(both_high)(lambda: send(0, far, rows))
    small_loads = [
        pltpu.make_async_copy(column_hbm, column_taps, row_sem),
        pltpu.make_async_copy(mix_hbm, channel_mix, x_sem),
    ]
    for load in small_loads:
        load.start()
    for chunk in range(1, CHUNKS):
        pl.when(inner)(lambda: send(chunk, near))
        pl.when(both_high)(lambda: send(chunk, far))
    for to in (beside, second, band):
        filter_band(to, range(local_channels))

    @pl.when(both_low)
    def _():
        pl.semaphore_wait(inner_ready, middle)
        for chunk in range(CHUNKS):
            send(chunk, far)

    @pl.when(inner)
    def _():
        pl.semaphore_wait(outer_ready, chans)
        greet(go_first, device(chan, beside))
        greet(go_outer, device(chan, across))

    pl.when(inner)(lambda: send(0, whole(beside)))

    @pl.when(outer)
    def _():
        pl.semaphore_wait(go_first, 1)
        send(0, near + far)
        send(0, whole(beside))
        send(0, own)

    @pl.when(inner)
    def _():
        pl.semaphore_wait(go_outer, 1)
        greet(go_all, device(chan, beside))

    @pl.when(outer)
    def _():
        pl.semaphore_wait(go_all, 1)

    send(0, whole(second))
    pl.when(inner)(lambda: send(0, own))
    for chunk in range(1, CHUNKS):
        pl.when(outer)(lambda: send(chunk, near + far))
        send(chunk, whole(second))
        send(chunk, whole(beside))
        send(chunk, own)
    recv_one[:, me] = send_one[me]

    for load in small_loads:
        load.wait()
    table = mixing_table(
        column_taps[...], channel_mix[...], chans, bands, local_channels, local_rows
    )
    mixing[0], mixing[1] = split(table)

    rows = step * local_rows

    def back(chunk, name, slot):
        pltpu.make_async_remote_copy(
            src_ref=send_two.at[slot, :, pl.ds(chunk * rows, rows)],
            dst_ref=out_ref.at[
                :, pl.ds(pl.multiple_of(me * block_rows + chunk * rows, 8), rows)
            ],
            send_sem=send_sem.at[1],
            recv_sem=recv_two_sem,
            device_id=name,
            device_id_type=pl.DeviceIdType.MESH,
        ).start()

    late = band == half
    prompt = jnp.logical_not(late)

    def send_back(chunk):
        for part, k in ((0, 0), (1, 0), (0, 1), (1, 1)):
            if True:
                for name, slot in whole(jnp.where(left, half + k, k))[
                    part * middle : (part + 1) * middle
                ]:
                    if part == 0 or k == 0:
                        back(chunk, name, slot)
                    elif chunk < CHUNKS - 1:
                        pl.when(prompt)(functools.partial(back, chunk, name, slot))
                    else:
                        for held in range(chunk):
                            pl.when(late)(functools.partial(back, held, name, slot))
                        back(chunk, name, slot)
        for name, slot in whole(beside) + own:
            back(chunk, name, slot)

    for chunk in range(CHUNKS):
        part = pl.ds(chunk * step, step)
        landed = recv_one.at[part, others]
        pltpu.make_async_copy(landed, landed, recv_one_sem.at[chunk]).wait()
        columns = jnp.concatenate(
            [
                recv_one[chunk * step + tile].reshape(mixing.shape[1], LANES)
                for tile in range(step)
            ],
            axis=1,
        )
        mixed = product((mixing[0], mixing[1]), split(columns), ((1,), (0,)))
        for to_device in range(devices):
            for c in range(local_channels):
                at = (to_device * local_channels + c) * local_rows
                for tile in range(step):
                    to = (chunk * step + tile) * local_rows
                    send_two[to_device, c, to : to + local_rows, :] = mixed[
                        at : at + local_rows, tile * LANES : (tile + 1) * LANES
                    ]
        there = pl.ds(pl.multiple_of(me * block_rows + chunk * rows, 8), rows)
        send_back(chunk)
        out_ref[:, there, :] = send_two[me, :, chunk * rows : (chunk + 1) * rows, :]

    sent = send_one.at[others]
    pltpu.make_async_copy(sent, sent, send_sem.at[0]).wait()
    sent = send_two.at[others]
    pltpu.make_async_copy(sent, sent, send_sem.at[1]).wait()
    landed = out_ref.at[:, pl.ds(0, (devices - 1) * block_rows)]
    pltpu.make_async_copy(landed, landed, recv_two_sem).wait()


def fused(chans, bands, slide_region, row_taps, column_taps, channel_mix):
    local_channels, local_rows, width = slide_region.shape
    devices = chans * bands
    total_tiles = width // LANES
    tiles = total_tiles // devices
    block = local_channels * local_rows
    tiled = slide_region.reshape(local_channels, local_rows, total_tiles, LANES)
    tiled = tiled.transpose(0, 2, 1, 3).reshape(local_channels, total_tiles * local_rows, LANES)
    vmem = pl.BlockSpec(memory_space=pltpu.VMEM)
    anywhere = pl.BlockSpec(memory_space=pl.ANY)
    dma = pltpu.SemaphoreType.DMA
    out = pl.pallas_call(
        functools.partial(fused_kernel, chans, bands),
        out_shape=pltpu.VMEM(tiled.shape, jnp.float32),
        in_specs=[anywhere] * 4,
        out_specs=vmem,
        scratch_shapes=[
            pltpu.VMEM((local_channels, tiled.shape[1] + 16, LANES), jnp.float32),
            pltpu.VMEM(row_taps.shape, jnp.float32),
            pltpu.VMEM(column_taps.shape, jnp.float32),
            pltpu.VMEM(channel_mix.shape, jnp.float32),
            pltpu.VMEM((local_channels, 2 * LANES, 3 * LANES), jnp.bfloat16),
            pltpu.VMEM((devices, tiles, block, LANES), jnp.float32),
            pltpu.VMEM((tiles, devices, block, LANES), jnp.float32),
            pltpu.VMEM((devices, local_channels, tiles * local_rows, LANES), jnp.float32),
            pltpu.VMEM((2, devices * block, devices * block), jnp.bfloat16),
            pltpu.SemaphoreType.REGULAR((3,)),
            dma,
            dma,
            dma((2,)),
            dma((CHUNKS,)),
            dma,
        ],
        compiler_params=pltpu.CompilerParams(collective_id=0, has_side_effects=True),
    )(tiled, row_taps, column_taps, channel_mix)
    out = out.reshape(local_channels, total_tiles, local_rows, LANES)
    return out.transpose(0, 2, 1, 3).reshape(slide_region.shape)


def power_of_two(number):
    return number & (number - 1) == 0


def program(chans, bands, slide_region, row_taps, column_taps, channel_mix):
    local_channels, local_rows, width = slide_region.shape
    devices = chans * bands
    margin = (row_taps.shape[1] - 1) // 2
    fits = (
        power_of_two(chans)
        and chans > 1
        and bands == 4
        and width % (devices * LANES * CHUNKS) == 0
        and margin == LANES
        and column_taps.shape[1] == row_taps.shape[1]
        and local_rows == 4
        and local_channels * local_rows % 16 == 0
        and local_rows * bands <= margin
        and width // (devices * LANES * CHUNKS) * local_rows % 8 == 0
        and devices * local_channels * local_rows <= 512
    )
    if fits:
        return fused(chans, bands, slide_region, row_taps, column_taps, channel_mix)
    return on_device(slide_region, row_taps, column_taps, channel_mix)


def solution(mesh):
    in_specs = (P("chan", ("groups", "band"), None), P("chan", None), P(), P())
    out_specs = P("chan", ("groups", "band"), None)
    return jax.shard_map(
        functools.partial(program, mesh.shape["chan"], mesh.shape["band"]),
        mesh=mesh,
        in_specs=in_specs,
        out_specs=out_specs,
        check_vma=False,
    )
```

```python
import functools

import jax
import jax.numpy as jnp
from jax import lax
from jax.experimental import pallas as pl
from jax.experimental.pallas import tpu as pltpu
from jax.sharding import PartitionSpec as P

precise = lax.Precision.HIGHEST


def band_tables(filter_taps, tile_size):
    channels, length = filter_taps.shape
    margin = (length - 1) // 2
    period = 4 * tile_size
    border = 3 * tile_size + length
    widened = jnp.pad(filter_taps, ((0, 0), (border, border)))
    lowest = margin - tile_size + border
    window = widened[:, lowest : lowest + 3 * tile_size]
    vector = jnp.pad(window, ((0, 0), (0, tile_size)))
    repeated = jnp.tile(vector, (1, tile_size))[:, : tile_size * (period - 1)]
    toeplitz = repeated.reshape(channels, tile_size, period - 1)[:, :, : 3 * tile_size]
    stacked = jnp.transpose(toeplitz, (0, 2, 1))
    return stacked.reshape(channels, 3, tile_size, tile_size)


def along_columns(signal, filter_taps):
    tile_size = 128
    tables = band_tables(filter_taps, tile_size)
    channels, row_count, col_count = signal.shape
    tile_count = col_count // tile_size
    tiled = signal.reshape(channels, row_count, tile_count, tile_size)
    padded = jnp.pad(tiled, ((0, 0), (0, 0), (1, 1), (0, 0)))
    result = jnp.einsum(
        "crti,cij->crtj", padded[:, :, 0:tile_count], tables[:, 0], precision=precise
    )
    result = result + jnp.einsum(
        "crti,cij->crtj", padded[:, :, 1 : tile_count + 1], tables[:, 1], precision=precise
    )
    result = result + jnp.einsum(
        "crti,cij->crtj", padded[:, :, 2:], tables[:, 2], precision=precise
    )
    return result.reshape(channels, row_count, col_count)


def along_rows(signal, filter_taps):
    channels, row_count, col_count = signal.shape
    tile_size = 128 if row_count % 128 == 0 else row_count
    tables = band_tables(filter_taps, tile_size)
    tile_count = row_count // tile_size
    tiled = signal.reshape(channels, tile_count, tile_size, col_count)
    padded = jnp.pad(tiled, ((0, 0), (1, 1), (0, 0), (0, 0)))
    result = jnp.einsum("ctiw,cij->ctjw", padded[:, 0:tile_count], tables[:, 0], precision=precise)
    result = result + jnp.einsum(
        "ctiw,cij->ctjw", padded[:, 1 : tile_count + 1], tables[:, 1], precision=precise
    )
    result = result + jnp.einsum("ctiw,cij->ctjw", padded[:, 2:], tables[:, 2], precision=precise)
    return result.reshape(channels, row_count, col_count)


def on_device(slide_region, row_taps, column_taps, channel_mix):
    local_channels = slide_region.shape[0]
    across = along_columns(slide_region, row_taps)
    column_band = lax.all_to_all(across, "band", split_axis=2, concat_axis=1, tiled=True)
    first_channel = lax.axis_index("chan") * local_channels
    own_taps = lax.dynamic_slice_in_dim(column_taps, first_channel, local_channels, 0)
    vertical = along_rows(column_band, own_taps)
    own_mixing = lax.dynamic_slice_in_dim(channel_mix, first_channel, local_channels, 0)
    blended = jnp.einsum(
        "oc,chw->ohw",
        own_mixing,
        lax.all_gather(vertical, "chan", axis=0, tiled=True),
        precision=precise,
    )
    return lax.all_to_all(blended, "band", split_axis=1, concat_axis=2, tiled=True)


LANES = 128
CHUNKS = 2


def split(value):
    high = value.astype(jnp.bfloat16)
    return high, (value - high.astype(jnp.float32)).astype(jnp.bfloat16)


def product(left, right, dims):
    (left_high, left_low), (right_high, right_low) = left, right
    dot = functools.partial(
        lax.dot_general, dimension_numbers=(dims, ((), ())), preferred_element_type=jnp.float32
    )
    return dot(left_high, right_high) + (dot(left_low, right_high) + dot(left_high, right_low))


def filter_table(taps):
    shape = (LANES, LANES)
    lane = lax.broadcasted_iota(jnp.int32, shape, 1)
    row = lax.broadcasted_iota(jnp.int32, shape, 0)
    first, second = (
        pltpu.roll(
            jnp.broadcast_to(taps[:, at : at + LANES], shape), 0, 1, stride=1, stride_axis=0
        )
        for at in (0, LANES)
    )
    last = jnp.broadcast_to(taps[:, 2 * LANES :], shape)
    zero = jnp.zeros(shape, jnp.float32)
    return jnp.concatenate(
        [
            jnp.where(lane >= row, first, zero),
            jnp.where(lane >= row, second, first),
            jnp.where(lane == row, last, jnp.where(lane < row, second, zero)),
        ],
        axis=1,
    )


def mixing_table(column_taps, channel_mix, chans, bands, local_channels, local_rows):
    channels = chans * local_channels
    height = bands * local_rows
    block = local_channels * local_rows
    size = chans * bands * block
    margin = (column_taps.shape[1] - 1) // 2

    def coordinates(index):
        device, inner = index // block, index % block
        return (
            local_channels * (device % chans) + inner // local_rows,
            local_rows * (device // chans) + inner % local_rows,
        )

    tall = (size, channels)
    wide = (channels, size)
    pick_tall = (
        coordinates(lax.broadcasted_iota(jnp.int32, tall, 0))[0]
        == lax.broadcasted_iota(jnp.int32, tall, 1)
    ).astype(jnp.float32)
    pick_wide = (
        coordinates(lax.broadcasted_iota(jnp.int32, wide, 1))[0]
        == lax.broadcasted_iota(jnp.int32, wide, 0)
    ).astype(jnp.float32)
    weights = jnp.dot(
        jnp.dot(pick_tall, channel_mix, precision=precise), pick_wide, precision=precise
    )
    taps = lax.dot_general(
        column_taps[:, : 2 * margin],
        pick_wide,
        (((0,), (0,)), ((), ())),
        precision=precise,
    )
    square = (size, size)
    apart = (
        coordinates(lax.broadcasted_iota(jnp.int32, square, 1))[1]
        - coordinates(lax.broadcasted_iota(jnp.int32, square, 0))[1]
    )
    spread = jnp.zeros(square, jnp.float32)
    for distance in range(1 - height, height):
        at = margin + distance
        spread = jnp.where(apart == distance, taps[at : at + 1, :], spread)
    return weights * spread


def fused_kernel(
    chans, bands, x_hbm, row_hbm, column_hbm, mix_hbm, out_ref,
    x_buf, row_taps, column_taps, channel_mix, tables,
    send_one, recv_one, send_two, mixing,
    ready, x_sem, row_sem, send_sem, recv_one_sem, recv_two_sem,
):
    local_channels, x_rows, _ = x_hbm.shape
    devices, _, block_rows, _ = send_two.shape
    tiles = send_one.shape[1]
    local_rows = block_rows // tiles
    band_rows = x_rows // bands
    others = pl.ds(0, devices - 1)
    chan, band = lax.axis_index("chan"), lax.axis_index("band")
    me = band * chans + chan
    half = bands // 2
    left = band < half

    row_load = pltpu.make_async_copy(row_hbm, row_taps, row_sem)
    row_load.start()
    x_inside = x_buf.at[:, pl.ds(8, x_rows)]
    for c in range(local_channels):
        pltpu.make_async_copy(x_hbm.at[c], x_inside.at[c], x_sem).start()

    low = 2 * chan < chans
    inner = jnp.logical_or(band == half - 1, band == half)
    outer = jnp.logical_not(inner)
    high = jnp.logical_not(low)
    beside = band ^ 1
    across = band ^ 3
    first = jnp.where(inner, across, band ^ 2)
    second = jnp.where(inner, band ^ 2, across)

    def device(to_chan, to_band):
        to_chan = jnp.int32(to_chan) if isinstance(to_chan, int) else to_chan
        return {"chan": to_chan, "band": to_band}, to_band * chans + to_chan

    def whole(to_band):
        return [device(to_chan, to_band) for to_chan in range(chans)]

    own = [device(chan ^ step, band) for step in range(1, chans)]
    middle = chans // 2

    barrier = pltpu.get_barrier_semaphore()
    inner_ready = ready.at[0]
    outer_ready = go_first = ready.at[1]
    go_outer = go_all = ready.at[2]

    def greet(semaphore, *names):
        for name, _slot in names:
            pl.semaphore_signal(
                semaphore, inc=1, device_id=name, device_id_type=pl.DeviceIdType.MESH
            )

    @pl.when(inner)
    def _():
        pl.when(low)(lambda: greet(barrier, *whole(across)[:middle]))
        vouched = jnp.logical_and(left, high)
        pl.when(vouched)(lambda: greet(barrier, *whole(band)[:middle]))
        greet(barrier, *whole(across)[middle:], *whole(beside))

    edge = jnp.zeros((8, LANES), jnp.float32)
    for c in range(local_channels):
        x_buf[c, 0:8, :] = edge
        x_buf[c, x_rows + 8 : x_rows + 16, :] = edge

    right_low = jnp.logical_and(jnp.logical_and(inner, low), jnp.logical_not(left))
    left_low = jnp.logical_and(jnp.logical_and(inner, low), left)

    def meet():
        pl.semaphore_wait(barrier, jnp.where(right_low, middle, chans))

        @pl.when(jnp.logical_and(inner, jnp.logical_not(left)))
        def _():
            pl.when(high)(lambda: greet(inner_ready, *whole(across)[:middle]))

        @pl.when(jnp.logical_and(inner, left))
        def _():
            pl.when(low)(lambda: greet(inner_ready, device(chan, across)))

        @pl.when(outer)
        def _():
            greet(outer_ready, *whole(beside))

    meet_first = jnp.logical_and(high, jnp.logical_not(left))
    pl.when(meet_first)(meet)

    def make_tables(channels):
        for c in channels:
            tables[c, 0:LANES], tables[c, LANES:] = split(filter_table(row_taps[c : c + 1, :]))

    def filter_band(which, channels):
        start = pl.multiple_of(which * band_rows, 8)
        for c in channels:
            wide = x_buf[c, pl.ds(start, band_rows + 16), :]
            window = jnp.concatenate(
                [
                    wide[8 + (k - 1) * local_rows : 8 + (k - 1) * local_rows + band_rows]
                    for k in range(3)
                ],
                axis=1,
            )
            both = lax.dot_general(
                jnp.concatenate(split(window), axis=0),
                tables[c],
                (((1,), (1,)), ((), ())),
                preferred_element_type=jnp.float32,
            )
            filtered = both[:band_rows, :LANES] + (
                both[band_rows:, :LANES] + both[:band_rows, LANES:]
            )
            for to in range(chans):
                for tile in range(tiles):
                    at = (to * tiles + tile) * local_rows
                    send_one[
                        which * chans + to,
                        tile,
                        c * local_rows : (c + 1) * local_rows,
                        :,
                    ] = filtered[at : at + local_rows, :]

    step = tiles // CHUNKS
    block = local_channels * local_rows
    every = (0, block)

    def send(chunk, names, rows=every):
        part, lines = pl.ds(chunk * step, step), pl.ds(rows[0], rows[1])
        for name, slot in names:
            pltpu.make_async_remote_copy(
                src_ref=send_one.at[slot, part, lines],
                dst_ref=recv_one.at[part, me, lines],
                send_sem=send_sem.at[0],
                recv_sem=recv_one_sem.at[chunk],
                device_id=name,
                device_id_type=pl.DeviceIdType.MESH,
            ).start()

    row_load.wait()
    near, far = whole(first)[:middle], whole(first)[middle:]
    both_high = jnp.logical_and(inner, high)
    for piece in range(2):
        channels = range(piece * local_channels // 2, (piece + 1) * local_channels // 2)
        rows = (piece * block // 2, block // 2)
        make_tables(channels)
        if piece == 0:
            pltpu.make_async_copy(x_hbm, x_inside, x_sem).wait()
        filter_band(first, channels)
        if piece == 0:
            pl.when(jnp.logical_not(meet_first))(meet)
        pl.when(inner)(lambda: send(0, near, rows))
        pl.when(both_high)(lambda: send(0, far, rows))
    small_loads = [
        pltpu.make_async_copy(column_hbm, column_taps, row_sem),
        pltpu.make_async_copy(mix_hbm, channel_mix, x_sem),
    ]
    for load in small_loads:
        load.start()
    for chunk in range(1, CHUNKS):
        pl.when(inner)(lambda: send(chunk, near))
        pl.when(both_high)(lambda: send(chunk, far))

    @pl.when(right_low)
    def _():
        pl.semaphore_wait(inner_ready, 1)
        for chunk in range(CHUNKS):
            send(chunk, far)

    for to in (beside, second, band):
        filter_band(to, range(local_channels))

    @pl.when(left_low)
    def _():
        pl.semaphore_wait(inner_ready, middle)
        for chunk in range(CHUNKS):
            send(chunk, far)

    @pl.when(inner)
    def _():
        pl.semaphore_wait(outer_ready, chans)
        greet(go_first, device(chan, beside))
        greet(go_outer, device(chan, across))

    pl.when(inner)(lambda: send(0, whole(beside)))

    @pl.when(outer)
    def _():
        pl.semaphore_wait(go_first, 1)
        send(0, near + far)
        send(0, whole(beside))
        send(0, own)

    @pl.when(inner)
    def _():
        pl.semaphore_wait(go_outer, 1)
        greet(go_all, device(chan, beside))

    @pl.when(outer)
    def _():
        pl.semaphore_wait(go_all, 1)

    send(0, whole(second))
    pl.when(inner)(lambda: send(0, own))
    for chunk in range(1, CHUNKS):
        pl.when(outer)(lambda: send(chunk, near + far))
        send(chunk, whole(second))
        send(chunk, whole(beside))
        send(chunk, own)
    recv_one[:, me] = send_one[me]

    for load in small_loads:
        load.wait()
    table = mixing_table(
        column_taps[...], channel_mix[...], chans, bands, local_channels, local_rows
    )
    mixing[0], mixing[1] = split(table)

    rows = step * local_rows

    def back(chunk, name, slot):
        pltpu.make_async_remote_copy(
            src_ref=send_two.at[slot, :, pl.ds(chunk * rows, rows)],
            dst_ref=out_ref.at[
                :, pl.ds(pl.multiple_of(me * block_rows + chunk * rows, 8), rows)
            ],
            send_sem=send_sem.at[1],
            recv_sem=recv_two_sem,
            device_id=name,
            device_id_type=pl.DeviceIdType.MESH,
        ).start()

    late = band == half
    prompt = jnp.logical_not(late)

    def send_near(chunk):
        for name, slot in whole(beside) + own:
            back(chunk, name, slot)

    def send_back(chunk):
        pl.when(left)(functools.partial(send_near, chunk))
        for k in range(half):
            to = jnp.where(left, half + k, k)
            crossed = [device(chan ^ step, to) for step in reversed(range(chans))]
            for at, (name, slot) in enumerate(crossed if k else whole(to)):
                if k == 0 or at not in (2, 3):
                    back(chunk, name, slot)
                elif chunk < CHUNKS - 1:
                    pl.when(prompt)(functools.partial(back, chunk, name, slot))
                else:
                    for held in range(chunk):
                        pl.when(late)(functools.partial(back, held, name, slot))
                    back(chunk, name, slot)
        pl.when(jnp.logical_not(left))(functools.partial(send_near, chunk))

    for chunk in range(CHUNKS):
        part = pl.ds(chunk * step, step)
        landed = recv_one.at[part, others]
        pltpu.make_async_copy(landed, landed, recv_one_sem.at[chunk]).wait()
        columns = jnp.concatenate(
            [
                recv_one[chunk * step + tile].reshape(mixing.shape[1], LANES)
                for tile in range(step)
            ],
            axis=1,
        )
        mixed = product((mixing[0], mixing[1]), split(columns), ((1,), (0,)))
        for to_device in range(devices):
            for c in range(local_channels):
                at = (to_device * local_channels + c) * local_rows
                for tile in range(step):
                    to = (chunk * step + tile) * local_rows
                    send_two[to_device, c, to : to + local_rows, :] = mixed[
                        at : at + local_rows, tile * LANES : (tile + 1) * LANES
                    ]
        there = pl.ds(pl.multiple_of(me * block_rows + chunk * rows, 8), rows)
        send_back(chunk)
        out_ref[:, there, :] = send_two[me, :, chunk * rows : (chunk + 1) * rows, :]

    sent = send_one.at[others]
    pltpu.make_async_copy(sent, sent, send_sem.at[0]).wait()
    sent = send_two.at[others]
    pltpu.make_async_copy(sent, sent, send_sem.at[1]).wait()
    landed = out_ref.at[:, pl.ds(0, (devices - 1) * block_rows)]
    pltpu.make_async_copy(landed, landed, recv_two_sem).wait()


def fused(chans, bands, slide_region, row_taps, column_taps, channel_mix):
    local_channels, local_rows, width = slide_region.shape
    devices = chans * bands
    total_tiles = width // LANES
    tiles = total_tiles // devices
    block = local_channels * local_rows
    tiled = slide_region.reshape(local_channels, local_rows, total_tiles, LANES)
    tiled = tiled.transpose(0, 2, 1, 3).reshape(local_channels, total_tiles * local_rows, LANES)
    vmem = pl.BlockSpec(memory_space=pltpu.VMEM)
    anywhere = pl.BlockSpec(memory_space=pl.ANY)
    dma = pltpu.SemaphoreType.DMA
    out = pl.pallas_call(
        functools.partial(fused_kernel, chans, bands),
        out_shape=pltpu.VMEM(tiled.shape, jnp.float32),
        in_specs=[anywhere] * 4,
        out_specs=vmem,
        scratch_shapes=[
            pltpu.VMEM((local_channels, tiled.shape[1] + 16, LANES), jnp.float32),
            pltpu.VMEM(row_taps.shape, jnp.float32),
            pltpu.VMEM(column_taps.shape, jnp.float32),
            pltpu.VMEM(channel_mix.shape, jnp.float32),
            pltpu.VMEM((local_channels, 2 * LANES, 3 * LANES), jnp.bfloat16),
            pltpu.VMEM((devices, tiles, block, LANES), jnp.float32),
            pltpu.VMEM((tiles, devices, block, LANES), jnp.float32),
            pltpu.VMEM((devices, local_channels, tiles * local_rows, LANES), jnp.float32),
            pltpu.VMEM((2, devices * block, devices * block), jnp.bfloat16),
            pltpu.SemaphoreType.REGULAR((3,)),
            dma,
            dma,
            dma((2,)),
            dma((CHUNKS,)),
            dma,
        ],
        compiler_params=pltpu.CompilerParams(collective_id=0, has_side_effects=True),
    )(tiled, row_taps, column_taps, channel_mix)
    out = out.reshape(local_channels, total_tiles, local_rows, LANES)
    return out.transpose(0, 2, 1, 3).reshape(slide_region.shape)


def power_of_two(number):
    return number & (number - 1) == 0


def program(chans, bands, slide_region, row_taps, column_taps, channel_mix):
    local_channels, local_rows, width = slide_region.shape
    devices = chans * bands
    margin = (row_taps.shape[1] - 1) // 2
    fits = (
        power_of_two(chans)
        and chans > 1
        and bands == 4
        and width % (devices * LANES * CHUNKS) == 0
        and margin == LANES
        and column_taps.shape[1] == row_taps.shape[1]
        and local_rows == 4
        and local_channels * local_rows % 16 == 0
        and local_rows * bands <= margin
        and width // (devices * LANES * CHUNKS) * local_rows % 8 == 0
        and devices * local_channels * local_rows <= 512
    )
    if fits:
        return fused(chans, bands, slide_region, row_taps, column_taps, channel_mix)
    return on_device(slide_region, row_taps, column_taps, channel_mix)


def solution(mesh):
    in_specs = (P("chan", ("groups", "band"), None), P("chan", None), P(), P())
    out_specs = P("chan", ("groups", "band"), None)
    return jax.shard_map(
        functools.partial(program, mesh.shape["chan"], mesh.shape["band"]),
        mesh=mesh,
        in_specs=in_specs,
        out_specs=out_specs,
        check_vma=False,
    )
```

```python
import functools

import jax
import jax.numpy as jnp
from jax import lax
from jax.experimental import pallas as pl
from jax.experimental.pallas import tpu as pltpu
from jax.sharding import PartitionSpec as P

precise = lax.Precision.HIGHEST


def band_tables(filter_taps, tile_size):
    channels, length = filter_taps.shape
    margin = (length - 1) // 2
    period = 4 * tile_size
    border = 3 * tile_size + length
    widened = jnp.pad(filter_taps, ((0, 0), (border, border)))
    lowest = margin - tile_size + border
    window = widened[:, lowest : lowest + 3 * tile_size]
    vector = jnp.pad(window, ((0, 0), (0, tile_size)))
    repeated = jnp.tile(vector, (1, tile_size))[:, : tile_size * (period - 1)]
    toeplitz = repeated.reshape(channels, tile_size, period - 1)[:, :, : 3 * tile_size]
    stacked = jnp.transpose(toeplitz, (0, 2, 1))
    return stacked.reshape(channels, 3, tile_size, tile_size)


def along_columns(signal, filter_taps):
    tile_size = 128
    tables = band_tables(filter_taps, tile_size)
    channels, row_count, col_count = signal.shape
    tile_count = col_count // tile_size
    tiled = signal.reshape(channels, row_count, tile_count, tile_size)
    padded = jnp.pad(tiled, ((0, 0), (0, 0), (1, 1), (0, 0)))
    result = jnp.einsum(
        "crti,cij->crtj", padded[:, :, 0:tile_count], tables[:, 0], precision=precise
    )
    result = result + jnp.einsum(
        "crti,cij->crtj", padded[:, :, 1 : tile_count + 1], tables[:, 1], precision=precise
    )
    result = result + jnp.einsum(
        "crti,cij->crtj", padded[:, :, 2:], tables[:, 2], precision=precise
    )
    return result.reshape(channels, row_count, col_count)


def along_rows(signal, filter_taps):
    channels, row_count, col_count = signal.shape
    tile_size = 128 if row_count % 128 == 0 else row_count
    tables = band_tables(filter_taps, tile_size)
    tile_count = row_count // tile_size
    tiled = signal.reshape(channels, tile_count, tile_size, col_count)
    padded = jnp.pad(tiled, ((0, 0), (1, 1), (0, 0), (0, 0)))
    result = jnp.einsum("ctiw,cij->ctjw", padded[:, 0:tile_count], tables[:, 0], precision=precise)
    result = result + jnp.einsum(
        "ctiw,cij->ctjw", padded[:, 1 : tile_count + 1], tables[:, 1], precision=precise
    )
    result = result + jnp.einsum("ctiw,cij->ctjw", padded[:, 2:], tables[:, 2], precision=precise)
    return result.reshape(channels, row_count, col_count)


def on_device(slide_region, row_taps, column_taps, channel_mix):
    local_channels = slide_region.shape[0]
    across = along_columns(slide_region, row_taps)
    column_band = lax.all_to_all(across, "band", split_axis=2, concat_axis=1, tiled=True)
    first_channel = lax.axis_index("chan") * local_channels
    own_taps = lax.dynamic_slice_in_dim(column_taps, first_channel, local_channels, 0)
    vertical = along_rows(column_band, own_taps)
    own_mixing = lax.dynamic_slice_in_dim(channel_mix, first_channel, local_channels, 0)
    blended = jnp.einsum(
        "oc,chw->ohw",
        own_mixing,
        lax.all_gather(vertical, "chan", axis=0, tiled=True),
        precision=precise,
    )
    return lax.all_to_all(blended, "band", split_axis=1, concat_axis=2, tiled=True)


LANES = 128
CHUNKS = 2


def split(value):
    high = value.astype(jnp.bfloat16)
    return high, (value - high.astype(jnp.float32)).astype(jnp.bfloat16)


def product(left, right, dims):
    (left_high, left_low), (right_high, right_low) = left, right
    dot = functools.partial(
        lax.dot_general, dimension_numbers=(dims, ((), ())), preferred_element_type=jnp.float32
    )
    return dot(left_high, right_high) + (dot(left_low, right_high) + dot(left_high, right_low))


def filter_table(taps):
    shape = (LANES, LANES)
    lane = lax.broadcasted_iota(jnp.int32, shape, 1)
    row = lax.broadcasted_iota(jnp.int32, shape, 0)
    first, second = (
        pltpu.roll(
            jnp.broadcast_to(taps[:, at : at + LANES], shape), 0, 1, stride=1, stride_axis=0
        )
        for at in (0, LANES)
    )
    last = jnp.broadcast_to(taps[:, 2 * LANES :], shape)
    zero = jnp.zeros(shape, jnp.float32)
    return jnp.concatenate(
        [
            jnp.where(lane >= row, first, zero),
            jnp.where(lane >= row, second, first),
            jnp.where(lane == row, last, jnp.where(lane < row, second, zero)),
        ],
        axis=1,
    )


def mixing_table(column_taps, channel_mix, chans, bands, local_channels, local_rows):
    channels = chans * local_channels
    height = bands * local_rows
    block = local_channels * local_rows
    size = chans * bands * block
    margin = (column_taps.shape[1] - 1) // 2

    def coordinates(index):
        device, inner = index // block, index % block
        return (
            local_channels * (device % chans) + inner // local_rows,
            local_rows * (device // chans) + inner % local_rows,
        )

    tall = (size, channels)
    wide = (channels, size)
    pick_tall = (
        coordinates(lax.broadcasted_iota(jnp.int32, tall, 0))[0]
        == lax.broadcasted_iota(jnp.int32, tall, 1)
    ).astype(jnp.float32)
    pick_wide = (
        coordinates(lax.broadcasted_iota(jnp.int32, wide, 1))[0]
        == lax.broadcasted_iota(jnp.int32, wide, 0)
    ).astype(jnp.float32)
    weights = jnp.dot(
        jnp.dot(pick_tall, channel_mix, precision=precise), pick_wide, precision=precise
    )
    taps = lax.dot_general(
        column_taps[:, : 2 * margin],
        pick_wide,
        (((0,), (0,)), ((), ())),
        precision=precise,
    )
    square = (size, size)
    apart = (
        coordinates(lax.broadcasted_iota(jnp.int32, square, 1))[1]
        - coordinates(lax.broadcasted_iota(jnp.int32, square, 0))[1]
    )
    spread = jnp.zeros(square, jnp.float32)
    for distance in range(1 - height, height):
        at = margin + distance
        spread = jnp.where(apart == distance, taps[at : at + 1, :], spread)
    return weights * spread


def fused_kernel(
    chans, bands, x_hbm, row_hbm, column_hbm, mix_hbm, out_ref,
    x_buf, row_taps, column_taps, channel_mix, tables,
    send_one, recv_one, send_two, mixing,
    ready, x_sem, row_sem, send_sem, recv_one_sem, recv_two_sem,
):
    local_channels, x_rows, _ = x_hbm.shape
    devices, _, block_rows, _ = send_two.shape
    tiles = send_one.shape[1]
    local_rows = block_rows // tiles
    band_rows = x_rows // bands
    others = pl.ds(0, devices - 1)
    chan, band = lax.axis_index("chan"), lax.axis_index("band")
    me = band * chans + chan
    half = bands // 2
    left = band < half

    row_load = pltpu.make_async_copy(row_hbm, row_taps, row_sem)
    row_load.start()
    x_inside = x_buf.at[:, pl.ds(8, x_rows)]
    for c in range(local_channels):
        pltpu.make_async_copy(
            x_hbm.at[c], x_inside.at[c], x_sem.at[2 * c // local_channels]
        ).start()

    low = 2 * chan < chans
    inner = jnp.logical_or(band == half - 1, band == half)
    outer = jnp.logical_not(inner)
    high = jnp.logical_not(low)
    beside = band ^ 1
    across = band ^ 3
    first = jnp.where(inner, across, band ^ 2)
    second = jnp.where(inner, band ^ 2, across)

    def device(to_chan, to_band):
        to_chan = jnp.int32(to_chan) if isinstance(to_chan, int) else to_chan
        return {"chan": to_chan, "band": to_band}, to_band * chans + to_chan

    def whole(to_band):
        return [device(to_chan, to_band) for to_chan in range(chans)]

    own = [device(chan ^ step, band) for step in range(1, chans)]
    middle = chans // 2

    barrier = pltpu.get_barrier_semaphore()
    inner_ready = ready.at[0]
    outer_ready = go_first = ready.at[1]
    go_outer = go_all = ready.at[2]

    def greet(semaphore, *names):
        for name, _slot in names:
            pl.semaphore_signal(
                semaphore, inc=1, device_id=name, device_id_type=pl.DeviceIdType.MESH
            )

    @pl.when(inner)
    def _():
        pl.when(low)(lambda: greet(barrier, *whole(across)[:middle]))
        vouched = jnp.logical_and(left, high)
        pl.when(vouched)(lambda: greet(barrier, *whole(band)[:middle]))
        greet(barrier, *whole(across)[middle:], *whole(beside))

    mixing[...] = jnp.zeros(mixing.shape, mixing.dtype)
    span = devices // local_channels
    for lap in range(3):
        send_two[pl.ds(lap % local_channels * span, span)] = lax.dot_general(
            mixing[0], mixing[1], (((1,), (1,)), ((), ())), preferred_element_type=jnp.float32
        )[:, :LANES].reshape(span, *send_two.shape[1:])
    edge = jnp.zeros((8, LANES), jnp.float32)
    for c in range(local_channels):
        x_buf[c, 0:8, :] = edge
        x_buf[c, x_rows + 8 : x_rows + 16, :] = edge

    right_low = jnp.logical_and(jnp.logical_and(inner, low), jnp.logical_not(left))
    left_low = jnp.logical_and(jnp.logical_and(inner, low), left)

    def meet():
        pl.semaphore_wait(barrier, jnp.where(right_low, middle, chans))

        @pl.when(jnp.logical_and(inner, jnp.logical_not(left)))
        def _():
            pl.when(high)(lambda: greet(inner_ready, *whole(across)[:middle]))

        @pl.when(jnp.logical_and(inner, left))
        def _():
            pl.when(low)(lambda: greet(inner_ready, device(chan, across)))

        @pl.when(outer)
        def _():
            greet(outer_ready, *whole(beside))

    meet_first = jnp.logical_and(high, jnp.logical_not(left))
    pl.when(meet_first)(meet)

    def make_tables(channels):
        for c in channels:
            tables[c, 0:LANES], tables[c, LANES:] = split(filter_table(row_taps[c : c + 1, :]))

    def filter_band(which, channels):
        start = pl.multiple_of(which * band_rows, 8)
        for c in channels:
            wide = x_buf[c, pl.ds(start, band_rows + 16), :]
            window = jnp.concatenate(
                [
                    wide[8 + (k - 1) * local_rows : 8 + (k - 1) * local_rows + band_rows]
                    for k in range(3)
                ],
                axis=1,
            )
            both = lax.dot_general(
                jnp.concatenate(split(window), axis=0),
                tables[c],
                (((1,), (1,)), ((), ())),
                preferred_element_type=jnp.float32,
            )
            filtered = both[:band_rows, :LANES] + (
                both[band_rows:, :LANES] + both[:band_rows, LANES:]
            )
            for to in range(chans):
                for tile in range(tiles):
                    at = (to * tiles + tile) * local_rows
                    send_one[
                        which * chans + to,
                        tile,
                        c * local_rows : (c + 1) * local_rows,
                        :,
                    ] = filtered[at : at + local_rows, :]

    step = tiles // CHUNKS
    block = local_channels * local_rows
    every = (0, block)

    def send(chunk, names, rows=every):
        part, lines = pl.ds(chunk * step, step), pl.ds(rows[0], rows[1])
        for name, slot in names:
            pltpu.make_async_remote_copy(
                src_ref=send_one.at[slot, part, lines],
                dst_ref=recv_one.at[part, me, lines],
                send_sem=send_sem.at[0],
                recv_sem=recv_one_sem.at[chunk],
                device_id=name,
                device_id_type=pl.DeviceIdType.MESH,
            ).start()

    row_load.wait()
    near, far = whole(first)[:middle], whole(first)[middle:]
    both_high = jnp.logical_and(inner, high)
    for piece in range(2):
        channels = range(piece * local_channels // 2, (piece + 1) * local_channels // 2)
        rows = (piece * block // 2, block // 2)
        make_tables(channels)
        loaded = x_inside.at[pl.ds(channels[0], len(channels))]
        pltpu.make_async_copy(loaded, loaded, x_sem.at[piece]).wait()
        filter_band(first, channels)
        if piece == 0:
            pl.when(jnp.logical_not(meet_first))(meet)
        for chunk in range(CHUNKS):
            pl.when(inner)(lambda: send(chunk, near, rows))
            pl.when(both_high)(lambda: send(chunk, far, rows))
    small_loads = [
        pltpu.make_async_copy(column_hbm, column_taps, row_sem),
        pltpu.make_async_copy(mix_hbm, channel_mix, x_sem.at[0]),
    ]
    for load in small_loads:
        load.start()

    @pl.when(right_low)
    def _():
        pl.semaphore_wait(inner_ready, 1)
        for chunk in range(CHUNKS):
            send(chunk, far)

    for to in (beside, second, band):
        filter_band(to, range(local_channels))

    @pl.when(left_low)
    def _():
        pl.semaphore_wait(inner_ready, middle)
        for chunk in range(CHUNKS):
            send(chunk, far)

    @pl.when(inner)
    def _():
        pl.semaphore_wait(outer_ready, chans)
        greet(go_first, device(chan, beside))
        greet(go_outer, device(chan, across))

    pl.when(inner)(lambda: send(0, whole(beside)))

    @pl.when(outer)
    def _():
        pl.semaphore_wait(go_first, 1)
        send(0, near + far)
        send(0, whole(beside))
        send(0, own)

    @pl.when(inner)
    def _():
        pl.semaphore_wait(go_outer, 1)
        greet(go_all, device(chan, beside))

    @pl.when(outer)
    def _():
        pl.semaphore_wait(go_all, 1)

    send(0, whole(second))
    pl.when(inner)(lambda: send(0, own))
    for chunk in range(1, CHUNKS):
        pl.when(outer)(lambda: send(chunk, near + far))
        send(chunk, whole(second))
        send(chunk, whole(beside))
        send(chunk, own)
    recv_one[:, me] = send_one[me]

    for load in small_loads:
        load.wait()
    table = mixing_table(
        column_taps[...], channel_mix[...], chans, bands, local_channels, local_rows
    )
    mixing[0], mixing[1] = split(table)

    rows = step * local_rows

    def back(chunk, name, slot):
        pltpu.make_async_remote_copy(
            src_ref=send_two.at[slot, :, pl.ds(chunk * rows, rows)],
            dst_ref=out_ref.at[
                :, pl.ds(pl.multiple_of(me * block_rows + chunk * rows, 8), rows)
            ],
            send_sem=send_sem.at[1],
            recv_sem=recv_two_sem,
            device_id=name,
            device_id_type=pl.DeviceIdType.MESH,
        ).start()

    late = band == half

    def send_near(chunk):
        for name, slot in whole(beside) + own:
            back(chunk, name, slot)

    def send_back(chunk):
        pl.when(left)(functools.partial(send_near, chunk))
        for k in range(half):
            to = jnp.where(left, half + k, k)
            crossed = [device(chan ^ step, to) for step in reversed(range(chans))]
            for at, (name, slot) in enumerate(crossed if k else whole(to)):
                hold = jnp.logical_and(late, low) if at < 2 else late
                if k == 0:
                    back(chunk, name, slot)
                elif chunk < CHUNKS - 1:
                    pl.when(jnp.logical_not(hold))(functools.partial(back, chunk, name, slot))
                else:
                    for held in range(chunk):
                        pl.when(hold)(functools.partial(back, held, name, slot))
                    back(chunk, name, slot)
        pl.when(jnp.logical_not(left))(functools.partial(send_near, chunk))

    for chunk in range(CHUNKS):
        part = pl.ds(chunk * step, step)
        landed = recv_one.at[part, others]
        pltpu.make_async_copy(landed, landed, recv_one_sem.at[chunk]).wait()
        columns = jnp.concatenate(
            [
                recv_one[chunk * step + tile].reshape(mixing.shape[1], LANES)
                for tile in range(step)
            ],
            axis=1,
        )
        mixed = product((mixing[0], mixing[1]), split(columns), ((1,), (0,)))
        for to_device in range(devices):
            for c in range(local_channels):
                at = (to_device * local_channels + c) * local_rows
                for tile in range(step):
                    to = (chunk * step + tile) * local_rows
                    send_two[to_device, c, to : to + local_rows, :] = mixed[
                        at : at + local_rows, tile * LANES : (tile + 1) * LANES
                    ]
        there = pl.ds(pl.multiple_of(me * block_rows + chunk * rows, 8), rows)
        send_back(chunk)
        out_ref[:, there, :] = send_two[me, :, chunk * rows : (chunk + 1) * rows, :]

    sent = send_one.at[others]
    pltpu.make_async_copy(sent, sent, send_sem.at[0]).wait()
    sent = send_two.at[others]
    pltpu.make_async_copy(sent, sent, send_sem.at[1]).wait()
    landed = out_ref.at[:, pl.ds(0, (devices - 1) * block_rows)]
    pltpu.make_async_copy(landed, landed, recv_two_sem).wait()


def fused(chans, bands, slide_region, row_taps, column_taps, channel_mix):
    local_channels, local_rows, width = slide_region.shape
    devices = chans * bands
    total_tiles = width // LANES
    tiles = total_tiles // devices
    block = local_channels * local_rows
    tiled = slide_region.reshape(local_channels, local_rows, total_tiles, LANES)
    tiled = tiled.transpose(0, 2, 1, 3).reshape(local_channels, total_tiles * local_rows, LANES)
    vmem = pl.BlockSpec(memory_space=pltpu.VMEM)
    anywhere = pl.BlockSpec(memory_space=pl.ANY)
    dma = pltpu.SemaphoreType.DMA
    out = pl.pallas_call(
        functools.partial(fused_kernel, chans, bands),
        out_shape=pltpu.VMEM(tiled.shape, jnp.float32),
        in_specs=[anywhere] * 4,
        out_specs=vmem,
        scratch_shapes=[
            pltpu.VMEM((local_channels, tiled.shape[1] + 16, LANES), jnp.float32),
            pltpu.VMEM(row_taps.shape, jnp.float32),
            pltpu.VMEM(column_taps.shape, jnp.float32),
            pltpu.VMEM(channel_mix.shape, jnp.float32),
            pltpu.VMEM((local_channels, 2 * LANES, 3 * LANES), jnp.bfloat16),
            pltpu.VMEM((devices, tiles, block, LANES), jnp.float32),
            pltpu.VMEM((tiles, devices, block, LANES), jnp.float32),
            pltpu.VMEM((devices, local_channels, tiles * local_rows, LANES), jnp.float32),
            pltpu.VMEM((2, devices * block, devices * block), jnp.bfloat16),
            pltpu.SemaphoreType.REGULAR((3,)),
            dma((2,)),
            dma,
            dma((2,)),
            dma((CHUNKS,)),
            dma,
        ],
        compiler_params=pltpu.CompilerParams(collective_id=0, has_side_effects=True),
    )(tiled, row_taps, column_taps, channel_mix)
    out = out.reshape(local_channels, total_tiles, local_rows, LANES)
    return out.transpose(0, 2, 1, 3).reshape(slide_region.shape)


def power_of_two(number):
    return number & (number - 1) == 0


def program(chans, bands, slide_region, row_taps, column_taps, channel_mix):
    local_channels, local_rows, width = slide_region.shape
    devices = chans * bands
    margin = (row_taps.shape[1] - 1) // 2
    fits = (
        power_of_two(chans)
        and chans > 1
        and bands == 4
        and width % (devices * LANES * CHUNKS) == 0
        and margin == LANES
        and column_taps.shape[1] == row_taps.shape[1]
        and local_rows == 4
        and local_channels * local_rows % 16 == 0
        and local_rows * bands <= margin
        and width // (devices * LANES * CHUNKS) * local_rows % 8 == 0
        and devices * local_channels * local_rows <= 512
    )
    if fits:
        return fused(chans, bands, slide_region, row_taps, column_taps, channel_mix)
    return on_device(slide_region, row_taps, column_taps, channel_mix)


def solution(mesh):
    in_specs = (P("chan", ("groups", "band"), None), P("chan", None), P(), P())
    out_specs = P("chan", ("groups", "band"), None)
    return jax.shard_map(
        functools.partial(program, mesh.shape["chan"], mesh.shape["band"]),
        mesh=mesh,
        in_specs=in_specs,
        out_specs=out_specs,
        check_vma=False,
    )
```

```python
import functools

import jax
import jax.numpy as jnp
from jax import lax
from jax.experimental import pallas as pl
from jax.experimental.pallas import tpu as pltpu
from jax.sharding import PartitionSpec as P

precise = lax.Precision.HIGHEST


def band_tables(filter_taps, tile_size):
    channels, length = filter_taps.shape
    margin = (length - 1) // 2
    period = 4 * tile_size
    border = 3 * tile_size + length
    widened = jnp.pad(filter_taps, ((0, 0), (border, border)))
    lowest = margin - tile_size + border
    window = widened[:, lowest : lowest + 3 * tile_size]
    vector = jnp.pad(window, ((0, 0), (0, tile_size)))
    repeated = jnp.tile(vector, (1, tile_size))[:, : tile_size * (period - 1)]
    toeplitz = repeated.reshape(channels, tile_size, period - 1)[:, :, : 3 * tile_size]
    stacked = jnp.transpose(toeplitz, (0, 2, 1))
    return stacked.reshape(channels, 3, tile_size, tile_size)


def along_columns(signal, filter_taps):
    tile_size = 128
    tables = band_tables(filter_taps, tile_size)
    channels, row_count, col_count = signal.shape
    tile_count = col_count // tile_size
    tiled = signal.reshape(channels, row_count, tile_count, tile_size)
    padded = jnp.pad(tiled, ((0, 0), (0, 0), (1, 1), (0, 0)))
    result = jnp.einsum(
        "crti,cij->crtj", padded[:, :, 0:tile_count], tables[:, 0], precision=precise
    )
    result = result + jnp.einsum(
        "crti,cij->crtj", padded[:, :, 1 : tile_count + 1], tables[:, 1], precision=precise
    )
    result = result + jnp.einsum(
        "crti,cij->crtj", padded[:, :, 2:], tables[:, 2], precision=precise
    )
    return result.reshape(channels, row_count, col_count)


def along_rows(signal, filter_taps):
    channels, row_count, col_count = signal.shape
    tile_size = 128 if row_count % 128 == 0 else row_count
    tables = band_tables(filter_taps, tile_size)
    tile_count = row_count // tile_size
    tiled = signal.reshape(channels, tile_count, tile_size, col_count)
    padded = jnp.pad(tiled, ((0, 0), (1, 1), (0, 0), (0, 0)))
    result = jnp.einsum("ctiw,cij->ctjw", padded[:, 0:tile_count], tables[:, 0], precision=precise)
    result = result + jnp.einsum(
        "ctiw,cij->ctjw", padded[:, 1 : tile_count + 1], tables[:, 1], precision=precise
    )
    result = result + jnp.einsum("ctiw,cij->ctjw", padded[:, 2:], tables[:, 2], precision=precise)
    return result.reshape(channels, row_count, col_count)


def on_device(slide_region, row_taps, column_taps, channel_mix):
    local_channels = slide_region.shape[0]
    across = along_columns(slide_region, row_taps)
    column_band = lax.all_to_all(across, "band", split_axis=2, concat_axis=1, tiled=True)
    first_channel = lax.axis_index("chan") * local_channels
    own_taps = lax.dynamic_slice_in_dim(column_taps, first_channel, local_channels, 0)
    vertical = along_rows(column_band, own_taps)
    own_mixing = lax.dynamic_slice_in_dim(channel_mix, first_channel, local_channels, 0)
    blended = jnp.einsum(
        "oc,chw->ohw",
        own_mixing,
        lax.all_gather(vertical, "chan", axis=0, tiled=True),
        precision=precise,
    )
    return lax.all_to_all(blended, "band", split_axis=1, concat_axis=2, tiled=True)


LANES = 128
CHUNKS = 2


def split(value):
    high = value.astype(jnp.bfloat16)
    return high, (value - high.astype(jnp.float32)).astype(jnp.bfloat16)


def product(left, right, dims):
    (left_high, left_low), (right_high, right_low) = left, right
    dot = functools.partial(
        lax.dot_general, dimension_numbers=(dims, ((), ())), preferred_element_type=jnp.float32
    )
    return dot(left_high, right_high) + (dot(left_low, right_high) + dot(left_high, right_low))


def filter_table(taps):
    shape = (LANES, LANES)
    lane = lax.broadcasted_iota(jnp.int32, shape, 1)
    row = lax.broadcasted_iota(jnp.int32, shape, 0)
    first, second = (
        pltpu.roll(
            jnp.broadcast_to(taps[:, at : at + LANES], shape), 0, 1, stride=1, stride_axis=0
        )
        for at in (0, LANES)
    )
    last = jnp.broadcast_to(taps[:, 2 * LANES :], shape)
    zero = jnp.zeros(shape, jnp.float32)
    return jnp.concatenate(
        [
            jnp.where(lane >= row, first, zero),
            jnp.where(lane >= row, second, first),
            jnp.where(lane == row, last, jnp.where(lane < row, second, zero)),
        ],
        axis=1,
    )


def mixing_table(column_taps, channel_mix, chans, bands, local_channels, local_rows):
    channels = chans * local_channels
    height = bands * local_rows
    block = local_channels * local_rows
    size = chans * bands * block
    margin = (column_taps.shape[1] - 1) // 2

    def coordinates(index):
        device, inner = index // block, index % block
        return (
            local_channels * (device % chans) + inner // local_rows,
            local_rows * (device // chans) + inner % local_rows,
        )

    tall = (size, channels)
    wide = (channels, size)
    pick_tall = (
        coordinates(lax.broadcasted_iota(jnp.int32, tall, 0))[0]
        == lax.broadcasted_iota(jnp.int32, tall, 1)
    ).astype(jnp.float32)
    pick_wide = (
        coordinates(lax.broadcasted_iota(jnp.int32, wide, 1))[0]
        == lax.broadcasted_iota(jnp.int32, wide, 0)
    ).astype(jnp.float32)
    weights = jnp.dot(
        jnp.dot(pick_tall, channel_mix, precision=precise), pick_wide, precision=precise
    )
    taps = lax.dot_general(
        column_taps[:, : 2 * margin],
        pick_wide,
        (((0,), (0,)), ((), ())),
        precision=precise,
    )
    square = (size, size)
    apart = (
        coordinates(lax.broadcasted_iota(jnp.int32, square, 1))[1]
        - coordinates(lax.broadcasted_iota(jnp.int32, square, 0))[1]
    )
    spread = jnp.zeros(square, jnp.float32)
    for distance in range(1 - height, height):
        at = margin + distance
        spread = jnp.where(apart == distance, taps[at : at + 1, :], spread)
    return weights * spread


def fused_kernel(
    chans, bands, x_hbm, row_hbm, column_hbm, mix_hbm, out_ref,
    x_buf, row_taps, column_taps, channel_mix, tables,
    send_one, recv_one, send_two, mixing,
    ready, x_sem, row_sem, send_sem, recv_one_sem, recv_two_sem,
):
    local_channels, x_rows, _ = x_hbm.shape
    devices, _, block_rows, _ = send_two.shape
    tiles = send_one.shape[1]
    local_rows = block_rows // tiles
    band_rows = x_rows // bands
    others = pl.ds(0, devices - 1)
    chan, band = lax.axis_index("chan"), lax.axis_index("band")
    me = band * chans + chan
    half = bands // 2
    left = band < half

    row_load = pltpu.make_async_copy(row_hbm, row_taps, row_sem)
    row_load.start()
    x_inside = x_buf.at[:, pl.ds(8, x_rows)]
    for c in range(local_channels):
        pltpu.make_async_copy(
            x_hbm.at[c], x_inside.at[c], x_sem.at[2 * c // local_channels]
        ).start()

    low = 2 * chan < chans
    inner = jnp.logical_or(band == half - 1, band == half)
    outer = jnp.logical_not(inner)
    high = jnp.logical_not(low)
    beside = band ^ 1
    across = band ^ 3
    first = jnp.where(inner, across, band ^ 2)
    second = jnp.where(inner, band ^ 2, across)

    def device(to_chan, to_band):
        to_chan = jnp.int32(to_chan) if isinstance(to_chan, int) else to_chan
        return {"chan": to_chan, "band": to_band}, to_band * chans + to_chan

    def whole(to_band):
        return [device(to_chan, to_band) for to_chan in range(chans)]

    own = [device(chan ^ step, band) for step in range(1, chans)]
    middle = chans // 2

    barrier = pltpu.get_barrier_semaphore()
    inner_ready = ready.at[0]
    outer_ready = go_first = ready.at[1]
    go_outer = go_all = ready.at[2]

    def greet(semaphore, *names):
        for name, _slot in names:
            pl.semaphore_signal(
                semaphore, inc=1, device_id=name, device_id_type=pl.DeviceIdType.MESH
            )

    @pl.when(inner)
    def _():
        pl.when(low)(lambda: greet(barrier, *whole(across)[:middle]))
        vouched = jnp.logical_and(left, high)
        pl.when(vouched)(lambda: greet(barrier, *whole(band)[:middle]))
        greet(barrier, *whole(across)[middle:], *whole(beside))

    mixing[...] = jnp.zeros(mixing.shape, mixing.dtype)
    span = devices // local_channels
    for lap in range(3):
        send_two[pl.ds(lap % local_channels * span, span)] = lax.dot_general(
            mixing[0], mixing[1], (((1,), (1,)), ((), ())), preferred_element_type=jnp.float32
        )[:, :LANES].reshape(span, *send_two.shape[1:])
    edge = jnp.zeros((8, LANES), jnp.float32)
    for c in range(local_channels):
        x_buf[c, 0:8, :] = edge
        x_buf[c, x_rows + 8 : x_rows + 16, :] = edge

    right_low = jnp.logical_and(jnp.logical_and(inner, low), jnp.logical_not(left))
    left_low = jnp.logical_and(jnp.logical_and(inner, low), left)

    def meet():
        pl.semaphore_wait(barrier, jnp.where(right_low, middle, chans))

        @pl.when(jnp.logical_and(inner, jnp.logical_not(left)))
        def _():
            pl.when(high)(lambda: greet(inner_ready, *whole(across)[:middle]))

        @pl.when(jnp.logical_and(inner, left))
        def _():
            pl.when(low)(lambda: greet(inner_ready, device(chan, across)))

        @pl.when(outer)
        def _():
            greet(outer_ready, *whole(beside))

    meet_first = jnp.logical_and(high, jnp.logical_not(left))
    pl.when(meet_first)(meet)

    def make_tables(channels):
        for c in channels:
            tables[c, 0:LANES], tables[c, LANES:] = split(filter_table(row_taps[c : c + 1, :]))

    def filter_band(which, channels):
        start = pl.multiple_of(which * band_rows, 8)
        for c in channels:
            wide = x_buf[c, pl.ds(start, band_rows + 16), :]
            window = jnp.concatenate(
                [
                    wide[8 + (k - 1) * local_rows : 8 + (k - 1) * local_rows + band_rows]
                    for k in range(3)
                ],
                axis=1,
            )
            both = lax.dot_general(
                jnp.concatenate(split(window), axis=0),
                tables[c],
                (((1,), (1,)), ((), ())),
                preferred_element_type=jnp.float32,
            )
            filtered = both[:band_rows, :LANES] + (
                both[band_rows:, :LANES] + both[:band_rows, LANES:]
            )
            for to in range(chans):
                for tile in range(tiles):
                    at = (to * tiles + tile) * local_rows
                    send_one[
                        which * chans + to,
                        tile,
                        c * local_rows : (c + 1) * local_rows,
                        :,
                    ] = filtered[at : at + local_rows, :]

    step = tiles // CHUNKS
    block = local_channels * local_rows
    every = (0, block)

    def send(chunk, names, rows=every):
        part, lines = pl.ds(chunk * step, step), pl.ds(rows[0], rows[1])
        for name, slot in names:
            pltpu.make_async_remote_copy(
                src_ref=send_one.at[slot, part, lines],
                dst_ref=recv_one.at[part, me, lines],
                send_sem=send_sem.at[0],
                recv_sem=recv_one_sem.at[chunk],
                device_id=name,
                device_id_type=pl.DeviceIdType.MESH,
            ).start()

    row_load.wait()
    near, far = whole(first)[:middle], whole(first)[middle:]
    both_high = jnp.logical_and(inner, high)
    for piece in range(2):
        channels = range(piece * local_channels // 2, (piece + 1) * local_channels // 2)
        rows = (piece * block // 2, block // 2)
        make_tables(channels)
        loaded = x_inside.at[pl.ds(channels[0], len(channels))]
        pltpu.make_async_copy(loaded, loaded, x_sem.at[piece]).wait()
        filter_band(first, channels)
        if piece == 0:
            pl.when(jnp.logical_not(meet_first))(meet)
        for chunk in range(CHUNKS):
            pl.when(inner)(lambda: send(chunk, near, rows))
            pl.when(both_high)(lambda: send(chunk, far, rows))
    small_loads = [
        pltpu.make_async_copy(column_hbm, column_taps, row_sem),
        pltpu.make_async_copy(mix_hbm, channel_mix, x_sem.at[0]),
    ]
    for load in small_loads:
        load.start()

    @pl.when(right_low)
    def _():
        pl.semaphore_wait(inner_ready, 1)
        for chunk in range(CHUNKS):
            send(chunk, far)

    for to in (beside, second, band):
        filter_band(to, range(local_channels))

    @pl.when(left_low)
    def _():
        pl.semaphore_wait(inner_ready, middle)
        for chunk in range(CHUNKS):
            send(chunk, far)

    @pl.when(inner)
    def _():
        pl.semaphore_wait(outer_ready, chans)
        greet(go_first, device(chan, beside))
        greet(go_outer, device(chan, across))

    pl.when(inner)(lambda: send(0, whole(beside)))

    @pl.when(outer)
    def _():
        pl.semaphore_wait(go_first, 1)
        send(0, near + far)
        send(0, whole(beside))
        send(0, own)

    @pl.when(inner)
    def _():
        pl.semaphore_wait(go_outer, 1)
        greet(go_all, device(chan, beside))

    @pl.when(outer)
    def _():
        pl.semaphore_wait(go_all, 1)

    send(0, whole(second))
    pl.when(inner)(lambda: send(0, own))
    for chunk in range(1, CHUNKS):
        pl.when(outer)(lambda: send(chunk, near + far))
        send(chunk, whole(second))
        send(chunk, whole(beside))
        send(chunk, own)
    recv_one[:, me] = send_one[me]

    for load in small_loads:
        load.wait()
    table = mixing_table(
        column_taps[...], channel_mix[...], chans, bands, local_channels, local_rows
    )
    mixing[0], mixing[1] = split(table)

    rows = step * local_rows

    def back(chunk, name, slot):
        pltpu.make_async_remote_copy(
            src_ref=send_two.at[slot, :, pl.ds(chunk * rows, rows)],
            dst_ref=out_ref.at[
                :, pl.ds(pl.multiple_of(me * block_rows + chunk * rows, 8), rows)
            ],
            send_sem=send_sem.at[1],
            recv_sem=recv_two_sem,
            device_id=name,
            device_id_type=pl.DeviceIdType.MESH,
        ).start()

    late = band == half
    near_first = jnp.logical_or(left, band > half)

    def send_near(chunk):
        for name, slot in whole(beside) + own:
            back(chunk, name, slot)

    def send_back(chunk):
        early = near_first if chunk else left
        pl.when(early)(functools.partial(send_near, chunk))
        for k in range(half):
            to = jnp.where(left, half + k, k)
            crossed = [device(chan ^ step, to) for step in reversed(range(chans))]
            for at, (name, slot) in enumerate(crossed if k else whole(to)):
                hold = jnp.logical_and(late, low) if at < 2 else late
                if k == 0:
                    back(chunk, name, slot)
                elif chunk < CHUNKS - 1:
                    pl.when(jnp.logical_not(hold))(functools.partial(back, chunk, name, slot))
                else:
                    for held in range(chunk):
                        pl.when(hold)(functools.partial(back, held, name, slot))
                    back(chunk, name, slot)
        pl.when(jnp.logical_not(early))(functools.partial(send_near, chunk))

    for chunk in range(CHUNKS):
        part = pl.ds(chunk * step, step)
        landed = recv_one.at[part, others]
        pltpu.make_async_copy(landed, landed, recv_one_sem.at[chunk]).wait()
        columns = jnp.concatenate(
            [
                recv_one[chunk * step + tile].reshape(mixing.shape[1], LANES)
                for tile in range(step)
            ],
            axis=1,
        )
        mixed = product((mixing[0], mixing[1]), split(columns), ((1,), (0,)))
        for to_device in range(devices):
            for c in range(local_channels):
                at = (to_device * local_channels + c) * local_rows
                for tile in range(step):
                    to = (chunk * step + tile) * local_rows
                    send_two[to_device, c, to : to + local_rows, :] = mixed[
                        at : at + local_rows, tile * LANES : (tile + 1) * LANES
                    ]
        there = pl.ds(pl.multiple_of(me * block_rows + chunk * rows, 8), rows)
        send_back(chunk)
        out_ref[:, there, :] = send_two[me, :, chunk * rows : (chunk + 1) * rows, :]

    sent = send_one.at[others]
    pltpu.make_async_copy(sent, sent, send_sem.at[0]).wait()
    sent = send_two.at[others]
    pltpu.make_async_copy(sent, sent, send_sem.at[1]).wait()
    landed = out_ref.at[:, pl.ds(0, (devices - 1) * block_rows)]
    pltpu.make_async_copy(landed, landed, recv_two_sem).wait()


def fused(chans, bands, slide_region, row_taps, column_taps, channel_mix):
    local_channels, local_rows, width = slide_region.shape
    devices = chans * bands
    total_tiles = width // LANES
    tiles = total_tiles // devices
    block = local_channels * local_rows
    tiled = slide_region.reshape(local_channels, local_rows, total_tiles, LANES)
    tiled = tiled.transpose(0, 2, 1, 3).reshape(local_channels, total_tiles * local_rows, LANES)
    vmem = pl.BlockSpec(memory_space=pltpu.VMEM)
    anywhere = pl.BlockSpec(memory_space=pl.ANY)
    dma = pltpu.SemaphoreType.DMA
    out = pl.pallas_call(
        functools.partial(fused_kernel, chans, bands),
        out_shape=pltpu.VMEM(tiled.shape, jnp.float32),
        in_specs=[anywhere] * 4,
        out_specs=vmem,
        scratch_shapes=[
            pltpu.VMEM((local_channels, tiled.shape[1] + 16, LANES), jnp.float32),
            pltpu.VMEM(row_taps.shape, jnp.float32),
            pltpu.VMEM(column_taps.shape, jnp.float32),
            pltpu.VMEM(channel_mix.shape, jnp.float32),
            pltpu.VMEM((local_channels, 2 * LANES, 3 * LANES), jnp.bfloat16),
            pltpu.VMEM((devices, tiles, block, LANES), jnp.float32),
            pltpu.VMEM((tiles, devices, block, LANES), jnp.float32),
            pltpu.VMEM((devices, local_channels, tiles * local_rows, LANES), jnp.float32),
            pltpu.VMEM((2, devices * block, devices * block), jnp.bfloat16),
            pltpu.SemaphoreType.REGULAR((3,)),
            dma((2,)),
            dma,
            dma((2,)),
            dma((CHUNKS,)),
            dma,
        ],
        compiler_params=pltpu.CompilerParams(collective_id=0, has_side_effects=True),
    )(tiled, row_taps, column_taps, channel_mix)
    out = out.reshape(local_channels, total_tiles, local_rows, LANES)
    return out.transpose(0, 2, 1, 3).reshape(slide_region.shape)


def power_of_two(number):
    return number & (number - 1) == 0


def program(chans, bands, slide_region, row_taps, column_taps, channel_mix):
    local_channels, local_rows, width = slide_region.shape
    devices = chans * bands
    margin = (row_taps.shape[1] - 1) // 2
    fits = (
        power_of_two(chans)
        and chans > 1
        and bands == 4
        and width % (devices * LANES * CHUNKS) == 0
        and margin == LANES
        and column_taps.shape[1] == row_taps.shape[1]
        and local_rows == 4
        and local_channels * local_rows % 16 == 0
        and local_rows * bands <= margin
        and width // (devices * LANES * CHUNKS) * local_rows % 8 == 0
        and devices * local_channels * local_rows <= 512
    )
    if fits:
        return fused(chans, bands, slide_region, row_taps, column_taps, channel_mix)
    return on_device(slide_region, row_taps, column_taps, channel_mix)


def solution(mesh):
    in_specs = (P("chan", ("groups", "band"), None), P("chan", None), P(), P())
    out_specs = P("chan", ("groups", "band"), None)
    return jax.shard_map(
        functools.partial(program, mesh.shape["chan"], mesh.shape["band"]),
        mesh=mesh,
        in_specs=in_specs,
        out_specs=out_specs,
        check_vma=False,
    )
```

```python
import functools

import jax
import jax.numpy as jnp
from jax import lax
from jax.experimental import pallas as pl
from jax.experimental.pallas import tpu as pltpu
from jax.sharding import PartitionSpec as P

precise = lax.Precision.HIGHEST


def band_tables(filter_taps, tile_size):
    channels, length = filter_taps.shape
    margin = (length - 1) // 2
    period = 4 * tile_size
    border = 3 * tile_size + length
    widened = jnp.pad(filter_taps, ((0, 0), (border, border)))
    lowest = margin - tile_size + border
    window = widened[:, lowest : lowest + 3 * tile_size]
    vector = jnp.pad(window, ((0, 0), (0, tile_size)))
    repeated = jnp.tile(vector, (1, tile_size))[:, : tile_size * (period - 1)]
    toeplitz = repeated.reshape(channels, tile_size, period - 1)[:, :, : 3 * tile_size]
    stacked = jnp.transpose(toeplitz, (0, 2, 1))
    return stacked.reshape(channels, 3, tile_size, tile_size)


def along_columns(signal, filter_taps):
    tile_size = 128
    tables = band_tables(filter_taps, tile_size)
    channels, row_count, col_count = signal.shape
    tile_count = col_count // tile_size
    tiled = signal.reshape(channels, row_count, tile_count, tile_size)
    padded = jnp.pad(tiled, ((0, 0), (0, 0), (1, 1), (0, 0)))
    result = jnp.einsum(
        "crti,cij->crtj", padded[:, :, 0:tile_count], tables[:, 0], precision=precise
    )
    result = result + jnp.einsum(
        "crti,cij->crtj", padded[:, :, 1 : tile_count + 1], tables[:, 1], precision=precise
    )
    result = result + jnp.einsum(
        "crti,cij->crtj", padded[:, :, 2:], tables[:, 2], precision=precise
    )
    return result.reshape(channels, row_count, col_count)


def along_rows(signal, filter_taps):
    channels, row_count, col_count = signal.shape
    tile_size = 128 if row_count % 128 == 0 else row_count
    tables = band_tables(filter_taps, tile_size)
    tile_count = row_count // tile_size
    tiled = signal.reshape(channels, tile_count, tile_size, col_count)
    padded = jnp.pad(tiled, ((0, 0), (1, 1), (0, 0), (0, 0)))
    result = jnp.einsum("ctiw,cij->ctjw", padded[:, 0:tile_count], tables[:, 0], precision=precise)
    result = result + jnp.einsum(
        "ctiw,cij->ctjw", padded[:, 1 : tile_count + 1], tables[:, 1], precision=precise
    )
    result = result + jnp.einsum("ctiw,cij->ctjw", padded[:, 2:], tables[:, 2], precision=precise)
    return result.reshape(channels, row_count, col_count)


def on_device(slide_region, row_taps, column_taps, channel_mix):
    local_channels = slide_region.shape[0]
    across = along_columns(slide_region, row_taps)
    column_band = lax.all_to_all(across, "band", split_axis=2, concat_axis=1, tiled=True)
    first_channel = lax.axis_index("chan") * local_channels
    own_taps = lax.dynamic_slice_in_dim(column_taps, first_channel, local_channels, 0)
    vertical = along_rows(column_band, own_taps)
    own_mixing = lax.dynamic_slice_in_dim(channel_mix, first_channel, local_channels, 0)
    blended = jnp.einsum(
        "oc,chw->ohw",
        own_mixing,
        lax.all_gather(vertical, "chan", axis=0, tiled=True),
        precision=precise,
    )
    return lax.all_to_all(blended, "band", split_axis=1, concat_axis=2, tiled=True)


LANES = 128
CHUNKS = 2


def split(value):
    high = value.astype(jnp.bfloat16)
    return high, (value - high.astype(jnp.float32)).astype(jnp.bfloat16)


def product(left, right, dims):
    (left_high, left_low), (right_high, right_low) = left, right
    dot = functools.partial(
        lax.dot_general, dimension_numbers=(dims, ((), ())), preferred_element_type=jnp.float32
    )
    return dot(left_high, right_high) + (dot(left_low, right_high) + dot(left_high, right_low))


def filter_table(taps):
    shape = (LANES, LANES)
    lane = lax.broadcasted_iota(jnp.int32, shape, 1)
    row = lax.broadcasted_iota(jnp.int32, shape, 0)
    first, second = (
        pltpu.roll(
            jnp.broadcast_to(taps[:, at : at + LANES], shape), 0, 1, stride=1, stride_axis=0
        )
        for at in (0, LANES)
    )
    last = jnp.broadcast_to(taps[:, 2 * LANES :], shape)
    zero = jnp.zeros(shape, jnp.float32)
    return jnp.concatenate(
        [
            jnp.where(lane >= row, first, zero),
            jnp.where(lane >= row, second, first),
            jnp.where(lane == row, last, jnp.where(lane < row, second, zero)),
        ],
        axis=1,
    )


def mixing_table(column_taps, channel_mix, chans, bands, local_channels, local_rows):
    channels = chans * local_channels
    height = bands * local_rows
    block = local_channels * local_rows
    size = chans * bands * block
    margin = (column_taps.shape[1] - 1) // 2

    def coordinates(index):
        device, inner = index // block, index % block
        return (
            local_channels * (device % chans) + inner // local_rows,
            local_rows * (device // chans) + inner % local_rows,
        )

    tall = (size, channels)
    wide = (channels, size)
    pick_tall = (
        coordinates(lax.broadcasted_iota(jnp.int32, tall, 0))[0]
        == lax.broadcasted_iota(jnp.int32, tall, 1)
    ).astype(jnp.float32)
    pick_wide = (
        coordinates(lax.broadcasted_iota(jnp.int32, wide, 1))[0]
        == lax.broadcasted_iota(jnp.int32, wide, 0)
    ).astype(jnp.float32)
    weights = jnp.dot(
        jnp.dot(pick_tall, channel_mix, precision=precise), pick_wide, precision=precise
    )
    taps = lax.dot_general(
        column_taps[:, : 2 * margin],
        pick_wide,
        (((0,), (0,)), ((), ())),
        precision=precise,
    )
    square = (size, size)
    apart = (
        coordinates(lax.broadcasted_iota(jnp.int32, square, 1))[1]
        - coordinates(lax.broadcasted_iota(jnp.int32, square, 0))[1]
    )
    spread = jnp.zeros(square, jnp.float32)
    for distance in range(1 - height, height):
        at = margin + distance
        spread = jnp.where(apart == distance, taps[at : at + 1, :], spread)
    return weights * spread


def fused_kernel(
    chans, bands, x_hbm, row_hbm, column_hbm, mix_hbm, out_ref,
    x_buf, row_taps, column_taps, channel_mix, tables,
    send_one, recv_one, send_two, mixing,
    ready, x_sem, row_sem, send_sem, recv_one_sem, recv_two_sem,
):
    local_channels, x_rows, _ = x_hbm.shape
    devices, _, block_rows, _ = send_two.shape
    tiles = send_one.shape[1]
    local_rows = block_rows // tiles
    band_rows = x_rows // bands
    others = pl.ds(0, devices - 1)
    chan, band = lax.axis_index("chan"), lax.axis_index("band")
    me = band * chans + chan
    half = bands // 2
    left = band < half

    row_load = pltpu.make_async_copy(row_hbm, row_taps, row_sem)
    row_load.start()
    x_inside = x_buf.at[:, pl.ds(8, x_rows)]
    for c in range(local_channels):
        pltpu.make_async_copy(
            x_hbm.at[c], x_inside.at[c], x_sem.at[2 * c // local_channels]
        ).start()

    low = 2 * chan < chans
    inner = jnp.logical_or(band == half - 1, band == half)
    outer = jnp.logical_not(inner)
    high = jnp.logical_not(low)
    beside = band ^ 1
    across = band ^ 3
    first = jnp.where(inner, across, band ^ 2)
    second = jnp.where(inner, band ^ 2, across)

    def device(to_chan, to_band):
        to_chan = jnp.int32(to_chan) if isinstance(to_chan, int) else to_chan
        return {"chan": to_chan, "band": to_band}, to_band * chans + to_chan

    def whole(to_band):
        return [device(to_chan, to_band) for to_chan in range(chans)]

    own = [device(chan ^ step, band) for step in range(1, chans)]
    middle = chans // 2

    barrier = pltpu.get_barrier_semaphore()
    inner_ready = ready.at[0]
    outer_ready = go_first = ready.at[1]
    go_outer = go_all = ready.at[2]

    def greet(semaphore, *names):
        for name, _slot in names:
            pl.semaphore_signal(
                semaphore, inc=1, device_id=name, device_id_type=pl.DeviceIdType.MESH
            )

    @pl.when(inner)
    def _():
        pl.when(low)(lambda: greet(barrier, *whole(across)[:middle]))
        vouched = jnp.logical_and(left, high)
        pl.when(vouched)(lambda: greet(barrier, *whole(band)[:middle]))
        greet(barrier, *whole(across)[middle:], *whole(beside))

    mixing[...] = jnp.zeros(mixing.shape, mixing.dtype)
    span = devices // local_channels
    for lap in range(3):
        send_two[pl.ds(lap % local_channels * span, span)] = lax.dot_general(
            mixing[0], mixing[1], (((1,), (1,)), ((), ())), preferred_element_type=jnp.float32
        )[:, :LANES].reshape(span, *send_two.shape[1:])
    edge = jnp.zeros((8, LANES), jnp.float32)
    for c in range(local_channels):
        x_buf[c, 0:8, :] = edge
        x_buf[c, x_rows + 8 : x_rows + 16, :] = edge

    right_low = jnp.logical_and(jnp.logical_and(inner, low), jnp.logical_not(left))
    left_low = jnp.logical_and(jnp.logical_and(inner, low), left)

    def meet():
        pl.semaphore_wait(barrier, jnp.where(right_low, middle, chans))

        @pl.when(jnp.logical_and(inner, jnp.logical_not(left)))
        def _():
            pl.when(high)(lambda: greet(inner_ready, *whole(across)[:middle]))

        @pl.when(jnp.logical_and(inner, left))
        def _():
            pl.when(low)(lambda: greet(inner_ready, device(chan, across)))

        @pl.when(outer)
        def _():
            greet(outer_ready, *whole(beside))

    meet_first = jnp.logical_and(high, jnp.logical_not(left))
    pl.when(meet_first)(meet)

    def make_tables(channels):
        for c in channels:
            tables[c, 0:LANES], tables[c, LANES:] = split(filter_table(row_taps[c : c + 1, :]))

    def filter_band(which, channels):
        start = pl.multiple_of(which * band_rows, 8)
        for c in channels:
            wide = x_buf[c, pl.ds(start, band_rows + 16), :]
            window = jnp.concatenate(
                [
                    wide[8 + (k - 1) * local_rows : 8 + (k - 1) * local_rows + band_rows]
                    for k in range(3)
                ],
                axis=1,
            )
            both = lax.dot_general(
                jnp.concatenate(split(window), axis=0),
                tables[c],
                (((1,), (1,)), ((), ())),
                preferred_element_type=jnp.float32,
            )
            filtered = both[:band_rows, :LANES] + (
                both[band_rows:, :LANES] + both[:band_rows, LANES:]
            )
            for to in range(chans):
                for tile in range(tiles):
                    at = (to * tiles + tile) * local_rows
                    send_one[
                        which * chans + to,
                        tile,
                        c * local_rows : (c + 1) * local_rows,
                        :,
                    ] = filtered[at : at + local_rows, :]

    step = tiles // CHUNKS
    block = local_channels * local_rows
    every = (0, block)

    def send(chunk, names, rows=every):
        part, lines = pl.ds(chunk * step, step), pl.ds(rows[0], rows[1])
        for name, slot in names:
            pltpu.make_async_remote_copy(
                src_ref=send_one.at[slot, part, lines],
                dst_ref=recv_one.at[part, me, lines],
                send_sem=send_sem.at[0],
                recv_sem=recv_one_sem.at[chunk],
                device_id=name,
                device_id_type=pl.DeviceIdType.MESH,
            ).start()

    row_load.wait()
    near, far = whole(first)[:middle], whole(first)[middle:]
    both_high = jnp.logical_and(inner, high)
    for piece in range(2):
        channels = range(piece * local_channels // 2, (piece + 1) * local_channels // 2)
        rows = (piece * block // 2, block // 2)
        make_tables(channels)
        loaded = x_inside.at[pl.ds(channels[0], len(channels))]
        pltpu.make_async_copy(loaded, loaded, x_sem.at[piece]).wait()
        filter_band(first, channels)
        if piece == 0:
            pl.when(jnp.logical_not(meet_first))(meet)
        for chunk in range(CHUNKS):
            pl.when(inner)(lambda: send(chunk, near, rows))
            pl.when(both_high)(lambda: send(chunk, far, rows))
    small_loads = [
        pltpu.make_async_copy(column_hbm, column_taps, row_sem),
        pltpu.make_async_copy(mix_hbm, channel_mix, x_sem.at[0]),
    ]
    for load in small_loads:
        load.start()

    @pl.when(right_low)
    def _():
        pl.semaphore_wait(inner_ready, 1)
        for chunk in range(CHUNKS):
            send(chunk, far)

    for to in (beside, second, band):
        filter_band(to, range(local_channels))

    @pl.when(left_low)
    def _():
        pl.semaphore_wait(inner_ready, middle)
        for chunk in range(CHUNKS):
            send(chunk, far)

    @pl.when(inner)
    def _():
        pl.semaphore_wait(outer_ready, chans)
        greet(go_first, device(chan, beside))
        greet(go_outer, device(chan, across))

    pl.when(inner)(lambda: send(0, whole(beside)))

    @pl.when(outer)
    def _():
        pl.semaphore_wait(go_first, 1)
        send(0, near + far)
        send(0, whole(beside))
        send(0, own)

    @pl.when(inner)
    def _():
        pl.semaphore_wait(go_outer, 1)
        greet(go_all, device(chan, beside))

    @pl.when(outer)
    def _():
        pl.semaphore_wait(go_all, 1)

    send(0, whole(second))
    pl.when(inner)(lambda: send(0, own))
    for chunk in range(1, CHUNKS):
        pl.when(outer)(lambda: send(chunk, whole(beside)))
        pl.when(outer)(lambda: send(chunk, near + far))
        send(chunk, whole(second))
        pl.when(inner)(lambda: send(chunk, whole(beside)))
        send(chunk, own)
    recv_one[:, me] = send_one[me]

    for load in small_loads:
        load.wait()
    table = mixing_table(
        column_taps[...], channel_mix[...], chans, bands, local_channels, local_rows
    )
    mixing[0], mixing[1] = split(table)

    rows = step * local_rows

    def back(chunk, name, slot):
        pltpu.make_async_remote_copy(
            src_ref=send_two.at[slot, :, pl.ds(chunk * rows, rows)],
            dst_ref=out_ref.at[
                :, pl.ds(pl.multiple_of(me * block_rows + chunk * rows, 8), rows)
            ],
            send_sem=send_sem.at[1],
            recv_sem=recv_two_sem,
            device_id=name,
            device_id_type=pl.DeviceIdType.MESH,
        ).start()

    late = band == half
    near_first = jnp.logical_or(left, band > half)

    def send_near(chunk):
        for name, slot in whole(beside) + own:
            back(chunk, name, slot)

    def send_back(chunk):
        early = near_first if chunk else left
        pl.when(early)(functools.partial(send_near, chunk))
        for k in range(half):
            to = jnp.where(left, half + k, k)
            crossed = [device(chan ^ step, to) for step in reversed(range(chans))]
            for at, (name, slot) in enumerate(crossed if k else whole(to)):
                hold = jnp.logical_and(late, low) if at < 2 else late
                if k == 0:
                    back(chunk, name, slot)
                elif chunk < CHUNKS - 1:
                    pl.when(jnp.logical_not(hold))(functools.partial(back, chunk, name, slot))
                else:
                    for held in range(chunk):
                        pl.when(hold)(functools.partial(back, held, name, slot))
                    back(chunk, name, slot)
        pl.when(jnp.logical_not(early))(functools.partial(send_near, chunk))

    for chunk in range(CHUNKS):
        part = pl.ds(chunk * step, step)
        landed = recv_one.at[part, others]
        pltpu.make_async_copy(landed, landed, recv_one_sem.at[chunk]).wait()
        columns = jnp.concatenate(
            [
                recv_one[chunk * step + tile].reshape(mixing.shape[1], LANES)
                for tile in range(step)
            ],
            axis=1,
        )
        mixed = product((mixing[0], mixing[1]), split(columns), ((1,), (0,)))
        for to_device in range(devices):
            for c in range(local_channels):
                at = (to_device * local_channels + c) * local_rows
                for tile in range(step):
                    to = (chunk * step + tile) * local_rows
                    send_two[to_device, c, to : to + local_rows, :] = mixed[
                        at : at + local_rows, tile * LANES : (tile + 1) * LANES
                    ]
        there = pl.ds(pl.multiple_of(me * block_rows + chunk * rows, 8), rows)
        send_back(chunk)
        out_ref[:, there, :] = send_two[me, :, chunk * rows : (chunk + 1) * rows, :]

    sent = send_one.at[others]
    pltpu.make_async_copy(sent, sent, send_sem.at[0]).wait()
    sent = send_two.at[others]
    pltpu.make_async_copy(sent, sent, send_sem.at[1]).wait()
    landed = out_ref.at[:, pl.ds(0, (devices - 1) * block_rows)]
    pltpu.make_async_copy(landed, landed, recv_two_sem).wait()


def fused(chans, bands, slide_region, row_taps, column_taps, channel_mix):
    local_channels, local_rows, width = slide_region.shape
    devices = chans * bands
    total_tiles = width // LANES
    tiles = total_tiles // devices
    block = local_channels * local_rows
    tiled = slide_region.reshape(local_channels, local_rows, total_tiles, LANES)
    tiled = tiled.transpose(0, 2, 1, 3).reshape(local_channels, total_tiles * local_rows, LANES)
    vmem = pl.BlockSpec(memory_space=pltpu.VMEM)
    anywhere = pl.BlockSpec(memory_space=pl.ANY)
    dma = pltpu.SemaphoreType.DMA
    out = pl.pallas_call(
        functools.partial(fused_kernel, chans, bands),
        out_shape=pltpu.VMEM(tiled.shape, jnp.float32),
        in_specs=[anywhere] * 4,
        out_specs=vmem,
        scratch_shapes=[
            pltpu.VMEM((local_channels, tiled.shape[1] + 16, LANES), jnp.float32),
            pltpu.VMEM(row_taps.shape, jnp.float32),
            pltpu.VMEM(column_taps.shape, jnp.float32),
            pltpu.VMEM(channel_mix.shape, jnp.float32),
            pltpu.VMEM((local_channels, 2 * LANES, 3 * LANES), jnp.bfloat16),
            pltpu.VMEM((devices, tiles, block, LANES), jnp.float32),
            pltpu.VMEM((tiles, devices, block, LANES), jnp.float32),
            pltpu.VMEM((devices, local_channels, tiles * local_rows, LANES), jnp.float32),
            pltpu.VMEM((2, devices * block, devices * block), jnp.bfloat16),
            pltpu.SemaphoreType.REGULAR((3,)),
            dma((2,)),
            dma,
            dma((2,)),
            dma((CHUNKS,)),
            dma,
        ],
        compiler_params=pltpu.CompilerParams(collective_id=0, has_side_effects=True),
    )(tiled, row_taps, column_taps, channel_mix)
    out = out.reshape(local_channels, total_tiles, local_rows, LANES)
    return out.transpose(0, 2, 1, 3).reshape(slide_region.shape)


def power_of_two(number):
    return number & (number - 1) == 0


def program(chans, bands, slide_region, row_taps, column_taps, channel_mix):
    local_channels, local_rows, width = slide_region.shape
    devices = chans * bands
    margin = (row_taps.shape[1] - 1) // 2
    fits = (
        power_of_two(chans)
        and chans > 1
        and bands == 4
        and width % (devices * LANES * CHUNKS) == 0
        and margin == LANES
        and column_taps.shape[1] == row_taps.shape[1]
        and local_rows == 4
        and local_channels * local_rows % 16 == 0
        and local_rows * bands <= margin
        and width // (devices * LANES * CHUNKS) * local_rows % 8 == 0
        and devices * local_channels * local_rows <= 512
    )
    if fits:
        return fused(chans, bands, slide_region, row_taps, column_taps, channel_mix)
    return on_device(slide_region, row_taps, column_taps, channel_mix)


def solution(mesh):
    in_specs = (P("chan", ("groups", "band"), None), P("chan", None), P(), P())
    out_specs = P("chan", ("groups", "band"), None)
    return jax.shard_map(
        functools.partial(program, mesh.shape["chan"], mesh.shape["band"]),
        mesh=mesh,
        in_specs=in_specs,
        out_specs=out_specs,
        check_vma=False,
    )
```

```python
import functools

import jax
import jax.numpy as jnp
from jax import lax
from jax.experimental import pallas as pl
from jax.experimental.pallas import tpu as pltpu
from jax.sharding import PartitionSpec as P

precise = lax.Precision.HIGHEST


def band_tables(filter_taps, tile_size):
    channels, length = filter_taps.shape
    margin = (length - 1) // 2
    period = 4 * tile_size
    border = 3 * tile_size + length
    widened = jnp.pad(filter_taps, ((0, 0), (border, border)))
    lowest = margin - tile_size + border
    window = widened[:, lowest : lowest + 3 * tile_size]
    vector = jnp.pad(window, ((0, 0), (0, tile_size)))
    repeated = jnp.tile(vector, (1, tile_size))[:, : tile_size * (period - 1)]
    toeplitz = repeated.reshape(channels, tile_size, period - 1)[:, :, : 3 * tile_size]
    stacked = jnp.transpose(toeplitz, (0, 2, 1))
    return stacked.reshape(channels, 3, tile_size, tile_size)


def along_columns(signal, filter_taps):
    tile_size = 128
    tables = band_tables(filter_taps, tile_size)
    channels, row_count, col_count = signal.shape
    tile_count = col_count // tile_size
    tiled = signal.reshape(channels, row_count, tile_count, tile_size)
    padded = jnp.pad(tiled, ((0, 0), (0, 0), (1, 1), (0, 0)))
    result = jnp.einsum(
        "crti,cij->crtj", padded[:, :, 0:tile_count], tables[:, 0], precision=precise
    )
    result = result + jnp.einsum(
        "crti,cij->crtj", padded[:, :, 1 : tile_count + 1], tables[:, 1], precision=precise
    )
    result = result + jnp.einsum(
        "crti,cij->crtj", padded[:, :, 2:], tables[:, 2], precision=precise
    )
    return result.reshape(channels, row_count, col_count)


def along_rows(signal, filter_taps):
    channels, row_count, col_count = signal.shape
    tile_size = 128 if row_count % 128 == 0 else row_count
    tables = band_tables(filter_taps, tile_size)
    tile_count = row_count // tile_size
    tiled = signal.reshape(channels, tile_count, tile_size, col_count)
    padded = jnp.pad(tiled, ((0, 0), (1, 1), (0, 0), (0, 0)))
    result = jnp.einsum("ctiw,cij->ctjw", padded[:, 0:tile_count], tables[:, 0], precision=precise)
    result = result + jnp.einsum(
        "ctiw,cij->ctjw", padded[:, 1 : tile_count + 1], tables[:, 1], precision=precise
    )
    result = result + jnp.einsum("ctiw,cij->ctjw", padded[:, 2:], tables[:, 2], precision=precise)
    return result.reshape(channels, row_count, col_count)


def on_device(slide_region, row_taps, column_taps, channel_mix):
    local_channels = slide_region.shape[0]
    across = along_columns(slide_region, row_taps)
    column_band = lax.all_to_all(across, "band", split_axis=2, concat_axis=1, tiled=True)
    first_channel = lax.axis_index("chan") * local_channels
    own_taps = lax.dynamic_slice_in_dim(column_taps, first_channel, local_channels, 0)
    vertical = along_rows(column_band, own_taps)
    own_mixing = lax.dynamic_slice_in_dim(channel_mix, first_channel, local_channels, 0)
    blended = jnp.einsum(
        "oc,chw->ohw",
        own_mixing,
        lax.all_gather(vertical, "chan", axis=0, tiled=True),
        precision=precise,
    )
    return lax.all_to_all(blended, "band", split_axis=1, concat_axis=2, tiled=True)


LANES = 128
CHUNKS = 2


def split(value):
    high = value.astype(jnp.bfloat16)
    return high, (value - high.astype(jnp.float32)).astype(jnp.bfloat16)


def product(left, right, dims):
    (left_high, left_low), (right_high, right_low) = left, right
    dot = functools.partial(
        lax.dot_general, dimension_numbers=(dims, ((), ())), preferred_element_type=jnp.float32
    )
    return dot(left_high, right_high) + (dot(left_low, right_high) + dot(left_high, right_low))


def filter_table(taps):
    shape = (LANES, LANES)
    lane = lax.broadcasted_iota(jnp.int32, shape, 1)
    row = lax.broadcasted_iota(jnp.int32, shape, 0)
    first, second = (
        pltpu.roll(
            jnp.broadcast_to(taps[:, at : at + LANES], shape), 0, 1, stride=1, stride_axis=0
        )
        for at in (0, LANES)
    )
    last = jnp.broadcast_to(taps[:, 2 * LANES :], shape)
    zero = jnp.zeros(shape, jnp.float32)
    return jnp.concatenate(
        [
            jnp.where(lane >= row, first, zero),
            jnp.where(lane >= row, second, first),
            jnp.where(lane == row, last, jnp.where(lane < row, second, zero)),
        ],
        axis=1,
    )


def mixing_table(column_taps, channel_mix, chans, bands, local_channels, local_rows):
    channels = chans * local_channels
    height = bands * local_rows
    block = local_channels * local_rows
    size = chans * bands * block
    margin = (column_taps.shape[1] - 1) // 2

    def coordinates(index):
        device, inner = index // block, index % block
        return (
            local_channels * (device % chans) + inner // local_rows,
            local_rows * (device // chans) + inner % local_rows,
        )

    tall = (size, channels)
    wide = (channels, size)
    pick_tall = (
        coordinates(lax.broadcasted_iota(jnp.int32, tall, 0))[0]
        == lax.broadcasted_iota(jnp.int32, tall, 1)
    ).astype(jnp.float32)
    pick_wide = (
        coordinates(lax.broadcasted_iota(jnp.int32, wide, 1))[0]
        == lax.broadcasted_iota(jnp.int32, wide, 0)
    ).astype(jnp.float32)
    weights = jnp.dot(
        jnp.dot(pick_tall, channel_mix, precision=precise), pick_wide, precision=precise
    )
    taps = lax.dot_general(
        column_taps[:, : 2 * margin],
        pick_wide,
        (((0,), (0,)), ((), ())),
        precision=precise,
    )
    square = (size, size)
    apart = (
        coordinates(lax.broadcasted_iota(jnp.int32, square, 1))[1]
        - coordinates(lax.broadcasted_iota(jnp.int32, square, 0))[1]
    )
    spread = jnp.zeros(square, jnp.float32)
    for distance in range(1 - height, height):
        at = margin + distance
        spread = jnp.where(apart == distance, taps[at : at + 1, :], spread)
    return weights * spread


def fused_kernel(
    chans, bands, x_hbm, row_hbm, column_hbm, mix_hbm, out_ref,
    x_buf, row_taps, column_taps, channel_mix, tables,
    send_one, recv_one, send_two, mixing,
    ready, x_sem, row_sem, send_sem, recv_one_sem, recv_two_sem,
):
    local_channels, x_rows, _ = x_hbm.shape
    devices, _, block_rows, _ = send_two.shape
    tiles = send_one.shape[1]
    local_rows = block_rows // tiles
    band_rows = x_rows // bands
    others = pl.ds(0, devices - 1)
    chan, band = lax.axis_index("chan"), lax.axis_index("band")
    me = band * chans + chan
    half = bands // 2
    left = band < half

    row_load = pltpu.make_async_copy(row_hbm, row_taps, row_sem)
    row_load.start()
    x_inside = x_buf.at[:, pl.ds(8, x_rows)]
    for c in range(local_channels):
        pltpu.make_async_copy(
            x_hbm.at[c], x_inside.at[c], x_sem.at[2 * c // local_channels]
        ).start()

    low = 2 * chan < chans
    inner = jnp.logical_or(band == half - 1, band == half)
    outer = jnp.logical_not(inner)
    high = jnp.logical_not(low)
    beside = band ^ 1
    across = band ^ 3
    first = jnp.where(inner, across, band ^ 2)
    second = jnp.where(inner, band ^ 2, across)

    def device(to_chan, to_band):
        to_chan = jnp.int32(to_chan) if isinstance(to_chan, int) else to_chan
        return {"chan": to_chan, "band": to_band}, to_band * chans + to_chan

    def whole(to_band):
        return [device(to_chan, to_band) for to_chan in range(chans)]

    own = [device(chan ^ step, band) for step in range(1, chans)]
    middle = chans // 2

    barrier = pltpu.get_barrier_semaphore()
    inner_ready = ready.at[0]
    outer_ready = go_first = ready.at[1]
    go_outer = go_all = ready.at[2]

    def greet(semaphore, *names):
        for name, _slot in names:
            pl.semaphore_signal(
                semaphore, inc=1, device_id=name, device_id_type=pl.DeviceIdType.MESH
            )

    @pl.when(inner)
    def _():
        pl.when(low)(lambda: greet(barrier, *whole(across)[:middle]))
        vouched = jnp.logical_and(left, high)
        pl.when(vouched)(lambda: greet(barrier, *whole(band)[:middle]))
        greet(barrier, *whole(across)[middle:], *whole(beside))

    mixing[...] = jnp.zeros(mixing.shape, mixing.dtype)
    span = devices // local_channels
    for lap in range(3):
        send_two[pl.ds(lap % local_channels * span, span)] = lax.dot_general(
            mixing[0], mixing[1], (((1,), (1,)), ((), ())), preferred_element_type=jnp.float32
        )[:, :LANES].reshape(span, *send_two.shape[1:])
    edge = jnp.zeros((8, LANES), jnp.float32)
    for c in range(local_channels):
        x_buf[c, 0:8, :] = edge
        x_buf[c, x_rows + 8 : x_rows + 16, :] = edge

    right_low = jnp.logical_and(jnp.logical_and(inner, low), jnp.logical_not(left))
    left_low = jnp.logical_and(jnp.logical_and(inner, low), left)

    def meet():
        pl.semaphore_wait(barrier, jnp.where(right_low, middle, chans))

        @pl.when(jnp.logical_and(inner, jnp.logical_not(left)))
        def _():
            pl.when(high)(lambda: greet(inner_ready, *whole(across)[:middle]))

        @pl.when(jnp.logical_and(inner, left))
        def _():
            pl.when(low)(lambda: greet(inner_ready, device(chan, across)))

        @pl.when(outer)
        def _():
            greet(outer_ready, *whole(beside))

    meet_first = jnp.logical_and(high, jnp.logical_not(left))
    pl.when(meet_first)(meet)

    def make_tables(channels):
        for c in channels:
            tables[c, 0:LANES], tables[c, LANES:] = split(filter_table(row_taps[c : c + 1, :]))

    def filter_band(which, channels):
        start = pl.multiple_of(which * band_rows, 8)
        for c in channels:
            wide = x_buf[c, pl.ds(start, band_rows + 16), :]
            window = jnp.concatenate(
                [
                    wide[8 + (k - 1) * local_rows : 8 + (k - 1) * local_rows + band_rows]
                    for k in range(3)
                ],
                axis=1,
            )
            both = lax.dot_general(
                jnp.concatenate(split(window), axis=0),
                tables[c],
                (((1,), (1,)), ((), ())),
                preferred_element_type=jnp.float32,
            )
            filtered = both[:band_rows, :LANES] + (
                both[band_rows:, :LANES] + both[:band_rows, LANES:]
            )
            for to in range(chans):
                for tile in range(tiles):
                    at = (to * tiles + tile) * local_rows
                    send_one[
                        which * chans + to,
                        tile,
                        c * local_rows : (c + 1) * local_rows,
                        :,
                    ] = filtered[at : at + local_rows, :]

    step = tiles // CHUNKS
    block = local_channels * local_rows
    every = (0, block)

    def send(chunk, names, rows=every):
        part, lines = pl.ds(chunk * step, step), pl.ds(rows[0], rows[1])
        for name, slot in names:
            pltpu.make_async_remote_copy(
                src_ref=send_one.at[slot, part, lines],
                dst_ref=recv_one.at[part, me, lines],
                send_sem=send_sem.at[0],
                recv_sem=recv_one_sem.at[chunk],
                device_id=name,
                device_id_type=pl.DeviceIdType.MESH,
            ).start()

    row_load.wait()
    near, far = whole(first)[:middle], whole(first)[middle:]
    both_high = jnp.logical_and(inner, high)
    for piece in range(2):
        channels = range(piece * local_channels // 2, (piece + 1) * local_channels // 2)
        rows = (piece * block // 2, block // 2)
        make_tables(channels)
        loaded = x_inside.at[pl.ds(channels[0], len(channels))]
        pltpu.make_async_copy(loaded, loaded, x_sem.at[piece]).wait()
        filter_band(first, channels)
        if piece == 0:
            pl.when(jnp.logical_not(meet_first))(meet)
        for chunk in range(CHUNKS):
            pl.when(inner)(lambda: send(chunk, near, rows))
            pl.when(both_high)(lambda: send(chunk, far, rows))
    small_loads = [
        pltpu.make_async_copy(column_hbm, column_taps, row_sem),
        pltpu.make_async_copy(mix_hbm, channel_mix, x_sem.at[0]),
    ]
    for load in small_loads:
        load.start()

    @pl.when(right_low)
    def _():
        pl.semaphore_wait(inner_ready, 1)
        for chunk in range(CHUNKS):
            send(chunk, far)

    for to in (beside, second, band):
        filter_band(to, range(local_channels))

    @pl.when(left_low)
    def _():
        pl.semaphore_wait(inner_ready, middle)
        for chunk in range(CHUNKS):
            send(chunk, far)

    @pl.when(inner)
    def _():
        pl.semaphore_wait(outer_ready, chans)
        greet(go_first, device(chan, beside))
        greet(go_outer, device(chan, across))

    pl.when(inner)(lambda: send(0, whole(beside)))

    @pl.when(outer)
    def _():
        pl.semaphore_wait(go_first, 1)
        send(0, near + far)
        send(0, whole(beside))
        send(0, own)

    @pl.when(inner)
    def _():
        pl.semaphore_wait(go_outer, 1)
        greet(go_all, device(chan, beside))

    @pl.when(outer)
    def _():
        pl.semaphore_wait(go_all, 1)

    send(0, whole(second))
    pl.when(inner)(lambda: send(0, own))
    for chunk in range(1, CHUNKS):
        pl.when(outer)(lambda: send(chunk, whole(beside)))
        pl.when(outer)(lambda: send(chunk, near + far))
        send(chunk, whole(second))
        pl.when(inner)(lambda: send(chunk, whole(beside)))
        send(chunk, own)
    recv_one[:, me] = send_one[me]

    for load in small_loads:
        load.wait()
    table = mixing_table(
        column_taps[...], channel_mix[...], chans, bands, local_channels, local_rows
    )
    mixing[0], mixing[1] = split(table)

    rows = step * local_rows

    def back(chunk, name, slot):
        pltpu.make_async_remote_copy(
            src_ref=send_two.at[slot, :, pl.ds(chunk * rows, rows)],
            dst_ref=out_ref.at[
                :, pl.ds(pl.multiple_of(me * block_rows + chunk * rows, 8), rows)
            ],
            send_sem=send_sem.at[1],
            recv_sem=recv_two_sem,
            device_id=name,
            device_id_type=pl.DeviceIdType.MESH,
        ).start()

    late = band == half
    near_first = jnp.logical_or(left, band > half)

    def send_near(chunk):
        for name, slot in whole(beside) + own:
            back(chunk, name, slot)

    def send_back(chunk):
        early = near_first if chunk else left
        pl.when(early)(functools.partial(send_near, chunk))
        for k in range(half):
            to = jnp.where(left, half + k, k)
            crossed = [device(chan ^ jnp.where(low, a, b), to) for a, b in zip([1, 0, 3, 2], [3, 2, 1, 0])]
            for at, (name, slot) in enumerate(crossed if k else whole(to)):
                hold = jnp.logical_and(late, low) if at < 2 else late
                if k == 0:
                    back(chunk, name, slot)
                elif chunk < CHUNKS - 1:
                    pl.when(jnp.logical_not(hold))(functools.partial(back, chunk, name, slot))
                else:
                    for held in range(chunk):
                        pl.when(hold)(functools.partial(back, held, name, slot))
                    back(chunk, name, slot)
        pl.when(jnp.logical_not(early))(functools.partial(send_near, chunk))

    for chunk in range(CHUNKS):
        part = pl.ds(chunk * step, step)
        landed = recv_one.at[part, others]
        pltpu.make_async_copy(landed, landed, recv_one_sem.at[chunk]).wait()
        columns = jnp.concatenate(
            [
                recv_one[chunk * step + tile].reshape(mixing.shape[1], LANES)
                for tile in range(step)
            ],
            axis=1,
        )
        mixed = product((mixing[0], mixing[1]), split(columns), ((1,), (0,)))
        for to_device in range(devices):
            for c in range(local_channels):
                at = (to_device * local_channels + c) * local_rows
                for tile in range(step):
                    to = (chunk * step + tile) * local_rows
                    send_two[to_device, c, to : to + local_rows, :] = mixed[
                        at : at + local_rows, tile * LANES : (tile + 1) * LANES
                    ]
        there = pl.ds(pl.multiple_of(me * block_rows + chunk * rows, 8), rows)
        send_back(chunk)
        out_ref[:, there, :] = send_two[me, :, chunk * rows : (chunk + 1) * rows, :]

    sent = send_one.at[others]
    pltpu.make_async_copy(sent, sent, send_sem.at[0]).wait()
    sent = send_two.at[others]
    pltpu.make_async_copy(sent, sent, send_sem.at[1]).wait()
    landed = out_ref.at[:, pl.ds(0, (devices - 1) * block_rows)]
    pltpu.make_async_copy(landed, landed, recv_two_sem).wait()


def fused(chans, bands, slide_region, row_taps, column_taps, channel_mix):
    local_channels, local_rows, width = slide_region.shape
    devices = chans * bands
    total_tiles = width // LANES
    tiles = total_tiles // devices
    block = local_channels * local_rows
    tiled = slide_region.reshape(local_channels, local_rows, total_tiles, LANES)
    tiled = tiled.transpose(0, 2, 1, 3).reshape(local_channels, total_tiles * local_rows, LANES)
    vmem = pl.BlockSpec(memory_space=pltpu.VMEM)
    anywhere = pl.BlockSpec(memory_space=pl.ANY)
    dma = pltpu.SemaphoreType.DMA
    out = pl.pallas_call(
        functools.partial(fused_kernel, chans, bands),
        out_shape=pltpu.VMEM(tiled.shape, jnp.float32),
        in_specs=[anywhere] * 4,
        out_specs=vmem,
        scratch_shapes=[
            pltpu.VMEM((local_channels, tiled.shape[1] + 16, LANES), jnp.float32),
            pltpu.VMEM(row_taps.shape, jnp.float32),
            pltpu.VMEM(column_taps.shape, jnp.float32),
            pltpu.VMEM(channel_mix.shape, jnp.float32),
            pltpu.VMEM((local_channels, 2 * LANES, 3 * LANES), jnp.bfloat16),
            pltpu.VMEM((devices, tiles, block, LANES), jnp.float32),
            pltpu.VMEM((tiles, devices, block, LANES), jnp.float32),
            pltpu.VMEM((devices, local_channels, tiles * local_rows, LANES), jnp.float32),
            pltpu.VMEM((2, devices * block, devices * block), jnp.bfloat16),
            pltpu.SemaphoreType.REGULAR((3,)),
            dma((2,)),
            dma,
            dma((2,)),
            dma((CHUNKS,)),
            dma,
        ],
        compiler_params=pltpu.CompilerParams(collective_id=0, has_side_effects=True),
    )(tiled, row_taps, column_taps, channel_mix)
    out = out.reshape(local_channels, total_tiles, local_rows, LANES)
    return out.transpose(0, 2, 1, 3).reshape(slide_region.shape)


def power_of_two(number):
    return number & (number - 1) == 0


def program(chans, bands, slide_region, row_taps, column_taps, channel_mix):
    local_channels, local_rows, width = slide_region.shape
    devices = chans * bands
    margin = (row_taps.shape[1] - 1) // 2
    fits = (
        power_of_two(chans)
        and chans > 1
        and bands == 4
        and width % (devices * LANES * CHUNKS) == 0
        and margin == LANES
        and column_taps.shape[1] == row_taps.shape[1]
        and local_rows == 4
        and local_channels * local_rows % 16 == 0
        and local_rows * bands <= margin
        and width // (devices * LANES * CHUNKS) * local_rows % 8 == 0
        and devices * local_channels * local_rows <= 512
    )
    if fits:
        return fused(chans, bands, slide_region, row_taps, column_taps, channel_mix)
    return on_device(slide_region, row_taps, column_taps, channel_mix)


def solution(mesh):
    in_specs = (P("chan", ("groups", "band"), None), P("chan", None), P(), P())
    out_specs = P("chan", ("groups", "band"), None)
    return jax.shard_map(
        functools.partial(program, mesh.shape["chan"], mesh.shape["band"]),
        mesh=mesh,
        in_specs=in_specs,
        out_specs=out_specs,
        check_vma=False,
    )
```

```python
import functools

import jax
import jax.numpy as jnp
from jax import lax
from jax.experimental import pallas as pl
from jax.experimental.pallas import tpu as pltpu
from jax.sharding import PartitionSpec as P

precise = lax.Precision.HIGHEST


def band_tables(filter_taps, tile_size):
    channels, length = filter_taps.shape
    margin = (length - 1) // 2
    period = 4 * tile_size
    border = 3 * tile_size + length
    widened = jnp.pad(filter_taps, ((0, 0), (border, border)))
    lowest = margin - tile_size + border
    window = widened[:, lowest : lowest + 3 * tile_size]
    vector = jnp.pad(window, ((0, 0), (0, tile_size)))
    repeated = jnp.tile(vector, (1, tile_size))[:, : tile_size * (period - 1)]
    toeplitz = repeated.reshape(channels, tile_size, period - 1)[:, :, : 3 * tile_size]
    stacked = jnp.transpose(toeplitz, (0, 2, 1))
    return stacked.reshape(channels, 3, tile_size, tile_size)


def along_columns(signal, filter_taps):
    tile_size = 128
    tables = band_tables(filter_taps, tile_size)
    channels, row_count, col_count = signal.shape
    tile_count = col_count // tile_size
    tiled = signal.reshape(channels, row_count, tile_count, tile_size)
    padded = jnp.pad(tiled, ((0, 0), (0, 0), (1, 1), (0, 0)))
    result = jnp.einsum(
        "crti,cij->crtj", padded[:, :, 0:tile_count], tables[:, 0], precision=precise
    )
    result = result + jnp.einsum(
        "crti,cij->crtj", padded[:, :, 1 : tile_count + 1], tables[:, 1], precision=precise
    )
    result = result + jnp.einsum(
        "crti,cij->crtj", padded[:, :, 2:], tables[:, 2], precision=precise
    )
    return result.reshape(channels, row_count, col_count)


def along_rows(signal, filter_taps):
    channels, row_count, col_count = signal.shape
    tile_size = 128 if row_count % 128 == 0 else row_count
    tables = band_tables(filter_taps, tile_size)
    tile_count = row_count // tile_size
    tiled = signal.reshape(channels, tile_count, tile_size, col_count)
    padded = jnp.pad(tiled, ((0, 0), (1, 1), (0, 0), (0, 0)))
    result = jnp.einsum("ctiw,cij->ctjw", padded[:, 0:tile_count], tables[:, 0], precision=precise)
    result = result + jnp.einsum(
        "ctiw,cij->ctjw", padded[:, 1 : tile_count + 1], tables[:, 1], precision=precise
    )
    result = result + jnp.einsum("ctiw,cij->ctjw", padded[:, 2:], tables[:, 2], precision=precise)
    return result.reshape(channels, row_count, col_count)


def on_device(slide_region, row_taps, column_taps, channel_mix):
    local_channels = slide_region.shape[0]
    across = along_columns(slide_region, row_taps)
    column_band = lax.all_to_all(across, "band", split_axis=2, concat_axis=1, tiled=True)
    first_channel = lax.axis_index("chan") * local_channels
    own_taps = lax.dynamic_slice_in_dim(column_taps, first_channel, local_channels, 0)
    vertical = along_rows(column_band, own_taps)
    own_mixing = lax.dynamic_slice_in_dim(channel_mix, first_channel, local_channels, 0)
    blended = jnp.einsum(
        "oc,chw->ohw",
        own_mixing,
        lax.all_gather(vertical, "chan", axis=0, tiled=True),
        precision=precise,
    )
    return lax.all_to_all(blended, "band", split_axis=1, concat_axis=2, tiled=True)


LANES = 128
CHUNKS = 2


def split(value):
    high = value.astype(jnp.bfloat16)
    return high, (value - high.astype(jnp.float32)).astype(jnp.bfloat16)


def product(left, right, dims):
    (left_high, left_low), (right_high, right_low) = left, right
    dot = functools.partial(
        lax.dot_general, dimension_numbers=(dims, ((), ())), preferred_element_type=jnp.float32
    )
    return dot(left_high, right_high) + (dot(left_low, right_high) + dot(left_high, right_low))


def filter_table(taps):
    shape = (LANES, LANES)
    lane = lax.broadcasted_iota(jnp.int32, shape, 1)
    row = lax.broadcasted_iota(jnp.int32, shape, 0)
    first, second = (
        pltpu.roll(
            jnp.broadcast_to(taps[:, at : at + LANES], shape), 0, 1, stride=1, stride_axis=0
        )
        for at in (0, LANES)
    )
    last = jnp.broadcast_to(taps[:, 2 * LANES :], shape)
    zero = jnp.zeros(shape, jnp.float32)
    return jnp.concatenate(
        [
            jnp.where(lane >= row, first, zero),
            jnp.where(lane >= row, second, first),
            jnp.where(lane == row, last, jnp.where(lane < row, second, zero)),
        ],
        axis=1,
    )


def mixing_table(column_taps, channel_mix, chans, bands, local_channels, local_rows):
    channels = chans * local_channels
    height = bands * local_rows
    block = local_channels * local_rows
    size = chans * bands * block
    margin = (column_taps.shape[1] - 1) // 2

    def coordinates(index):
        device, inner = index // block, index % block
        return (
            local_channels * (device % chans) + inner // local_rows,
            local_rows * (device // chans) + inner % local_rows,
        )

    tall = (size, channels)
    wide = (channels, size)
    pick_tall = (
        coordinates(lax.broadcasted_iota(jnp.int32, tall, 0))[0]
        == lax.broadcasted_iota(jnp.int32, tall, 1)
    ).astype(jnp.float32)
    pick_wide = (
        coordinates(lax.broadcasted_iota(jnp.int32, wide, 1))[0]
        == lax.broadcasted_iota(jnp.int32, wide, 0)
    ).astype(jnp.float32)
    weights = jnp.dot(
        jnp.dot(pick_tall, channel_mix, precision=precise), pick_wide, precision=precise
    )
    taps = lax.dot_general(
        column_taps[:, : 2 * margin],
        pick_wide,
        (((0,), (0,)), ((), ())),
        precision=precise,
    )
    square = (size, size)
    apart = (
        coordinates(lax.broadcasted_iota(jnp.int32, square, 1))[1]
        - coordinates(lax.broadcasted_iota(jnp.int32, square, 0))[1]
    )
    spread = jnp.zeros(square, jnp.float32)
    for distance in range(1 - height, height):
        at = margin + distance
        spread = jnp.where(apart == distance, taps[at : at + 1, :], spread)
    return weights * spread


def fused_kernel(
    chans, bands, x_hbm, row_hbm, column_hbm, mix_hbm, out_ref,
    x_buf, row_taps, column_taps, channel_mix, tables,
    send_one, recv_one, send_two, mixing,
    ready, x_sem, row_sem, send_sem, recv_one_sem, recv_two_sem,
):
    local_channels, x_rows, _ = x_hbm.shape
    devices, _, block_rows, _ = send_two.shape
    tiles = send_one.shape[1]
    local_rows = block_rows // tiles
    band_rows = x_rows // bands
    others = pl.ds(0, devices - 1)
    chan, band = lax.axis_index("chan"), lax.axis_index("band")
    me = band * chans + chan
    half = bands // 2
    left = band < half

    row_load = pltpu.make_async_copy(row_hbm, row_taps, row_sem)
    row_load.start()
    x_inside = x_buf.at[:, pl.ds(8, x_rows)]
    for c in range(local_channels):
        pltpu.make_async_copy(
            x_hbm.at[c], x_inside.at[c], x_sem.at[2 * c // local_channels]
        ).start()

    low = 2 * chan < chans
    inner = jnp.logical_or(band == half - 1, band == half)
    outer = jnp.logical_not(inner)
    high = jnp.logical_not(low)
    beside = band ^ 1
    across = band ^ 3
    first = jnp.where(inner, across, band ^ 2)
    second = jnp.where(inner, band ^ 2, across)

    def device(to_chan, to_band):
        to_chan = jnp.int32(to_chan) if isinstance(to_chan, int) else to_chan
        return {"chan": to_chan, "band": to_band}, to_band * chans + to_chan

    def whole(to_band):
        return [device(to_chan, to_band) for to_chan in range(chans)]

    own = [device(chan ^ step, band) for step in range(1, chans)]
    middle = chans // 2

    barrier = pltpu.get_barrier_semaphore()
    inner_ready = ready.at[0]
    outer_ready = go_first = ready.at[1]
    go_outer = go_all = ready.at[2]

    def greet(semaphore, *names):
        for name, _slot in names:
            pl.semaphore_signal(
                semaphore, inc=1, device_id=name, device_id_type=pl.DeviceIdType.MESH
            )

    @pl.when(inner)
    def _():
        pl.when(low)(lambda: greet(barrier, *whole(across)[:middle]))
        vouched = jnp.logical_and(left, high)
        pl.when(vouched)(lambda: greet(barrier, *whole(band)[:middle]))
        greet(barrier, *whole(across)[middle:], *whole(beside))

    mixing[...] = jnp.zeros(mixing.shape, mixing.dtype)
    span = devices // local_channels
    for lap in range(3):
        send_two[pl.ds(lap % local_channels * span, span)] = lax.dot_general(
            mixing[0], mixing[1], (((1,), (1,)), ((), ())), preferred_element_type=jnp.float32
        )[:, :LANES].reshape(span, *send_two.shape[1:])
    edge = jnp.zeros((8, LANES), jnp.float32)
    for c in range(local_channels):
        x_buf[c, 0:8, :] = edge
        x_buf[c, x_rows + 8 : x_rows + 16, :] = edge

    right_low = jnp.logical_and(jnp.logical_and(inner, low), jnp.logical_not(left))
    left_low = jnp.logical_and(jnp.logical_and(inner, low), left)

    def meet():
        pl.semaphore_wait(barrier, jnp.where(right_low, middle, chans))

        @pl.when(jnp.logical_and(inner, jnp.logical_not(left)))
        def _():
            pl.when(high)(lambda: greet(inner_ready, *whole(across)[:middle]))

        @pl.when(jnp.logical_and(inner, left))
        def _():
            pl.when(low)(lambda: greet(inner_ready, device(chan, across)))

        @pl.when(outer)
        def _():
            greet(outer_ready, *whole(beside))

    meet_first = jnp.logical_and(high, jnp.logical_not(left))
    pl.when(meet_first)(meet)

    def make_tables(channels):
        for c in channels:
            tables[c, 0:LANES], tables[c, LANES:] = split(filter_table(row_taps[c : c + 1, :]))

    def filter_band(which, channels):
        start = pl.multiple_of(which * band_rows, 8)
        for c in channels:
            wide = x_buf[c, pl.ds(start, band_rows + 16), :]
            window = jnp.concatenate(
                [
                    wide[8 + (k - 1) * local_rows : 8 + (k - 1) * local_rows + band_rows]
                    for k in range(3)
                ],
                axis=1,
            )
            both = lax.dot_general(
                jnp.concatenate(split(window), axis=0),
                tables[c],
                (((1,), (1,)), ((), ())),
                preferred_element_type=jnp.float32,
            )
            filtered = both[:band_rows, :LANES] + (
                both[band_rows:, :LANES] + both[:band_rows, LANES:]
            )
            for to in range(chans):
                for tile in range(tiles):
                    at = (to * tiles + tile) * local_rows
                    send_one[
                        which * chans + to,
                        tile,
                        c * local_rows : (c + 1) * local_rows,
                        :,
                    ] = filtered[at : at + local_rows, :]

    step = tiles // CHUNKS
    block = local_channels * local_rows
    every = (0, block)

    def send(chunk, names, rows=every):
        part, lines = pl.ds(chunk * step, step), pl.ds(rows[0], rows[1])
        for name, slot in names:
            pltpu.make_async_remote_copy(
                src_ref=send_one.at[slot, part, lines],
                dst_ref=recv_one.at[part, me, lines],
                send_sem=send_sem.at[0],
                recv_sem=recv_one_sem.at[chunk],
                device_id=name,
                device_id_type=pl.DeviceIdType.MESH,
            ).start()

    row_load.wait()
    near, far = whole(first)[:middle], whole(first)[middle:]
    both_high = jnp.logical_and(inner, high)
    for piece in range(2):
        channels = range(piece * local_channels // 2, (piece + 1) * local_channels // 2)
        rows = (piece * block // 2, block // 2)
        make_tables(channels)
        loaded = x_inside.at[pl.ds(channels[0], len(channels))]
        pltpu.make_async_copy(loaded, loaded, x_sem.at[piece]).wait()
        filter_band(first, channels)
        if piece == 0:
            pl.when(jnp.logical_not(meet_first))(meet)
        for chunk in range(CHUNKS):
            pl.when(inner)(lambda: send(chunk, near, rows))
            pl.when(both_high)(lambda: send(chunk, far, rows))
    small_loads = [
        pltpu.make_async_copy(column_hbm, column_taps, row_sem),
        pltpu.make_async_copy(mix_hbm, channel_mix, x_sem.at[0]),
    ]
    for load in small_loads:
        load.start()

    @pl.when(right_low)
    def _():
        pl.semaphore_wait(inner_ready, 1)
        for chunk in range(CHUNKS):
            send(chunk, far)

    for to in (beside, second, band):
        filter_band(to, range(local_channels))

    @pl.when(left_low)
    def _():
        pl.semaphore_wait(inner_ready, middle)
        for chunk in range(CHUNKS):
            send(chunk, far)

    @pl.when(inner)
    def _():
        pl.semaphore_wait(outer_ready, chans)
        greet(go_first, device(chan, beside))
        greet(go_outer, device(chan, across))

    pl.when(inner)(lambda: send(0, whole(beside)))

    @pl.when(outer)
    def _():
        pl.semaphore_wait(go_first, 1)
        send(0, near + far)
        send(0, whole(beside))
        send(0, own)

    @pl.when(inner)
    def _():
        pl.semaphore_wait(go_outer, 1)
        greet(go_all, device(chan, beside))

    @pl.when(outer)
    def _():
        pl.semaphore_wait(go_all, 1)

    send(0, whole(second))
    pl.when(inner)(lambda: send(0, own))
    for chunk in range(1, CHUNKS):
        pl.when(outer)(lambda: send(chunk, whole(beside)))
        pl.when(outer)(lambda: send(chunk, near + far))
        send(chunk, whole(second))
        pl.when(inner)(lambda: send(chunk, whole(beside)))
        send(chunk, own)
    recv_one[:, me] = send_one[me]

    for load in small_loads:
        load.wait()
    table = mixing_table(
        column_taps[...], channel_mix[...], chans, bands, local_channels, local_rows
    )
    mixing[0], mixing[1] = split(table)

    rows = step * local_rows

    def back(chunk, name, slot):
        pltpu.make_async_remote_copy(
            src_ref=send_two.at[slot, :, pl.ds(chunk * rows, rows)],
            dst_ref=out_ref.at[
                :, pl.ds(pl.multiple_of(me * block_rows + chunk * rows, 8), rows)
            ],
            send_sem=send_sem.at[1],
            recv_sem=recv_two_sem,
            device_id=name,
            device_id_type=pl.DeviceIdType.MESH,
        ).start()

    late = band == half
    near_first = jnp.logical_or(left, band > half)

    def send_near(chunk):
        for name, slot in whole(beside) + own:
            back(chunk, name, slot)

    def send_back(chunk):
        early = near_first if chunk else left
        pl.when(early)(functools.partial(send_near, chunk))
        for k in range(half):
            to = jnp.where(left, half + k, k)
            crossed = [device(chan ^ jnp.where(low, a, b), to) for a, b in zip([1, 0, 3, 2], [3, 2, 1, 0])]
            for at, (name, slot) in enumerate(crossed if k else whole(to)):
                hold = jnp.logical_and(late, low)
                if k == 0:
                    back(chunk, name, slot)
                elif chunk < CHUNKS - 1:
                    pl.when(jnp.logical_not(hold))(functools.partial(back, chunk, name, slot))
                else:
                    for held in range(chunk):
                        pl.when(hold)(functools.partial(back, held, name, slot))
                    back(chunk, name, slot)
        pl.when(jnp.logical_not(early))(functools.partial(send_near, chunk))

    for chunk in range(CHUNKS):
        part = pl.ds(chunk * step, step)
        landed = recv_one.at[part, others]
        pltpu.make_async_copy(landed, landed, recv_one_sem.at[chunk]).wait()
        columns = jnp.concatenate(
            [
                recv_one[chunk * step + tile].reshape(mixing.shape[1], LANES)
                for tile in range(step)
            ],
            axis=1,
        )
        mixed = product((mixing[0], mixing[1]), split(columns), ((1,), (0,)))
        for to_device in range(devices):
            for c in range(local_channels):
                at = (to_device * local_channels + c) * local_rows
                for tile in range(step):
                    to = (chunk * step + tile) * local_rows
                    send_two[to_device, c, to : to + local_rows, :] = mixed[
                        at : at + local_rows, tile * LANES : (tile + 1) * LANES
                    ]
        there = pl.ds(pl.multiple_of(me * block_rows + chunk * rows, 8), rows)
        send_back(chunk)
        out_ref[:, there, :] = send_two[me, :, chunk * rows : (chunk + 1) * rows, :]

    sent = send_one.at[others]
    pltpu.make_async_copy(sent, sent, send_sem.at[0]).wait()
    sent = send_two.at[others]
    pltpu.make_async_copy(sent, sent, send_sem.at[1]).wait()
    landed = out_ref.at[:, pl.ds(0, (devices - 1) * block_rows)]
    pltpu.make_async_copy(landed, landed, recv_two_sem).wait()


def fused(chans, bands, slide_region, row_taps, column_taps, channel_mix):
    local_channels, local_rows, width = slide_region.shape
    devices = chans * bands
    total_tiles = width // LANES
    tiles = total_tiles // devices
    block = local_channels * local_rows
    tiled = slide_region.reshape(local_channels, local_rows, total_tiles, LANES)
    tiled = tiled.transpose(0, 2, 1, 3).reshape(local_channels, total_tiles * local_rows, LANES)
    vmem = pl.BlockSpec(memory_space=pltpu.VMEM)
    anywhere = pl.BlockSpec(memory_space=pl.ANY)
    dma = pltpu.SemaphoreType.DMA
    out = pl.pallas_call(
        functools.partial(fused_kernel, chans, bands),
        out_shape=pltpu.VMEM(tiled.shape, jnp.float32),
        in_specs=[anywhere] * 4,
        out_specs=vmem,
        scratch_shapes=[
            pltpu.VMEM((local_channels, tiled.shape[1] + 16, LANES), jnp.float32),
            pltpu.VMEM(row_taps.shape, jnp.float32),
            pltpu.VMEM(column_taps.shape, jnp.float32),
            pltpu.VMEM(channel_mix.shape, jnp.float32),
            pltpu.VMEM((local_channels, 2 * LANES, 3 * LANES), jnp.bfloat16),
            pltpu.VMEM((devices, tiles, block, LANES), jnp.float32),
            pltpu.VMEM((tiles, devices, block, LANES), jnp.float32),
            pltpu.VMEM((devices, local_channels, tiles * local_rows, LANES), jnp.float32),
            pltpu.VMEM((2, devices * block, devices * block), jnp.bfloat16),
            pltpu.SemaphoreType.REGULAR((3,)),
            dma((2,)),
            dma,
            dma((2,)),
            dma((CHUNKS,)),
            dma,
        ],
        compiler_params=pltpu.CompilerParams(collective_id=0, has_side_effects=True),
    )(tiled, row_taps, column_taps, channel_mix)
    out = out.reshape(local_channels, total_tiles, local_rows, LANES)
    return out.transpose(0, 2, 1, 3).reshape(slide_region.shape)


def power_of_two(number):
    return number & (number - 1) == 0


def program(chans, bands, slide_region, row_taps, column_taps, channel_mix):
    local_channels, local_rows, width = slide_region.shape
    devices = chans * bands
    margin = (row_taps.shape[1] - 1) // 2
    fits = (
        power_of_two(chans)
        and chans > 1
        and bands == 4
        and width % (devices * LANES * CHUNKS) == 0
        and margin == LANES
        and column_taps.shape[1] == row_taps.shape[1]
        and local_rows == 4
        and local_channels * local_rows % 16 == 0
        and local_rows * bands <= margin
        and width // (devices * LANES * CHUNKS) * local_rows % 8 == 0
        and devices * local_channels * local_rows <= 512
    )
    if fits:
        return fused(chans, bands, slide_region, row_taps, column_taps, channel_mix)
    return on_device(slide_region, row_taps, column_taps, channel_mix)


def solution(mesh):
    in_specs = (P("chan", ("groups", "band"), None), P("chan", None), P(), P())
    out_specs = P("chan", ("groups", "band"), None)
    return jax.shard_map(
        functools.partial(program, mesh.shape["chan"], mesh.shape["band"]),
        mesh=mesh,
        in_specs=in_specs,
        out_specs=out_specs,
        check_vma=False,
    )
```

```python
import functools

import jax
import jax.numpy as jnp
from jax import lax
from jax.experimental import pallas as pl
from jax.experimental.pallas import tpu as pltpu
from jax.sharding import PartitionSpec as P

precise = lax.Precision.HIGHEST


def band_tables(filter_taps, tile_size):
    channels, length = filter_taps.shape
    margin = (length - 1) // 2
    period = 4 * tile_size
    border = 3 * tile_size + length
    widened = jnp.pad(filter_taps, ((0, 0), (border, border)))
    lowest = margin - tile_size + border
    window = widened[:, lowest : lowest + 3 * tile_size]
    vector = jnp.pad(window, ((0, 0), (0, tile_size)))
    repeated = jnp.tile(vector, (1, tile_size))[:, : tile_size * (period - 1)]
    toeplitz = repeated.reshape(channels, tile_size, period - 1)[:, :, : 3 * tile_size]
    stacked = jnp.transpose(toeplitz, (0, 2, 1))
    return stacked.reshape(channels, 3, tile_size, tile_size)


def along_columns(signal, filter_taps):
    tile_size = 128
    tables = band_tables(filter_taps, tile_size)
    channels, row_count, col_count = signal.shape
    tile_count = col_count // tile_size
    tiled = signal.reshape(channels, row_count, tile_count, tile_size)
    padded = jnp.pad(tiled, ((0, 0), (0, 0), (1, 1), (0, 0)))
    result = jnp.einsum(
        "crti,cij->crtj", padded[:, :, 0:tile_count], tables[:, 0], precision=precise
    )
    result = result + jnp.einsum(
        "crti,cij->crtj", padded[:, :, 1 : tile_count + 1], tables[:, 1], precision=precise
    )
    result = result + jnp.einsum(
        "crti,cij->crtj", padded[:, :, 2:], tables[:, 2], precision=precise
    )
    return result.reshape(channels, row_count, col_count)


def along_rows(signal, filter_taps):
    channels, row_count, col_count = signal.shape
    tile_size = 128 if row_count % 128 == 0 else row_count
    tables = band_tables(filter_taps, tile_size)
    tile_count = row_count // tile_size
    tiled = signal.reshape(channels, tile_count, tile_size, col_count)
    padded = jnp.pad(tiled, ((0, 0), (1, 1), (0, 0), (0, 0)))
    result = jnp.einsum("ctiw,cij->ctjw", padded[:, 0:tile_count], tables[:, 0], precision=precise)
    result = result + jnp.einsum(
        "ctiw,cij->ctjw", padded[:, 1 : tile_count + 1], tables[:, 1], precision=precise
    )
    result = result + jnp.einsum("ctiw,cij->ctjw", padded[:, 2:], tables[:, 2], precision=precise)
    return result.reshape(channels, row_count, col_count)


def on_device(slide_region, row_taps, column_taps, channel_mix):
    local_channels = slide_region.shape[0]
    across = along_columns(slide_region, row_taps)
    column_band = lax.all_to_all(across, "band", split_axis=2, concat_axis=1, tiled=True)
    first_channel = lax.axis_index("chan") * local_channels
    own_taps = lax.dynamic_slice_in_dim(column_taps, first_channel, local_channels, 0)
    vertical = along_rows(column_band, own_taps)
    own_mixing = lax.dynamic_slice_in_dim(channel_mix, first_channel, local_channels, 0)
    blended = jnp.einsum(
        "oc,chw->ohw",
        own_mixing,
        lax.all_gather(vertical, "chan", axis=0, tiled=True),
        precision=precise,
    )
    return lax.all_to_all(blended, "band", split_axis=1, concat_axis=2, tiled=True)


LANES = 128
CHUNKS = 2


def split(value):
    high = value.astype(jnp.bfloat16)
    return high, (value - high.astype(jnp.float32)).astype(jnp.bfloat16)


def product(left, right, dims):
    (left_high, left_low), (right_high, right_low) = left, right
    dot = functools.partial(
        lax.dot_general, dimension_numbers=(dims, ((), ())), preferred_element_type=jnp.float32
    )
    return dot(left_high, right_high) + (dot(left_low, right_high) + dot(left_high, right_low))


def filter_table(taps):
    shape = (LANES, LANES)
    lane = lax.broadcasted_iota(jnp.int32, shape, 1)
    row = lax.broadcasted_iota(jnp.int32, shape, 0)
    first, second = (
        pltpu.roll(
            jnp.broadcast_to(taps[:, at : at + LANES], shape), 0, 1, stride=1, stride_axis=0
        )
        for at in (0, LANES)
    )
    last = jnp.broadcast_to(taps[:, 2 * LANES :], shape)
    zero = jnp.zeros(shape, jnp.float32)
    return jnp.concatenate(
        [
            jnp.where(lane >= row, first, zero),
            jnp.where(lane >= row, second, first),
            jnp.where(lane == row, last, jnp.where(lane < row, second, zero)),
        ],
        axis=1,
    )


def mixing_table(column_taps, channel_mix, chans, bands, local_channels, local_rows):
    channels = chans * local_channels
    height = bands * local_rows
    block = local_channels * local_rows
    size = chans * bands * block
    margin = (column_taps.shape[1] - 1) // 2

    def coordinates(index):
        device, inner = index // block, index % block
        return (
            local_channels * (device % chans) + inner // local_rows,
            local_rows * (device // chans) + inner % local_rows,
        )

    tall = (size, channels)
    wide = (channels, size)
    pick_tall = (
        coordinates(lax.broadcasted_iota(jnp.int32, tall, 0))[0]
        == lax.broadcasted_iota(jnp.int32, tall, 1)
    ).astype(jnp.float32)
    pick_wide = (
        coordinates(lax.broadcasted_iota(jnp.int32, wide, 1))[0]
        == lax.broadcasted_iota(jnp.int32, wide, 0)
    ).astype(jnp.float32)
    weights = jnp.dot(
        jnp.dot(pick_tall, channel_mix, precision=precise), pick_wide, precision=precise
    )
    taps = lax.dot_general(
        column_taps[:, : 2 * margin],
        pick_wide,
        (((0,), (0,)), ((), ())),
        precision=precise,
    )
    square = (size, size)
    apart = (
        coordinates(lax.broadcasted_iota(jnp.int32, square, 1))[1]
        - coordinates(lax.broadcasted_iota(jnp.int32, square, 0))[1]
    )
    spread = jnp.zeros(square, jnp.float32)
    for distance in range(1 - height, height):
        at = margin + distance
        spread = jnp.where(apart == distance, taps[at : at + 1, :], spread)
    return weights * spread


def fused_kernel(
    chans, bands, x_hbm, row_hbm, column_hbm, mix_hbm, out_ref,
    x_buf, row_taps, column_taps, channel_mix, tables,
    send_one, recv_one, send_two, mixing,
    ready, x_sem, row_sem, send_sem, recv_one_sem, recv_two_sem,
):
    local_channels, x_rows, _ = x_hbm.shape
    devices, _, block_rows, _ = send_two.shape
    tiles = send_one.shape[1]
    local_rows = block_rows // tiles
    band_rows = x_rows // bands
    others = pl.ds(0, devices - 1)
    chan, band = lax.axis_index("chan"), lax.axis_index("band")
    me = band * chans + chan
    half = bands // 2
    left = band < half

    row_load = pltpu.make_async_copy(row_hbm, row_taps, row_sem)
    row_load.start()
    x_inside = x_buf.at[:, pl.ds(8, x_rows)]
    for c in range(local_channels):
        pltpu.make_async_copy(
            x_hbm.at[c], x_inside.at[c], x_sem.at[2 * c // local_channels]
        ).start()

    low = 2 * chan < chans
    inner = jnp.logical_or(band == half - 1, band == half)
    outer = jnp.logical_not(inner)
    high = jnp.logical_not(low)
    beside = band ^ 1
    across = band ^ 3
    first = jnp.where(inner, across, band ^ 2)
    second = jnp.where(inner, band ^ 2, across)

    def device(to_chan, to_band):
        to_chan = jnp.int32(to_chan) if isinstance(to_chan, int) else to_chan
        return {"chan": to_chan, "band": to_band}, to_band * chans + to_chan

    def whole(to_band):
        return [device(to_chan, to_band) for to_chan in range(chans)]

    own = [device(chan ^ step, band) for step in range(1, chans)]
    middle = chans // 2

    barrier = pltpu.get_barrier_semaphore()
    inner_ready = ready.at[0]
    outer_ready = go_first = ready.at[1]
    go_outer = go_all = ready.at[2]

    def greet(semaphore, *names):
        for name, _slot in names:
            pl.semaphore_signal(
                semaphore, inc=1, device_id=name, device_id_type=pl.DeviceIdType.MESH
            )

    @pl.when(inner)
    def _():
        pl.when(low)(lambda: greet(barrier, *whole(across)[:middle]))
        vouched = jnp.logical_and(left, high)
        pl.when(vouched)(lambda: greet(barrier, *whole(band)[:middle]))
        greet(barrier, *whole(across)[middle:], *whole(beside))

    mixing[...] = jnp.zeros(mixing.shape, mixing.dtype)
    span = devices // local_channels
    for lap in range(3):
        send_two[pl.ds(lap % local_channels * span, span)] = lax.dot_general(
            mixing[0], mixing[1], (((1,), (1,)), ((), ())), preferred_element_type=jnp.float32
        )[:, :LANES].reshape(span, *send_two.shape[1:])
    edge = jnp.zeros((8, LANES), jnp.float32)
    for c in range(local_channels):
        x_buf[c, 0:8, :] = edge
        x_buf[c, x_rows + 8 : x_rows + 16, :] = edge

    right_low = jnp.logical_and(jnp.logical_and(inner, low), jnp.logical_not(left))
    left_low = jnp.logical_and(jnp.logical_and(inner, low), left)

    def meet():
        pl.semaphore_wait(barrier, jnp.where(right_low, middle, chans))

        @pl.when(jnp.logical_and(inner, jnp.logical_not(left)))
        def _():
            pl.when(high)(lambda: greet(inner_ready, *whole(across)[:middle]))

        @pl.when(jnp.logical_and(inner, left))
        def _():
            pl.when(low)(lambda: greet(inner_ready, device(chan, across)))

        @pl.when(outer)
        def _():
            greet(outer_ready, *whole(beside))

    meet_first = jnp.logical_and(high, jnp.logical_not(left))
    pl.when(meet_first)(meet)

    def make_tables(channels):
        for c in channels:
            tables[c, 0:LANES], tables[c, LANES:] = split(filter_table(row_taps[c : c + 1, :]))

    def filter_band(which, channels):
        start = pl.multiple_of(which * band_rows, 8)
        for c in channels:
            wide = x_buf[c, pl.ds(start, band_rows + 16), :]
            window = jnp.concatenate(
                [
                    wide[8 + (k - 1) * local_rows : 8 + (k - 1) * local_rows + band_rows]
                    for k in range(3)
                ],
                axis=1,
            )
            both = lax.dot_general(
                jnp.concatenate(split(window), axis=0),
                tables[c],
                (((1,), (1,)), ((), ())),
                preferred_element_type=jnp.float32,
            )
            filtered = both[:band_rows, :LANES] + (
                both[band_rows:, :LANES] + both[:band_rows, LANES:]
            )
            for to in range(chans):
                for tile in range(tiles):
                    at = (to * tiles + tile) * local_rows
                    send_one[
                        which * chans + to,
                        tile,
                        c * local_rows : (c + 1) * local_rows,
                        :,
                    ] = filtered[at : at + local_rows, :]

    step = tiles // CHUNKS
    block = local_channels * local_rows
    every = (0, block)

    def send(chunk, names, rows=every):
        part, lines = pl.ds(chunk * step, step), pl.ds(rows[0], rows[1])
        for name, slot in names:
            pltpu.make_async_remote_copy(
                src_ref=send_one.at[slot, part, lines],
                dst_ref=recv_one.at[part, me, lines],
                send_sem=send_sem.at[0],
                recv_sem=recv_one_sem.at[chunk],
                device_id=name,
                device_id_type=pl.DeviceIdType.MESH,
            ).start()

    row_load.wait()
    near, far = whole(first)[:middle], whole(first)[middle:]
    both_high = jnp.logical_and(inner, high)
    for piece in range(2):
        channels = range(piece * local_channels // 2, (piece + 1) * local_channels // 2)
        rows = (piece * block // 2, block // 2)
        make_tables(channels)
        loaded = x_inside.at[pl.ds(channels[0], len(channels))]
        pltpu.make_async_copy(loaded, loaded, x_sem.at[piece]).wait()
        filter_band(first, channels)
        if piece == 0:
            pl.when(jnp.logical_not(meet_first))(meet)
        for chunk in range(CHUNKS):
            pl.when(inner)(lambda: send(chunk, near, rows))
            pl.when(both_high)(lambda: send(chunk, far, rows))
    small_loads = [
        pltpu.make_async_copy(column_hbm, column_taps, row_sem),
        pltpu.make_async_copy(mix_hbm, channel_mix, x_sem.at[0]),
    ]
    for load in small_loads:
        load.start()

    @pl.when(right_low)
    def _():
        pl.semaphore_wait(inner_ready, 1)
        for chunk in range(CHUNKS):
            send(chunk, far)

    for to in (beside, second, band):
        filter_band(to, range(local_channels))

    @pl.when(left_low)
    def _():
        pl.semaphore_wait(inner_ready, middle)
        for chunk in range(CHUNKS):
            send(chunk, far)

    @pl.when(inner)
    def _():
        pl.semaphore_wait(outer_ready, chans)
        greet(go_first, device(chan, beside))
        greet(go_outer, device(chan, across))

    pl.when(inner)(lambda: send(0, whole(beside)))

    @pl.when(outer)
    def _():
        pl.semaphore_wait(go_first, 1)
        send(0, near + far)
        send(0, whole(beside))
        send(0, own)

    @pl.when(inner)
    def _():
        pl.semaphore_wait(go_outer, 1)
        greet(go_all, device(chan, beside))

    @pl.when(outer)
    def _():
        pl.semaphore_wait(go_all, 1)

    send(0, whole(second))
    pl.when(inner)(lambda: send(0, own))
    for chunk in range(1, CHUNKS):
        pl.when(outer)(lambda: send(chunk, whole(beside)))
        pl.when(outer)(lambda: send(chunk, near + far))
        send(chunk, whole(second))
        pl.when(inner)(lambda: send(chunk, whole(beside)))
        send(chunk, own)
    recv_one[:, me] = send_one[me]

    for load in small_loads:
        load.wait()
    table = mixing_table(
        column_taps[...], channel_mix[...], chans, bands, local_channels, local_rows
    )
    mixing[0], mixing[1] = split(table)

    rows = step * local_rows

    def back(chunk, name, slot):
        pltpu.make_async_remote_copy(
            src_ref=send_two.at[slot, :, pl.ds(chunk * rows, rows)],
            dst_ref=out_ref.at[
                :, pl.ds(pl.multiple_of(me * block_rows + chunk * rows, 8), rows)
            ],
            send_sem=send_sem.at[1],
            recv_sem=recv_two_sem,
            device_id=name,
            device_id_type=pl.DeviceIdType.MESH,
        ).start()

    late = band == half
    near_first = jnp.logical_or(left, band > half)

    def send_near(chunk):
        for name, slot in whole(beside) + own:
            back(chunk, name, slot)

    def send_back(chunk):
        early = near_first if chunk else left
        pl.when(early)(functools.partial(send_near, chunk))
        for k in range(half):
            to = jnp.where(left, half + k, k)
            crossed = [device(chan ^ jnp.where(low, a, b), to) for a, b in zip([1, 0, 3, 2], [3, 1, 2, 0])]
            for at, (name, slot) in enumerate(crossed if k else whole(to)):
                hold = jnp.logical_and(late, low) if at < 2 else late
                if k == 0:
                    back(chunk, name, slot)
                elif chunk < CHUNKS - 1:
                    pl.when(jnp.logical_not(hold))(functools.partial(back, chunk, name, slot))
                else:
                    for held in range(chunk):
                        pl.when(hold)(functools.partial(back, held, name, slot))
                    back(chunk, name, slot)
        pl.when(jnp.logical_not(early))(functools.partial(send_near, chunk))

    for chunk in range(CHUNKS):
        part = pl.ds(chunk * step, step)
        landed = recv_one.at[part, others]
        pltpu.make_async_copy(landed, landed, recv_one_sem.at[chunk]).wait()
        columns = jnp.concatenate(
            [
                recv_one[chunk * step + tile].reshape(mixing.shape[1], LANES)
                for tile in range(step)
            ],
            axis=1,
        )
        mixed = product((mixing[0], mixing[1]), split(columns), ((1,), (0,)))
        for to_device in range(devices):
            for c in range(local_channels):
                at = (to_device * local_channels + c) * local_rows
                for tile in range(step):
                    to = (chunk * step + tile) * local_rows
                    send_two[to_device, c, to : to + local_rows, :] = mixed[
                        at : at + local_rows, tile * LANES : (tile + 1) * LANES
                    ]
        there = pl.ds(pl.multiple_of(me * block_rows + chunk * rows, 8), rows)
        send_back(chunk)
        out_ref[:, there, :] = send_two[me, :, chunk * rows : (chunk + 1) * rows, :]

    sent = send_one.at[others]
    pltpu.make_async_copy(sent, sent, send_sem.at[0]).wait()
    sent = send_two.at[others]
    pltpu.make_async_copy(sent, sent, send_sem.at[1]).wait()
    landed = out_ref.at[:, pl.ds(0, (devices - 1) * block_rows)]
    pltpu.make_async_copy(landed, landed, recv_two_sem).wait()


def fused(chans, bands, slide_region, row_taps, column_taps, channel_mix):
    local_channels, local_rows, width = slide_region.shape
    devices = chans * bands
    total_tiles = width // LANES
    tiles = total_tiles // devices
    block = local_channels * local_rows
    tiled = slide_region.reshape(local_channels, local_rows, total_tiles, LANES)
    tiled = tiled.transpose(0, 2, 1, 3).reshape(local_channels, total_tiles * local_rows, LANES)
    vmem = pl.BlockSpec(memory_space=pltpu.VMEM)
    anywhere = pl.BlockSpec(memory_space=pl.ANY)
    dma = pltpu.SemaphoreType.DMA
    out = pl.pallas_call(
        functools.partial(fused_kernel, chans, bands),
        out_shape=pltpu.VMEM(tiled.shape, jnp.float32),
        in_specs=[anywhere] * 4,
        out_specs=vmem,
        scratch_shapes=[
            pltpu.VMEM((local_channels, tiled.shape[1] + 16, LANES), jnp.float32),
            pltpu.VMEM(row_taps.shape, jnp.float32),
            pltpu.VMEM(column_taps.shape, jnp.float32),
            pltpu.VMEM(channel_mix.shape, jnp.float32),
            pltpu.VMEM((local_channels, 2 * LANES, 3 * LANES), jnp.bfloat16),
            pltpu.VMEM((devices, tiles, block, LANES), jnp.float32),
            pltpu.VMEM((tiles, devices, block, LANES), jnp.float32),
            pltpu.VMEM((devices, local_channels, tiles * local_rows, LANES), jnp.float32),
            pltpu.VMEM((2, devices * block, devices * block), jnp.bfloat16),
            pltpu.SemaphoreType.REGULAR((3,)),
            dma((2,)),
            dma,
            dma((2,)),
            dma((CHUNKS,)),
            dma,
        ],
        compiler_params=pltpu.CompilerParams(collective_id=0, has_side_effects=True),
    )(tiled, row_taps, column_taps, channel_mix)
    out = out.reshape(local_channels, total_tiles, local_rows, LANES)
    return out.transpose(0, 2, 1, 3).reshape(slide_region.shape)


def power_of_two(number):
    return number & (number - 1) == 0


def program(chans, bands, slide_region, row_taps, column_taps, channel_mix):
    local_channels, local_rows, width = slide_region.shape
    devices = chans * bands
    margin = (row_taps.shape[1] - 1) // 2
    fits = (
        power_of_two(chans)
        and chans > 1
        and bands == 4
        and width % (devices * LANES * CHUNKS) == 0
        and margin == LANES
        and column_taps.shape[1] == row_taps.shape[1]
        and local_rows == 4
        and local_channels * local_rows % 16 == 0
        and local_rows * bands <= margin
        and width // (devices * LANES * CHUNKS) * local_rows % 8 == 0
        and devices * local_channels * local_rows <= 512
    )
    if fits:
        return fused(chans, bands, slide_region, row_taps, column_taps, channel_mix)
    return on_device(slide_region, row_taps, column_taps, channel_mix)


def solution(mesh):
    in_specs = (P("chan", ("groups", "band"), None), P("chan", None), P(), P())
    out_specs = P("chan", ("groups", "band"), None)
    return jax.shard_map(
        functools.partial(program, mesh.shape["chan"], mesh.shape["band"]),
        mesh=mesh,
        in_specs=in_specs,
        out_specs=out_specs,
        check_vma=False,
    )
```
